256 devices in a mesh: gx: 8 (over z), gy: 4 (over y), gz: 8 (over x, core).
Axes of the slice: x: 4, y: 4, z: 8, core: 2. Of those that a mesh axis runs over, the one named last changes fastest.
Arguments:
- source_points: float32 [3, 13, 8, 16, 16, 512], P(None, None, 'gx', 'gy', 'gz'), may hold values from -3 to 3
- target_points: float32 [3, 13, 8, 16, 16, 512], P(None, None, 'gx', 'gy', 'gz'), may hold values from -3 to 3
- normals: float32 [3, 13, 8, 16, 16, 512], P(None, None, 'gx', 'gy', 'gz'), may hold values from -4 to 4
- weights: float32 [13, 8, 16, 16, 512], P(None, 'gx', 'gy', 'gz'), may hold values from 0.1 to 1
- blocks: int32 [13, 8, 16, 16], P(None, 'gx', 'gy', 'gz'), may hold values from 0 to 2
- affines: float32 [12, 8, 16, 16], P(None, 'gx', 'gy', 'gz'), may hold values from -0.5 to 0.5
- anchor: int32 [1], replicated, may hold values from 0 to 2047
Outputs:
- update: float32 [12, 8, 16, 16], P(None, 'gx', 'gy', 'gz')
- residual: float32 [12, 8, 16, 16], P(None, 'gx', 'gy', 'gz')
The draws below stay inside these ranges and needn't reach their ends.
Inputs may be any that keep to these rules, and one draw needn't show every extreme that they name: `blocks`: number of 256-point correspondence blocks of the correlation; entries of correlations whose second tile lies outside the grid are not read. `anchor`: a tile index (x 16 + y) * 16 + z.
All inputs are finite; a program needn't handle non-finite values.
Results may differ from the reference program's by a relative error of at most 0.0003.
Values sent between devices are 32-bit elements; how exact they have to be, the bound alone decides.
A program may use at most 128 MiB of HBM per device.

```python
import math
import jax
import jax.numpy as jnp
from jax import lax

DIRS = 13
BLOCK = 256
MAXB = 2
ITERS = 10
PTS = 512
NX = 8
NY = 16
NZ = 16


def touch_ends(drawn, stream_key, low, largest):
    index_at = [jax.random.randint(jax.random.fold_in(stream_key, axis), (), 0, length) for axis, length in enumerate(drawn.shape)]
    widest = drawn.shape.index(max(drawn.shape))
    next_to = index_at[:widest] + [(index_at[widest] + 1) % drawn.shape[widest]] + index_at[widest + 1:]
    return drawn.at[tuple(index_at)].set(low).at[tuple(next_to)].set(largest)


def steps_of(key, shape, pieces, smallest, largest):
    loudness, own = 1.0, jax.random.fold_in(key, 6)
    for dim, parts in pieces:
        draws = jnp.exp(jax.random.uniform(jax.random.fold_in(own, dim), (parts,), jnp.float32, smallest / len(pieces), largest / len(pieces)))
        loudness = loudness * jnp.repeat(draws, shape[dim] // parts).reshape([-1 if axis == dim else 1 for axis in range(len(shape))])
    return loudness


def centred(own_key, dims, scale, most, pieces=(), kind=jnp.bfloat16):
    factor_of = steps_of(own_key, dims, pieces, -0.22, 0.18) if pieces else 1.0
    array = jax.random.normal(own_key, dims, jnp.float32) * scale * factor_of
    return jnp.minimum(jnp.maximum(array, -most), most).astype(kind)


def setup_inputs(seed: int = 0) -> dict:
    keys = jax.random.split(jax.random.key(seed), 8)
    return {
        "source_points": centred(keys[0], (3, DIRS, NX, NY, NZ, PTS), 0.5, 3.0, ((2, 8), (3, 4), (4, 8)), jnp.float32),
        "target_points": centred(keys[1], (3, DIRS, NX, NY, NZ, PTS), 0.5, 3.0, ((2, 8), (3, 4), (4, 8)), jnp.float32),
        "normals": centred(keys[2], (3, DIRS, NX, NY, NZ, PTS), 1.0, 4.0, ((2, 8), (3, 4), (4, 8)), jnp.float32),
        "weights": jnp.clip(jnp.exp(math.log(1.0) - 2.3025851 * jax.random.uniform(keys[3], (DIRS, NX, NY, NZ, PTS), jnp.float32) ** steps_of(keys[3], (DIRS, NX, NY, NZ, PTS), ((1, 8), (2, 4), (3, 8)), -0.2, 0.2)), 0.1, 1.0),
        "blocks": touch_ends(jax.random.randint(keys[4], (DIRS, NX, NY, NZ), 0, MAXB + 1), jax.random.fold_in(keys[4], 1), 0, MAXB).astype(jnp.int32),
        "affines": centred(keys[5], (12, NX, NY, NZ), 0.1, 0.5, ((1, 8), (2, 4), (3, 8)), jnp.float32),
        "anchor": jax.random.randint(keys[6], (1,), 0, NX * NY * NZ).astype(jnp.int32),
    }


SPACING = 0.5
DAMPING = 1.0
OFFSETS = ((1, 0, 0), (0, 1, 0), (0, 0, 1), (1, 1, -1), (1, -1, 1), (-1, 1, 1), (1, 1, 0), (1, 0, 1), (0, 1, 1), (1, 1, 1), (1, -1, 0), (0, 1, -1), (-1, 0, 1))


def negated(offset):
    return tuple(-part for part in offset)


def moved(values, offset, first):
    widths = [(0, 0)] * values.ndim
    for axis in range(3):
        widths[first + axis] = (1, 1)
    padded = jnp.pad(values, widths)
    picks = [slice(None)] * values.ndim
    for axis in range(3):
        length = values.shape[first + axis]
        picks[first + axis] = slice(1 + offset[axis], 1 + offset[axis] + length)
    return padded[tuple(picks)]


def lifted(points):
    return jnp.concatenate([points, jnp.ones((1,) + points.shape[1:], points.dtype)], axis=0)


def mapped(affine, lifted_points):
    matrix = affine.reshape((3, 4) + affine.shape[1:]) + jnp.eye(3, 4, dtype=affine.dtype).reshape(3, 4, 1, 1, 1)
    return jnp.einsum("cexyz,exyzp->cxyzp", matrix, lifted_points, precision=lax.Precision.HIGHEST)


def correlation_terms(source, target, normal, weight, affine_here, affine_there, offset):
    exact = lax.Precision.HIGHEST
    source_lift = lifted(source)
    target_lift = lifted(target)
    stride = jnp.asarray(offset, source.dtype).reshape(3, 1, 1, 1, 1) * SPACING
    misfit = jnp.sum(normal * (mapped(affine_here, source_lift) - mapped(affine_there, target_lift) - stride), axis=0)
    layout = (12,) + source.shape[1:]
    rows_here = (normal[:, None] * source_lift[None]).reshape(layout)
    rows_there = -(normal[:, None] * target_lift[None]).reshape(layout)
    weighted_here = rows_here * weight
    weighted_there = rows_there * weight
    block_here = jnp.einsum("axyzp,bxyzp->abxyz", weighted_here, rows_here, precision=exact)
    block_pair = jnp.einsum("axyzp,bxyzp->abxyz", weighted_here, rows_there, precision=exact)
    block_there = jnp.einsum("axyzp,bxyzp->abxyz", weighted_there, rows_there, precision=exact)
    pull_here = jnp.einsum("axyzp,xyzp->axyz", weighted_here, misfit, precision=exact)
    pull_there = jnp.einsum("axyzp,xyzp->axyz", weighted_there, misfit, precision=exact)
    return block_here, block_pair, block_there, pull_here, pull_there


def invert_blocks(blocks):
    left = blocks
    right = jnp.broadcast_to(jnp.eye(12, dtype=blocks.dtype).reshape((12, 12) + (1,) * (blocks.ndim - 2)), blocks.shape)
    for pivot in range(12):
        factor = 1.0 / left[pivot, pivot]
        row_left = left[pivot] * factor
        row_right = right[pivot] * factor
        column = left[:, pivot]
        left = left - column[:, None] * row_left[None]
        right = right - column[:, None] * row_right[None]
        left = left.at[pivot].set(row_left)
        right = right.at[pivot].set(row_right)
    return right


def reference(source_points, target_points, normals, weights, blocks, affines, anchor):
    exact = lax.Precision.HIGHEST
    grid_x = jnp.arange(NX, dtype=jnp.int32).reshape(NX, 1, 1)
    grid_y = jnp.arange(NY, dtype=jnp.int32).reshape(1, NY, 1)
    grid_z = jnp.arange(NZ, dtype=jnp.int32).reshape(1, 1, NZ)
    flat = (grid_x * NY + grid_y) * NZ + grid_z
    keep = (flat != anchor[0]).astype(jnp.float32)
    filled = jnp.ones((NX, NY, NZ), jnp.float32)
    slots = jnp.arange(PTS, dtype=jnp.int32).reshape(1, 1, 1, PTS)
    diag = jnp.zeros((12, 12, NX, NY, NZ), jnp.float32)
    pull = jnp.zeros((12, NX, NY, NZ), jnp.float32)
    pairs = []
    for index, offset in enumerate(OFFSETS):
        inside = moved(filled, offset, 0)
        live = (slots < BLOCK * blocks[index][..., None]).astype(jnp.float32) * inside[..., None]
        target = moved(target_points[:, index], offset, 1)
        affine_there = moved(affines, offset, 1)
        block_here, block_pair, block_there, pull_here, pull_there = correlation_terms(
            source_points[:, index], target, normals[:, index], weights[index] * live, affines, affine_there, offset)
        diag = diag + block_here + moved(block_there, negated(offset), 2)
        pull = pull + pull_here + moved(pull_there, negated(offset), 1)
        pairs.append(block_pair * (keep * moved(keep, offset, 0)))
    coupling = jnp.stack(pairs)
    identity = jnp.eye(12, dtype=jnp.float32).reshape(12, 12, 1, 1, 1)
    diag = keep * (diag + DAMPING * identity) + (1.0 - keep) * identity
    rhs = -(keep * pull)
    inverse = invert_blocks(diag)

    def operate(vector):
        result = jnp.einsum("abxyz,bxyz->axyz", diag, vector, precision=exact)
        for index, offset in enumerate(OFFSETS):
            result = result + jnp.einsum("abxyz,bxyz->axyz", coupling[index], moved(vector, offset, 1), precision=exact)
            sent = jnp.einsum("baxyz,bxyz->axyz", coupling[index], vector, precision=exact)
            result = result + moved(sent, negated(offset), 1)
        return result

    def precondition(vector):
        return jnp.einsum("abxyz,bxyz->axyz", inverse, vector, precision=exact)

    update = jnp.zeros_like(rhs)
    residual = rhs
    scaled = precondition(residual)
    direction = scaled
    inner = jnp.sum(residual * scaled)
    for step in range(ITERS):
        image = operate(direction)
        alpha = inner / jnp.sum(direction * image)
        update = update + alpha * direction
        residual = residual - alpha * image
        scaled = precondition(residual)
        inner_next = jnp.sum(residual * scaled)
        direction = scaled + (inner_next / inner) * direction
        inner = inner_next
    return update, residual
```

```python
import functools

import jax
import jax.numpy as jnp
from jax import lax
from jax.experimental import pallas as pl
from jax.experimental.pallas import tpu as pltpu
from jax.sharding import PartitionSpec as P

BLOCK = 256
ITERS = 10
STEP = 2
SPACING = 0.5
DAMPING = 1.0
OFFSETS = (
    (1, 0, 0),
    (0, 1, 0),
    (0, 0, 1),
    (1, 1, -1),
    (1, -1, 1),
    (-1, 1, 1),
    (1, 1, 0),
    (1, 0, 1),
    (0, 1, 1),
    (1, 1, 1),
    (1, -1, 0),
    (0, 1, -1),
    (-1, 0, 1),
)
AXES = ("gx", "gy", "gz")
MESH = pl.DeviceIdType.MESH
LANES = 128
TY, TZ, TILES = 4, 2, 8
COMPS = 12
ROWS = COMPS * TILES
WIDE = ROWS + TILES
F32 = jnp.float32


def shifts(offset):
    seconds = (0,) if offset[1] == 0 else (0, offset[1])
    thirds = (0,) if offset[2] == 0 else (0, offset[2])
    return [(offset[0], y, z) for y in seconds for z in thirds]


SELF = (0, 0, 0)
REACH = (SELF, *sorted({s for o in OFFSETS for s in shifts(o)} - {SELF}))
OTHERS = len(REACH) - 1
GREET = tuple(sorted({s for s in REACH[1:]} | {tuple(-p for p in s) for s in REACH[1:]}))


def pieces():
    found = []
    for index, offset in enumerate(OFFSETS):
        for shift in shifts(offset):
            if shift == SELF:
                continue
            if offset[1] == 0:
                low, count = 0, TY
            elif shift[1] == 0:
                low, count = (1 if offset[1] > 0 else 0), TY - 1
            else:
                low, count = (0 if offset[1] > 0 else TY - 1), 1
            found.append((index, shift, low, count, 0 if shift[2] == 0 else 1))
    return tuple(found)


PIECES = pieces()


def device_at(shift, sign):
    there = []
    for axis, part in zip(AXES, shift):
        size = lax.axis_size(axis)
        there.append(lax.rem(lax.axis_index(axis) + (sign * part + size), size))
    return tuple(there)


def remote(source, target, sent, got, device):
    return pltpu.make_async_remote_copy(
        src_ref=source,
        dst_ref=target,
        send_sem=sent,
        recv_sem=got,
        device_id=device,
        device_id_type=MESH,
    )


def exchange_kernel(target, affine, near, far, affine_there, sent, got):
    barrier = pltpu.get_barrier_semaphore()
    for shift in GREET:
        pl.semaphore_signal(barrier, inc=1, device_id=device_at(shift, 1), device_id_type=MESH)
    pl.semaphore_wait(barrier, len(GREET))
    copies = []
    for number, (index, shift, low, count, which) in enumerate(PIECES):
        span = pl.ds(low, count)
        place = (near, far)[which]
        copies.append(
            remote(
                target.at[:, index, 0, span],
                place.at[:, index, span],
                sent.at[number],
                got.at[number],
                device_at(shift, -1),
            )
        )
    for number, shift in enumerate(REACH[1:]):
        at = len(PIECES) + number
        copies.append(
            remote(affine, affine_there.at[number], sent.at[at], got.at[at], device_at(shift, -1))
        )
    for copy in copies:
        copy.start()
    for copy in copies:
        copy.wait()


def iotas(rows=TILES):
    return (
        lax.broadcasted_iota(jnp.int32, (rows, LANES), 0),
        lax.broadcasted_iota(jnp.int32, (rows, LANES), 1),
    )


def tiled(mask, times):
    return jnp.concatenate([mask] * times, axis=0)


def cross(left, right):
    return lax.dot_general(
        left,
        right,
        (((1,), (1,)), ((), ())),
        precision=lax.Precision.HIGHEST,
        preferred_element_type=F32,
    )


def moments_kernel(
    source,
    target,
    near,
    far,
    normal,
    weight,
    affine,
    blocks,
    shares,
    own,
    slab,
    here,
    here_weighted,
    there,
    there_weighted,
    packed,
):
    sub, lane = iotas()
    slot = lane & (TILES - 1)
    blocks[...] = jnp.zeros_like(blocks)
    shares[...] = jnp.zeros_like(shares)
    own[...] = jnp.zeros_like(own)
    packed[...] = jnp.zeros_like(packed)
    here[WIDE:, :] = jnp.zeros((LANES - WIDE, here.shape[1]), F32)
    there[ROWS:, :] = jnp.zeros((LANES - ROWS, there.shape[1]), F32)
    same = sub == slot
    for index, offset in enumerate(OFFSETS):
        for y in range(TY):
            for c in range(3):
                slab[c, 2 * y : 2 * y + 2, :] = source[c, index, 0, y]
                slab[3 + c, 2 * y : 2 * y + 2, :] = normal[c, index, 0, y]
        for y in range(TY):
            before = (y - offset[1]) % TY
            shift_y = (y - offset[1]) // TY
            for z in range(TZ):
                back = (z - offset[2]) % TZ
                shift_z = (z - offset[2]) // TZ
                shift = (offset[0], -shift_y, -shift_z)
                to, come = y * TZ + z, before * TZ + back
                for c in range(3):
                    slab[6 + c, to : to + 1, :] = normal[c, index, 0, before, back : back + 1, :]
                    if shift == SELF:
                        row = target[c, index, 0, y, z : z + 1, :]
                    elif shift[2] == 0:
                        row = near[c, index, y, z : z + 1, :]
                    else:
                        row = far[c, index, y, z : z + 1, :]
                    slab[9 + c, to : to + 1, :] = row
                slab[12, to : to + 1, :] = weight[index, come : come + 1, :]
        share, share_there = weight[index], slab[12]
        for c in range(3):
            n, m = slab[3 + c], slab[6 + c]
            for e in range(4):
                at = (4 * c + e) * TILES
                a = n * slab[e] if e < 3 else n
                b = -(m * slab[9 + e]) if e < 3 else -m
                here[at : at + TILES, :] = a
                here_weighted[at : at + TILES, :] = a * share
                there[at : at + TILES, :] = b
                there_weighted[at : at + TILES, :] = b * share_there
        along = sum(part * slab[3 + c] for c, part in enumerate(offset) if part != 0)
        here[ROWS:WIDE, :] = along
        here_weighted[ROWS:WIDE, :] = along * share
        own[...] += cross(here_weighted[:ROWS, :], here[...])
        pair = cross(here_weighted[...], there[...])
        back = cross(there_weighted[...], there[...])
        for a in range(COMPS):
            at = a * TILES
            packed[a : a + 1, :] = jnp.sum(
                jnp.where(same, back[at : at + TILES, :], 0.0), axis=0, keepdims=True
            )
        second, third = sub // TZ + offset[1], sub % TZ + offset[2]
        slot_y, slot_z = slot // TZ, slot % TZ
        all_slots = packed[...]
        for shift in shifts(offset):
            j = REACH.index(shift)
            meets = (slot_y + TY * shift[1] == second) & (slot_z + TZ * shift[2] == third)
            blocks[j] += jnp.where(tiled(meets, WIDE // TILES), pair, 0.0)
            owned = jnp.ones((TILES, LANES), jnp.bool_)
            from_y, from_z = slot_y - offset[1] + TY * shift[1], slot_z - offset[2] + TZ * shift[2]
            owned = (from_y >= 0) & (from_y < TY) & (from_z >= 0) & (from_z < TZ)
            shares[j] += jnp.where(tiled(owned, 2), all_slots, 0.0)
    own[...] = jnp.where(tiled(same, COMPS), own[...], 0.0)
    row = affine[0]
    columns = [
        jnp.sum(jnp.where(lane == sub + a * TILES, row, 0.0), axis=1, keepdims=True)
        for a in range(COMPS + 1)
    ]
    for j in range(OTHERS + 1):
        total = jnp.zeros((TILES, LANES), F32)
        for a in range(COMPS + 1):
            total = total + blocks[j, a * TILES : (a + 1) * TILES, :] * columns[a]
        shares[j, COMPS : COMPS + 1, :] = jnp.sum(total, axis=0, keepdims=True)


def solve_kernel(steps, groups, *refs):
    blocks, shares, own, affine, affine_there, keep = refs[:6]
    update, residual = refs[6:8]
    shares_there, matrix, inverse, plane, basis, lifted_basis = refs[8:14]
    pair_sum, line_sum, pair_send, line_send = refs[14:18]
    rest = refs[18:]
    send_rows, got_rows, back_rows, got_back = (rest[k * steps : (k + 1) * steps] for k in range(4))
    share_sent, share_got, halo_sems, sum_sems = rest[4 * steps :]
    count = 2 * steps + 1
    first, second, third = (lax.axis_index(a) for a in AXES)
    size_first, size_second, size_third = (lax.axis_size(a) for a in AXES)
    in_pair = second * size_third + third
    pair_size = size_second * size_third

    def pair_peer(k):
        there = lax.rem(in_pair + k, pair_size)
        return (first, there // size_third, lax.rem(there, size_third))

    def line_peer(k):
        return (lax.rem(first + k, size_first), second, third)

    barrier = pltpu.get_barrier_semaphore()
    for shift in GREET:
        pl.semaphore_signal(barrier, inc=1, device_id=device_at(shift, 1), device_id_type=MESH)

    @pl.loop(1, pair_size)
    def _(k):
        pl.semaphore_signal(barrier, inc=1, device_id=pair_peer(k), device_id_type=MESH)

    @pl.loop(1, size_first)
    def _(k):
        pl.semaphore_signal(barrier, inc=1, device_id=line_peer(k), device_id_type=MESH)

    pl.semaphore_wait(barrier, len(GREET) + pair_size - 1 + size_first - 1)

    for number, shift in enumerate(REACH[1:]):
        remote(
            shares.at[number + 1],
            shares_there.at[number],
            share_sent,
            share_got,
            device_at(shift, 1),
        ).start()

    sub, lane = iotas()
    slot = lane & (TILES - 1)
    same = sub == slot
    eyes = [lane == sub + a * TILES for a in range(COMPS)]
    wide_sub, wide_lane = iotas(16)

    def column(row):
        return [jnp.sum(jnp.where(eyes[a], row, 0.0), axis=1, keepdims=True) for a in range(COMPS)]

    def group(a):
        return slice(a * TILES, (a + 1) * TILES)

    keep_row = keep[0]
    keep_column = column(keep_row)
    row = affine[0]
    sums = []
    for a in range(COMPS):
        total = own[group(a), :] * row + blocks[0, group(a), :] * row
        for j in range(OTHERS):
            total = total + blocks[j + 1, group(a), :] * affine_there[j]
        sums.append(total)
    everything = pltpu.make_async_copy(shares_there, shares_there, share_got)
    everything.wait()
    pltpu.make_async_copy(shares_there, shares_there, share_sent).wait()
    gathered = shares[0]
    for j in range(OTHERS):
        gathered = gathered + shares_there[j]
    right = []
    for a in range(COMPS):
        spread = jnp.where(same & (lane < ROWS), gathered[a : a + 1, :], 0.0)
        total = sums[a] + spread * row + jnp.where(eyes[a], gathered[COMPS : COMPS + 1, :], 0.0)
        right.append(-keep_column[a] * jnp.sum(total, axis=1, keepdims=True))
        mine = jnp.where(lane < ROWS, own[group(a), :], 0.0)
        compact = jnp.sum(mine, axis=0, keepdims=True) + gathered[a : a + 1, :]
        unit = jnp.where((lane[:1] >= a * TILES) & (lane[:1] < (a + 1) * TILES), 1.0, 0.0)
        compact = keep_row * (compact + DAMPING * unit) + (1.0 - keep_row) * unit
        picked = jnp.where(wide_lane // TILES == wide_sub, compact, 0.0)
        for by in (8, 16, 32, 64):
            picked = picked + pltpu.roll(picked, by, 1)
        matrix[a] = picked

    rows = [matrix[a] for a in range(COMPS)]
    for k in range(COMPS):
        factor = 1.0 / rows[k][k : k + 1, :]
        at_pivot = wide_sub == k
        pivot_row = jnp.where(at_pivot, factor, rows[k] * factor)
        for i in range(COMPS):
            if i != k:
                f = rows[i][k : k + 1, :]
                rows[i] = jnp.where(at_pivot, 0.0, rows[i]) - f * pivot_row
        rows[k] = pivot_row
    for a in range(COMPS):
        compact = jnp.sum(
            jnp.where(wide_lane // TILES == wide_sub, rows[a], 0.0), axis=0, keepdims=True
        )
        inverse[group(a), :] = jnp.where(same & (lane < ROWS), compact, 0.0)

    def as_row(col):
        total = jnp.zeros((TILES, LANES), F32)
        for a in range(COMPS):
            total = total + jnp.where(eyes[a], col[a], 0.0)
        return jnp.sum(total, axis=0, keepdims=True)

    def precondition(col):
        total = jnp.zeros((TILES, LANES), F32)
        for a in range(COMPS):
            total = total + inverse[group(a), :] * col[a]
        return jnp.sum(total, axis=0, keepdims=True)

    def couple(step, vectors):
        amount = len(vectors)
        cols = [column(v) for v in vectors]
        for r, v in enumerate(vectors):
            send_rows[step][0, r : r + 1, :] = v
        for number, shift in enumerate(REACH[1:]):
            remote(
                send_rows[step].at[0],
                got_rows[step].at[number],
                halo_sems.at[step, 0],
                halo_sems.at[step, 1],
                device_at(shift, -1),
            ).start()
        local = []
        for j in range(OTHERS + 1):
            totals = [jnp.zeros((TILES, LANES), F32) for _ in vectors]
            for a in range(COMPS):
                block = blocks[j, group(a), :]
                for r in range(amount):
                    totals[r] = totals[r] + block * cols[r][a]
            for r in range(amount):
                total = jnp.sum(totals[r], axis=0, keepdims=True)
                if j == 0:
                    local.append(total)
                else:
                    back_rows[step][j - 1, r : r + 1, :] = total
            if j > 0:
                remote(
                    back_rows[step].at[j - 1],
                    got_back[step].at[j - 1],
                    halo_sems.at[step, 2],
                    halo_sems.at[step, 3],
                    device_at(REACH[j], 1),
                ).start()
        sums = [[blocks[0, group(a), :] * v for a in range(COMPS)] for v in vectors]
        rows_there, back_there = got_rows[step], got_back[step]
        pltpu.make_async_copy(rows_there, rows_there, halo_sems.at[step, 1]).wait()
        for j in range(OTHERS):
            for r in range(amount):
                v = rows_there[j, r : r + 1, :]
                for a in range(COMPS):
                    sums[r][a] = sums[r][a] + blocks[j + 1, group(a), :] * v
        pltpu.make_async_copy(back_there, back_there, halo_sems.at[step, 3]).wait()
        results = []
        for r in range(amount):
            came = local[r]
            for j in range(OTHERS):
                came = came + back_there[j, r : r + 1, :]
            results.append(
                [
                    keep_column[a]
                    * jnp.sum(sums[r][a] + jnp.where(eyes[a], came, 0.0), axis=1, keepdims=True)
                    for a in range(COMPS)
                ]
            )
        pltpu.make_async_copy(rows_there, rows_there, halo_sems.at[step, 0]).wait()
        pltpu.make_async_copy(back_there, back_there, halo_sems.at[step, 2]).wait()
        return results

    def reduce_all(value, parity):
        pair_send[parity] = value
        pair_sum[parity, in_pair] = value

        @pl.loop(1, pair_size)
        def _(k):
            remote(
                pair_send.at[parity],
                pair_sum.at[parity, in_pair],
                sum_sems.at[parity, 0],
                sum_sems.at[parity, 1],
                pair_peer(k),
            ).start()

        part = pair_sum.at[parity, pl.ds(0, pair_size - 1)]
        pltpu.make_async_copy(part, part, sum_sems.at[parity, 1]).wait()
        total = pair_sum[parity, 0]
        for k in range(1, pair_size):
            total = total + pair_sum[parity, k]
        line_send[parity] = total
        line_sum[parity, first] = total

        @pl.loop(1, size_first)
        def _(k):
            remote(
                line_send.at[parity],
                line_sum.at[parity, first],
                sum_sems.at[parity, 2],
                sum_sems.at[parity, 3],
                line_peer(k),
            ).start()

        row_part = line_sum.at[parity, pl.ds(0, size_first - 1)]
        pltpu.make_async_copy(row_part, row_part, sum_sems.at[parity, 3]).wait()
        total = line_sum[parity, 0]
        for k in range(1, size_first):
            total = total + line_sum[parity, k]
        pltpu.make_async_copy(part, part, sum_sems.at[parity, 0]).wait()
        pltpu.make_async_copy(row_part, row_part, sum_sems.at[parity, 2]).wait()
        return total

    basis[...] = jnp.zeros_like(basis)
    lifted_basis[...] = jnp.zeros_like(lifted_basis)
    start, start_lifted = as_row(right), precondition(right)
    for at in (0, steps + 1):
        basis[at : at + 1, :] = start
        lifted_basis[at : at + 1, :] = start_lifted
    update[...] = jnp.zeros_like(update)

    major = jnp.zeros((TILES, LANES), jnp.int32)
    for k in range(1, count + 1):
        major = major + jnp.where(lane >= k * count, 1, 0)
    minor = lane - count * major

    def form(mask):
        return jnp.where(mask & (lane < count * count), 1.0, 0.0)

    @pl.loop(0, groups)
    def _(number):
        for step in range(steps):
            places = [step] + ([steps + 1 + step] if step < steps - 1 else [])
            found = couple(step, [lifted_basis[at : at + 1, :] for at in places])
            for at, col in zip(places, found):
                basis[at + 1 : at + 2, :] = as_row(col)
                lifted_basis[at + 1 : at + 2, :] = precondition(col)
        gram = cross(basis[...], lifted_basis[...])
        spread = jnp.zeros((16, LANES), F32)
        for k in range(count):
            moved = pltpu.roll(gram, k * count, 1) if k else gram
            spread = spread + jnp.where(wide_sub == k, moved, 0.0)
        mine = jnp.sum(spread, axis=0, keepdims=True)
        g = jnp.broadcast_to(reduce_all(mine, lax.rem(number, 2)), (TILES, LANES))

        def inner(x, y):
            return jnp.sum(g * x * y, axis=1, keepdims=True)

        p_major, p_minor = form(major == 0), form(minor == 0)
        r_major, r_minor = form(major == steps + 1), form(minor == steps + 1)
        u_minor = jnp.zeros((TILES, LANES), F32)
        product = inner(r_major, r_minor)
        for _ in range(steps):
            a_major = p_major + pltpu.roll(p_major, count, 1)
            a_minor = p_minor + pltpu.roll(p_minor, 1, 1)
            alpha = product / inner(p_major, a_minor)
            u_minor = u_minor + alpha * p_minor
            r_major = r_major - alpha * a_major
            r_minor = r_minor - alpha * a_minor
            following = inner(r_major, r_minor)
            ratio = following / product
            p_major = r_major + ratio * p_major
            p_minor = r_minor + ratio * p_minor
            product = following

        def combined(minor_form, vectors):
            both = jnp.concatenate([minor_form, minor_form], axis=0)
            weights = jnp.sum(
                jnp.where((wide_lane == wide_sub) & (wide_lane < count), both, 0.0),
                axis=1,
                keepdims=True,
            )
            return jnp.sum(weights * vectors, axis=0, keepdims=True)

        ys, zs = basis[...], lifted_basis[0:16, :]
        update[...] += combined(u_minor, zs)
        for at, shape in ((0, p_minor), (steps + 1, r_minor)):
            basis[at : at + 1, :] = combined(shape, ys)
            lifted_basis[at : at + 1, :] = combined(shape, zs)

    residual[...] = basis[steps + 1 : steps + 2, :]


def vmem(*shape):
    return pltpu.VMEM(shape, F32)


def on_device(source_points, target_points, normals, weights, blocks, affines, anchor):
    points = source_points.shape[5]
    dirs = len(OFFSETS)
    in_vmem = pl.BlockSpec(memory_space=pltpu.VMEM)
    sizes = [lax.axis_size(a) for a in AXES]

    tile = jnp.arange(TILES, dtype=jnp.int32)
    x = lax.axis_index("gx")
    y = lax.axis_index("gy") * TY + tile // TZ
    z = lax.axis_index("gz") * TZ + tile % TZ
    spans = (sizes[0], sizes[1] * TY, sizes[2] * TZ)
    keep = ((x * spans[1] + y) * spans[2] + z != anchor[0]).astype(F32)
    keep_row = jnp.pad(jnp.tile(keep, COMPS), (0, LANES - ROWS)).reshape(1, 1, LANES)
    identity = jnp.eye(3, 4, dtype=F32).reshape(COMPS, 1)
    matrix = (affines.reshape(COMPS, TILES) + identity).reshape(-1)
    affine_row = jnp.concatenate(
        [matrix, jnp.full((TILES,), -SPACING, F32), jnp.zeros((LANES - WIDE,), F32)]
    ).reshape(1, 1, LANES)
    offsets = jnp.array(OFFSETS, jnp.int32).T[:, :, None]
    there = [p + o for p, o in zip((x, y, z), offsets)]
    inside = functools.reduce(
        jnp.logical_and, [(p >= 0) & (p < span) for p, span in zip(there, spans)]
    )
    limit = jnp.where(inside, BLOCK * blocks.reshape(dirs, TILES), 0)
    slots = jnp.arange(points, dtype=jnp.int32)
    live = (slots < limit[..., None]).astype(F32)
    weight = weights.reshape(dirs, TILES, points) * live

    moved = jax.ShapeDtypeStruct((3, dirs, TY, TZ, points), F32)
    copies = len(PIECES) + OTHERS
    near, far, affine_there = pl.pallas_call(
        exchange_kernel,
        out_shape=(moved, moved, jax.ShapeDtypeStruct((OTHERS, 1, LANES), F32)),
        in_specs=[in_vmem] * 2,
        out_specs=[in_vmem] * 3,
        scratch_shapes=[pltpu.SemaphoreType.DMA((copies,)), pltpu.SemaphoreType.DMA((copies,))],
        compiler_params=pltpu.CompilerParams(
            collective_id=0, has_side_effects=True, vmem_limit_bytes=60 * 2**20
        ),
        name="exchange",
    )(target_points, affine_row[0])

    pairs, shares, own = pl.pallas_call(
        moments_kernel,
        out_shape=(
            jax.ShapeDtypeStruct((OTHERS + 1, WIDE, LANES), F32),
            jax.ShapeDtypeStruct((OTHERS + 1, 16, LANES), F32),
            jax.ShapeDtypeStruct((ROWS, LANES), F32),
        ),
        in_specs=[in_vmem] * 7,
        out_specs=[in_vmem] * 3,
        scratch_shapes=[
            vmem(13, TILES, points),
            vmem(LANES, points),
            vmem(WIDE, points),
            vmem(LANES, points),
            vmem(ROWS, points),
            vmem(16, LANES),
        ],
        compiler_params=pltpu.CompilerParams(vmem_limit_bytes=60 * 2**20),
        name="moments",
    )(source_points, target_points, near, far, normals, weight, affine_row)

    steps = STEP
    amounts = [2] * (steps - 1) + [1]
    pair_size = sizes[1] * sizes[2]
    update, residual = pl.pallas_call(
        functools.partial(solve_kernel, steps, ITERS // steps),
        out_shape=(jax.ShapeDtypeStruct((1, LANES), F32),) * 2,
        in_specs=[in_vmem] * 6,
        out_specs=[in_vmem] * 2,
        scratch_shapes=[
            vmem(OTHERS, 16, LANES),
            vmem(COMPS, 16, LANES),
            vmem(ROWS, LANES),
            vmem(16, LANES),
            vmem(16, LANES),
            vmem(LANES, LANES),
            vmem(2, pair_size, 1, LANES),
            vmem(2, sizes[0], 1, LANES),
            vmem(2, 1, LANES),
            vmem(2, 1, LANES),
            *[vmem(1, r, LANES) for r in amounts],
            *[vmem(OTHERS, r, LANES) for r in amounts],
            *[vmem(OTHERS, r, LANES) for r in amounts],
            *[vmem(OTHERS, r, LANES) for r in amounts],
            pltpu.SemaphoreType.DMA,
            pltpu.SemaphoreType.DMA,
            pltpu.SemaphoreType.DMA((steps, 4)),
            pltpu.SemaphoreType.DMA((2, 4)),
        ],
        compiler_params=pltpu.CompilerParams(
            collective_id=1, has_side_effects=True, vmem_limit_bytes=60 * 2**20
        ),
        name="solve",
    )(pairs, shares, own, affine_row, affine_there, keep_row)
    shape = affines.shape
    return update[0, :ROWS].reshape(shape), residual[0, :ROWS].reshape(shape)


def solution(mesh):
    placed = (
        P(None, None, "gx", "gy", "gz", None),
        P(None, None, "gx", "gy", "gz", None),
        P(None, None, "gx", "gy", "gz", None),
        P(None, "gx", "gy", "gz", None),
        P(None, "gx", "gy", "gz"),
        P(None, "gx", "gy", "gz"),
        P(),
    )
    return jax.shard_map(
        on_device,
        mesh=mesh,
        in_specs=placed,
        out_specs=(P(None, "gx", "gy", "gz"), P(None, "gx", "gy", "gz")),
        check_vma=False,
    )
```

```python
import functools

import jax
import jax.numpy as jnp
from jax import lax
from jax.experimental import pallas as pl
from jax.experimental.pallas import tpu as pltpu
from jax.sharding import PartitionSpec as P

BLOCK = 256
FIRST, SECOND, AHEAD = 6, 4, 1
SPACING = 0.5
DAMPING = 1.0
OFFSETS = (
    (1, 0, 0),
    (0, 1, 0),
    (0, 0, 1),
    (1, 1, -1),
    (1, -1, 1),
    (-1, 1, 1),
    (1, 1, 0),
    (1, 0, 1),
    (0, 1, 1),
    (1, 1, 1),
    (1, -1, 0),
    (0, 1, -1),
    (-1, 0, 1),
)
AXES = ("gx", "gy", "gz")
MESH = pl.DeviceIdType.MESH
LANES = 128
TY, TZ, TILES = 4, 2, 8
COMPS = 12
ROWS = COMPS * TILES
WIDE = ROWS + TILES
F32 = jnp.float32


def shifts(offset):
    seconds = (0,) if offset[1] == 0 else (0, offset[1])
    thirds = (0,) if offset[2] == 0 else (0, offset[2])
    return [(offset[0], y, z) for y in seconds for z in thirds]


SELF = (0, 0, 0)
REACH = (
    SELF,
    *sorted(
        {s for o in OFFSETS for s in shifts(o)} - {SELF}, key=lambda s: (-sum(map(abs, s)), s)
    ),
)
OTHERS = len(REACH) - 1
GREET = tuple(sorted({s for s in REACH[1:]} | {tuple(-p for p in s) for s in REACH[1:]}))


def pieces():
    found = []
    for index, offset in enumerate(OFFSETS):
        for shift in shifts(offset):
            if shift == SELF:
                continue
            if offset[1] == 0:
                low, count = 0, TY
            elif shift[1] == 0:
                low, count = (1 if offset[1] > 0 else 0), TY - 1
            else:
                low, count = (0 if offset[1] > 0 else TY - 1), 1
            found.append((index, shift, low, count, 0 if shift[2] == 0 else 1))
    return tuple(found)


PIECES = pieces()


def device_at(shift, sign):
    there = []
    for axis, part in zip(AXES, shift):
        size = lax.axis_size(axis)
        there.append(lax.rem(lax.axis_index(axis) + (sign * part + size), size))
    return tuple(there)


def remote(source, target, sent, got, device):
    return pltpu.make_async_remote_copy(
        src_ref=source,
        dst_ref=target,
        send_sem=sent,
        recv_sem=got,
        device_id=device,
        device_id_type=MESH,
    )


def exchange_kernel(target, affine, near, far, affine_there, sent, got):
    barrier = pltpu.get_barrier_semaphore()
    for shift in GREET:
        pl.semaphore_signal(barrier, inc=1, device_id=device_at(shift, 1), device_id_type=MESH)
    pl.semaphore_wait(barrier, len(GREET))
    copies = []
    for number, (index, shift, low, count, which) in enumerate(PIECES):
        span = pl.ds(low, count)
        place = (near, far)[which]
        copies.append(
            remote(
                target.at[:, index, 0, span],
                place.at[:, index, span],
                sent.at[number],
                got.at[number],
                device_at(shift, -1),
            )
        )
    for number, shift in enumerate(REACH[1:]):
        at = len(PIECES) + number
        copies.append(
            remote(affine, affine_there.at[number], sent.at[at], got.at[at], device_at(shift, -1))
        )
    for copy in copies:
        copy.start()
    for copy in copies:
        copy.wait()


def iotas(rows=TILES):
    return (
        lax.broadcasted_iota(jnp.int32, (rows, LANES), 0),
        lax.broadcasted_iota(jnp.int32, (rows, LANES), 1),
    )


def tiled(mask, times):
    return jnp.concatenate([mask] * times, axis=0)


def cross(left, right):
    return lax.dot_general(
        left,
        right,
        (((1,), (1,)), ((), ())),
        precision=lax.Precision.HIGHEST,
        preferred_element_type=F32,
    )


def moments_kernel(
    source,
    target,
    near,
    far,
    normal,
    weight,
    affine,
    blocks,
    shares,
    own,
    slab,
    here,
    here_weighted,
    there,
    there_weighted,
    packed,
):
    sub, lane = iotas()
    slot = lane & (TILES - 1)
    blocks[...] = jnp.zeros_like(blocks)
    shares[...] = jnp.zeros_like(shares)
    own[...] = jnp.zeros_like(own)
    packed[...] = jnp.zeros_like(packed)
    here[WIDE:, :] = jnp.zeros((LANES - WIDE, here.shape[1]), F32)
    there[ROWS:, :] = jnp.zeros((LANES - ROWS, there.shape[1]), F32)
    same = sub == slot
    for index, offset in enumerate(OFFSETS):
        for y in range(TY):
            for c in range(3):
                slab[c, 2 * y : 2 * y + 2, :] = source[c, index, 0, y]
                slab[3 + c, 2 * y : 2 * y + 2, :] = normal[c, index, 0, y]
        for y in range(TY):
            before = (y - offset[1]) % TY
            shift_y = (y - offset[1]) // TY
            for z in range(TZ):
                back = (z - offset[2]) % TZ
                shift_z = (z - offset[2]) // TZ
                shift = (offset[0], -shift_y, -shift_z)
                to, come = y * TZ + z, before * TZ + back
                for c in range(3):
                    slab[6 + c, to : to + 1, :] = normal[c, index, 0, before, back : back + 1, :]
                    if shift == SELF:
                        row = target[c, index, 0, y, z : z + 1, :]
                    elif shift[2] == 0:
                        row = near[c, index, y, z : z + 1, :]
                    else:
                        row = far[c, index, y, z : z + 1, :]
                    slab[9 + c, to : to + 1, :] = row
                slab[12, to : to + 1, :] = weight[index, come : come + 1, :]
        share, share_there = weight[index], slab[12]
        for c in range(3):
            n, m = slab[3 + c], slab[6 + c]
            for e in range(4):
                at = (4 * c + e) * TILES
                a = n * slab[e] if e < 3 else n
                b = -(m * slab[9 + e]) if e < 3 else -m
                here[at : at + TILES, :] = a
                here_weighted[at : at + TILES, :] = a * share
                there[at : at + TILES, :] = b
                there_weighted[at : at + TILES, :] = b * share_there
        along = sum(part * slab[3 + c] for c, part in enumerate(offset) if part != 0)
        here[ROWS:WIDE, :] = along
        here_weighted[ROWS:WIDE, :] = along * share
        own[...] += cross(here_weighted[:ROWS, :], here[...])
        pair = cross(here_weighted[...], there[...])
        back = cross(there_weighted[...], there[...])
        for a in range(COMPS):
            at = a * TILES
            packed[a : a + 1, :] = jnp.sum(
                jnp.where(same, back[at : at + TILES, :], 0.0), axis=0, keepdims=True
            )
        second, third = sub // TZ + offset[1], sub % TZ + offset[2]
        slot_y, slot_z = slot // TZ, slot % TZ
        all_slots = packed[...]
        for shift in shifts(offset):
            j = REACH.index(shift)
            meets = (slot_y + TY * shift[1] == second) & (slot_z + TZ * shift[2] == third)
            blocks[j] += jnp.where(tiled(meets, WIDE // TILES), pair, 0.0)
            owned = jnp.ones((TILES, LANES), jnp.bool_)
            from_y, from_z = slot_y - offset[1] + TY * shift[1], slot_z - offset[2] + TZ * shift[2]
            owned = (from_y >= 0) & (from_y < TY) & (from_z >= 0) & (from_z < TZ)
            shares[j] += jnp.where(tiled(owned, 2), all_slots, 0.0)
    own[...] = jnp.where(tiled(same, COMPS), own[...], 0.0)
    row = affine[0]
    columns = [
        jnp.sum(jnp.where(lane == sub + a * TILES, row, 0.0), axis=1, keepdims=True)
        for a in range(COMPS + 1)
    ]
    for j in range(OTHERS + 1):
        total = jnp.zeros((TILES, LANES), F32)
        for a in range(COMPS + 1):
            total = total + blocks[j, a * TILES : (a + 1) * TILES, :] * columns[a]
        shares[j, COMPS : COMPS + 1, :] = jnp.sum(total, axis=0, keepdims=True)


def split(x):
    big = x * 4097.0
    high = big - (big - x)
    return high, x - high


def exact_product(x, y):
    (xh, xl), (yh, yl) = split(x), split(y)
    product = x * y
    return product, ((xh * yh - product) + xh * yl + xl * yh) + xl * yl


def lane_total(values, small, bound):
    grid = bound * 256.0
    top = (values + grid) - grid
    rest = values - top
    grid = grid * 2.0**-16
    middle = (rest + grid) - grid
    small = small + (rest - middle)
    top, middle, small = (jnp.sum(v, axis=1, keepdims=True) for v in (top, middle, small))
    high = top + middle
    back = high - top
    return high, ((top - (high - back)) + (middle - back)) + small


def compensated(parts):
    total, error = parts[0], jnp.zeros_like(parts[0])
    for part in parts[1:]:
        following = total + part
        back = following - total
        error = error + ((total - (following - back)) + (part - back))
        total = following
    high, low = total[0:1], error[0:1] + total[1:2]
    both = high + low
    return both, low - (both - high)


def solve_kernel(plan, *refs):
    first_steps, second_steps, ahead, amounts = plan
    steps = len(amounts)
    blocks, shares, own, affine, affine_there, keep = refs[:6]
    update, residual = refs[6:8]
    shares_there, matrix, inverse, chain, chain_lifted, basis, lifted = refs[8:15]
    pair_sum, line_sum, pair_send, line_send = refs[15:19]
    rest = refs[19:]
    send_rows, got_rows, back_rows, got_back = (rest[k * steps : (k + 1) * steps] for k in range(4))
    share_sent, share_got, halo_sems, sum_sems = rest[4 * steps :]
    first, second, third = (lax.axis_index(a) for a in AXES)
    size_first, size_second, size_third = (lax.axis_size(a) for a in AXES)
    in_pair = second * size_third + third
    pair_size = size_second * size_third

    def pair_peer(k):
        there = lax.rem(in_pair + k, pair_size)
        return (first, there // size_third, lax.rem(there, size_third))

    def line_peer(k):
        return (lax.rem(first + k, size_first), second, third)

    barrier = pltpu.get_barrier_semaphore()
    for shift in GREET:
        pl.semaphore_signal(barrier, inc=1, device_id=device_at(shift, 1), device_id_type=MESH)

    @pl.loop(1, pair_size)
    def _(k):
        pl.semaphore_signal(barrier, inc=1, device_id=pair_peer(k), device_id_type=MESH)

    @pl.loop(1, size_first)
    def _(k):
        pl.semaphore_signal(barrier, inc=1, device_id=line_peer(k), device_id_type=MESH)

    pl.semaphore_wait(barrier, len(GREET) + pair_size - 1 + size_first - 1)

    for number, shift in enumerate(REACH[1:]):
        remote(
            shares.at[number + 1],
            shares_there.at[number],
            share_sent,
            share_got,
            device_at(shift, 1),
        ).start()

    sub, lane = iotas()
    slot = lane & (TILES - 1)
    same = sub == slot
    eyes = [lane == sub + a * TILES for a in range(COMPS)]
    wide_sub, wide_lane = iotas(16)

    def column(row):
        return [jnp.sum(jnp.where(eyes[a], row, 0.0), axis=1, keepdims=True) for a in range(COMPS)]

    def group(a):
        return slice(a * TILES, (a + 1) * TILES)

    keep_row = keep[0]
    keep_column = column(keep_row)
    row = affine[0]
    sums = []
    for a in range(COMPS):
        total = own[group(a), :] * row + blocks[0, group(a), :] * row
        for j in range(OTHERS):
            total = total + blocks[j + 1, group(a), :] * affine_there[j]
        sums.append(total)
    everything = pltpu.make_async_copy(shares_there, shares_there, share_got)
    everything.wait()
    pltpu.make_async_copy(shares_there, shares_there, share_sent).wait()
    gathered = shares[0]
    for j in range(OTHERS):
        gathered = gathered + shares_there[j]
    right = []
    for a in range(COMPS):
        spread = jnp.where(same & (lane < ROWS), gathered[a : a + 1, :], 0.0)
        total = sums[a] + spread * row + jnp.where(eyes[a], gathered[COMPS : COMPS + 1, :], 0.0)
        right.append(-keep_column[a] * jnp.sum(total, axis=1, keepdims=True))
        mine = jnp.where(lane < ROWS, own[group(a), :], 0.0)
        compact = jnp.sum(mine, axis=0, keepdims=True) + gathered[a : a + 1, :]
        unit = jnp.where((lane[:1] >= a * TILES) & (lane[:1] < (a + 1) * TILES), 1.0, 0.0)
        compact = keep_row * (compact + DAMPING * unit) + (1.0 - keep_row) * unit
        picked = jnp.where(wide_lane // TILES == wide_sub, compact, 0.0)
        for by in (8, 16, 32, 64):
            picked = picked + pltpu.roll(picked, by, 1)
        matrix[a] = picked

    rows = [matrix[a] for a in range(COMPS)]
    for k in range(COMPS):
        factor = 1.0 / rows[k][k : k + 1, :]
        at_pivot = wide_sub == k
        pivot_row = jnp.where(at_pivot, factor, rows[k] * factor)
        for i in range(COMPS):
            if i != k:
                f = rows[i][k : k + 1, :]
                rows[i] = jnp.where(at_pivot, 0.0, rows[i]) - f * pivot_row
        rows[k] = pivot_row
    for a in range(COMPS):
        compact = jnp.sum(
            jnp.where(wide_lane // TILES == wide_sub, rows[a], 0.0), axis=0, keepdims=True
        )
        inverse[group(a), :] = jnp.where(same & (lane < ROWS), compact, 0.0)

    def as_row(col):
        total = jnp.zeros((TILES, LANES), F32)
        for a in range(COMPS):
            total = total + jnp.where(eyes[a], col[a], 0.0)
        return jnp.sum(total, axis=0, keepdims=True)

    def precondition(col):
        total = jnp.zeros((TILES, LANES), F32)
        for a in range(COMPS):
            total = total + inverse[group(a), :] * col[a]
        return jnp.sum(total, axis=0, keepdims=True)

    def couple(step, vectors, meanwhile=None):
        amount = len(vectors)
        cols = [column(v) for v in vectors]
        for r, v in enumerate(vectors):
            send_rows[step][0, r : r + 1, :] = v
        for number, shift in enumerate(REACH[1:]):
            remote(
                send_rows[step].at[0],
                got_rows[step].at[number],
                halo_sems.at[step, 0],
                halo_sems.at[step, 1],
                device_at(shift, -1),
            ).start()
        local = []
        for j in range(OTHERS + 1):
            totals = [jnp.zeros((TILES, LANES), F32) for _ in vectors]
            for a in range(COMPS):
                block = blocks[j, group(a), :]
                for r in range(amount):
                    totals[r] = totals[r] + block * cols[r][a]
            for r in range(amount):
                total = jnp.sum(totals[r], axis=0, keepdims=True)
                if j == 0:
                    local.append(total)
                else:
                    back_rows[step][j - 1, r : r + 1, :] = total
            if j > 0:
                remote(
                    back_rows[step].at[j - 1],
                    got_back[step].at[j - 1],
                    halo_sems.at[step, 2],
                    halo_sems.at[step, 3],
                    device_at(REACH[j], 1),
                ).start()
        if meanwhile is not None:
            meanwhile()
        sums = [[blocks[0, group(a), :] * v for a in range(COMPS)] for v in vectors]
        rows_there, back_there = got_rows[step], got_back[step]
        pltpu.make_async_copy(rows_there, rows_there, halo_sems.at[step, 1]).wait()
        for j in range(OTHERS):
            for r in range(amount):
                v = rows_there[j, r : r + 1, :]
                for a in range(COMPS):
                    sums[r][a] = sums[r][a] + blocks[j + 1, group(a), :] * v
        pltpu.make_async_copy(back_there, back_there, halo_sems.at[step, 3]).wait()
        results = []
        for r in range(amount):
            came = local[r]
            for j in range(OTHERS):
                came = came + back_there[j, r : r + 1, :]
            results.append(
                [
                    keep_column[a]
                    * jnp.sum(sums[r][a] + jnp.where(eyes[a], came, 0.0), axis=1, keepdims=True)
                    for a in range(COMPS)
                ]
            )
        pltpu.make_async_copy(rows_there, rows_there, halo_sems.at[step, 0]).wait()
        pltpu.make_async_copy(back_there, back_there, halo_sems.at[step, 2]).wait()
        return results

    def pair_part(at):
        return pair_sum.at[at, pl.ds(0, pair_size - 1)]

    def line_part(at):
        return line_sum.at[at, pl.ds(0, size_first - 1)]

    def wait_for(part, sem):
        pltpu.make_async_copy(part, part, sem).wait()

    def start_sum(high, low, at):
        for row, value in ((0, high), (1, low)):
            pair_send[at, row : row + 1, :] = value
            pair_sum[at, in_pair, row : row + 1, :] = value

        @pl.loop(1, pair_size)
        def _(k):
            remote(
                pair_send.at[at],
                pair_sum.at[at, in_pair],
                sum_sems.at[at, 0],
                sum_sems.at[at, 1],
                pair_peer(k),
            ).start()

    def go_on_sum(at):
        wait_for(pair_part(at), sum_sems.at[at, 1])
        high, low = compensated([pair_sum[at, k] for k in range(pair_size)])
        for row, value in ((0, high), (1, low)):
            line_send[at, row : row + 1, :] = value
            line_sum[at, first, row : row + 1, :] = value

        @pl.loop(1, size_first)
        def _(k):
            remote(
                line_send.at[at],
                line_sum.at[at, first],
                sum_sems.at[at, 2],
                sum_sems.at[at, 3],
                line_peer(k),
            ).start()

    def end_sum(at):
        wait_for(line_part(at), sum_sems.at[at, 3])
        high, low = compensated([line_sum[at, k] for k in range(size_first)])
        wait_for(pair_part(at), sum_sems.at[at, 0])
        wait_for(line_part(at), sum_sems.at[at, 2])
        return tuple(jnp.broadcast_to(v, (TILES, LANES)) for v in (high, low))

    def largest(values):
        return jnp.max(jnp.abs(values), axis=1, keepdims=True)

    def gram(count, ys, zs):
        y_bound, z_bound = largest(ys), largest(zs)
        row_of, lane_of = iotas(ys.shape[0])
        high = low = jnp.zeros(ys.shape, F32)
        for j in range(count):
            at = (lane_of == row_of * count + j) & (row_of < count)
            product, error = exact_product(ys, zs[j : j + 1, :])
            h, l = lane_total(product, error, y_bound * z_bound[j : j + 1, :])
            high, low = jnp.where(at, h, high), jnp.where(at, l, low)
        return tuple(jnp.sum(v, axis=0, keepdims=True) for v in (high, low))

    def iterate(count, amount, at_p, at_r, high, low):
        major = jnp.zeros((TILES, LANES), jnp.int32)
        for k in range(1, count + 1):
            major = major + jnp.where(lane >= k * count, 1, 0)
        minor = lane - count * major

        def form(mask):
            return jnp.where(mask & (lane < count * count), 1.0, 0.0)

        g_bound = largest(high)

        def inner(x, y, bound):
            product, error = exact_product(x, y)
            values, small = exact_product(product, high)
            total = lane_total(values, small + (product * low + error * high), g_bound * bound)
            return total[0] + total[1]

        p_major, p_minor = form(major == at_p), form(minor == at_p)
        r_major, r_minor = form(major == at_r), form(minor == at_r)
        u_minor = jnp.zeros((TILES, LANES), F32)
        p_most = r_most = jnp.ones((TILES, 1), F32)
        product = inner(r_major, r_minor, r_most)
        for _ in range(amount):
            a_major = p_major + pltpu.roll(p_major, count, 1)
            a_minor = p_minor + pltpu.roll(p_minor, 1, 1)
            a_most = 2.0 * p_most
            alpha = product / inner(p_major, a_minor, p_most * a_most)
            u_minor = u_minor + alpha * p_minor
            r_major = r_major - alpha * a_major
            r_minor = r_minor - alpha * a_minor
            r_most = (r_most + jnp.abs(alpha) * a_most) * 1.01
            following = inner(r_major, r_minor, r_most * r_most)
            ratio = following / product
            p_major = r_major + ratio * p_major
            p_minor = r_minor + ratio * p_minor
            p_most = (r_most + jnp.abs(ratio) * p_most) * 1.01
            product = following
        return u_minor, r_minor, p_minor

    def combined(count, minor_form, vectors, by=0):
        both = jnp.concatenate([minor_form, minor_form], axis=0)
        weights = jnp.sum(
            jnp.where((wide_lane + by == wide_sub) & (wide_lane < count), both, 0.0),
            axis=1,
            keepdims=True,
        )
        return jnp.sum(weights * vectors, axis=0, keepdims=True)

    for ref in (chain, chain_lifted, basis, lifted):
        ref[...] = jnp.zeros_like(ref)
    chain[0:1, :] = as_row(right)
    chain_lifted[0:1, :] = precondition(right)

    def extend(step, places, ys, zs, meanwhile=None):
        found = couple(step, [zs[at : at + 1, :] for at in places], meanwhile)
        for at, col in zip(places, found):
            ys[at + 1 : at + 2, :] = as_row(col)
            zs[at + 1 : at + 2, :] = precondition(col)

    for step in range(first_steps):
        extend(step, [step], chain, chain_lifted)
    count = first_steps + 1
    start_sum(*gram(count, chain[0:8, :], chain_lifted[0:8, :]), 0)
    for step in range(first_steps, first_steps + ahead):
        extend(
            step,
            [step],
            chain,
            chain_lifted,
            functools.partial(go_on_sum, 0) if step == first_steps else None,
        )
    u_form, r_form, p_form = iterate(count, first_steps, 0, 0, *end_sum(0))
    ys, zs = chain[...], chain_lifted[...]
    part = combined(count, u_form, zs)
    at_r = second_steps + 1
    for begin, shape in ((0, p_form), (at_r, r_form)):
        for by in range(ahead + 1):
            at = begin + by
            basis[at : at + 1, :] = combined(count, shape, ys, by)
            lifted[at : at + 1, :] = combined(count, shape, zs, by)
    for step in range(first_steps + ahead, steps):
        degree = step - first_steps
        extend(step, [degree, at_r + degree][: amounts[step]], basis, lifted)
    count = 2 * second_steps + 1
    start_sum(*gram(count, basis[...], lifted[...]), 1)
    go_on_sum(1)
    u_form, r_form, _ = iterate(count, second_steps, 0, at_r, *end_sum(1))
    update[...] = part + combined(count, u_form, lifted[...])
    residual[...] = combined(count, r_form, basis[...])


def vmem(*shape):
    return pltpu.VMEM(shape, F32)


def on_device(source_points, target_points, normals, weights, blocks, affines, anchor):
    points = source_points.shape[5]
    dirs = len(OFFSETS)
    in_vmem = pl.BlockSpec(memory_space=pltpu.VMEM)
    sizes = [lax.axis_size(a) for a in AXES]

    tile = jnp.arange(TILES, dtype=jnp.int32)
    x = lax.axis_index("gx")
    y = lax.axis_index("gy") * TY + tile // TZ
    z = lax.axis_index("gz") * TZ + tile % TZ
    spans = (sizes[0], sizes[1] * TY, sizes[2] * TZ)
    keep = ((x * spans[1] + y) * spans[2] + z != anchor[0]).astype(F32)
    keep_row = jnp.pad(jnp.tile(keep, COMPS), (0, LANES - ROWS)).reshape(1, 1, LANES)
    identity = jnp.eye(3, 4, dtype=F32).reshape(COMPS, 1)
    matrix = (affines.reshape(COMPS, TILES) + identity).reshape(-1)
    affine_row = jnp.concatenate(
        [matrix, jnp.full((TILES,), -SPACING, F32), jnp.zeros((LANES - WIDE,), F32)]
    ).reshape(1, 1, LANES)
    offsets = jnp.array(OFFSETS, jnp.int32).T[:, :, None]
    there = [p + o for p, o in zip((x, y, z), offsets)]
    inside = functools.reduce(
        jnp.logical_and, [(p >= 0) & (p < span) for p, span in zip(there, spans)]
    )
    limit = jnp.where(inside, BLOCK * blocks.reshape(dirs, TILES), 0)
    slots = jnp.arange(points, dtype=jnp.int32)
    live = (slots < limit[..., None]).astype(F32)
    weight = weights.reshape(dirs, TILES, points) * live

    moved = jax.ShapeDtypeStruct((3, dirs, TY, TZ, points), F32)
    copies = len(PIECES) + OTHERS
    near, far, affine_there = pl.pallas_call(
        exchange_kernel,
        out_shape=(moved, moved, jax.ShapeDtypeStruct((OTHERS, 1, LANES), F32)),
        in_specs=[in_vmem] * 2,
        out_specs=[in_vmem] * 3,
        scratch_shapes=[pltpu.SemaphoreType.DMA((copies,)), pltpu.SemaphoreType.DMA((copies,))],
        compiler_params=pltpu.CompilerParams(
            collective_id=0, has_side_effects=True, vmem_limit_bytes=60 * 2**20
        ),
        name="exchange",
    )(target_points, affine_row[0])

    pairs, shares, own = pl.pallas_call(
        moments_kernel,
        out_shape=(
            jax.ShapeDtypeStruct((OTHERS + 1, WIDE, LANES), F32),
            jax.ShapeDtypeStruct((OTHERS + 1, 16, LANES), F32),
            jax.ShapeDtypeStruct((ROWS, LANES), F32),
        ),
        in_specs=[in_vmem] * 7,
        out_specs=[in_vmem] * 3,
        scratch_shapes=[
            vmem(13, TILES, points),
            vmem(LANES, points),
            vmem(WIDE, points),
            vmem(LANES, points),
            vmem(ROWS, points),
            vmem(16, LANES),
        ],
        compiler_params=pltpu.CompilerParams(vmem_limit_bytes=60 * 2**20),
        name="moments",
    )(source_points, target_points, near, far, normals, weight, affine_row)

    later = SECOND - AHEAD
    amounts = (1,) * (FIRST + AHEAD) + (2,) * (later - 1) + (1,)
    steps = len(amounts)
    pair_size = sizes[1] * sizes[2]
    update, residual = pl.pallas_call(
        functools.partial(solve_kernel, (FIRST, SECOND, AHEAD, amounts)),
        out_shape=(jax.ShapeDtypeStruct((1, LANES), F32),) * 2,
        in_specs=[in_vmem] * 6,
        out_specs=[in_vmem] * 2,
        scratch_shapes=[
            vmem(OTHERS, 16, LANES),
            vmem(COMPS, 16, LANES),
            vmem(ROWS, LANES),
            *[vmem(16, LANES)] * 4,
            vmem(2, pair_size, 2, LANES),
            vmem(2, sizes[0], 2, LANES),
            vmem(2, 2, LANES),
            vmem(2, 2, LANES),
            *[vmem(1, r, LANES) for r in amounts],
            *[vmem(OTHERS, r, LANES) for r in amounts],
            *[vmem(OTHERS, r, LANES) for r in amounts],
            *[vmem(OTHERS, r, LANES) for r in amounts],
            pltpu.SemaphoreType.DMA,
            pltpu.SemaphoreType.DMA,
            pltpu.SemaphoreType.DMA((steps, 4)),
            pltpu.SemaphoreType.DMA((2, 4)),
        ],
        compiler_params=pltpu.CompilerParams(
            collective_id=1, has_side_effects=True, vmem_limit_bytes=60 * 2**20
        ),
        name="solve",
    )(pairs, shares, own, affine_row, affine_there, keep_row)
    shape = affines.shape
    return update[0, :ROWS].reshape(shape), residual[0, :ROWS].reshape(shape)


def solution(mesh):
    placed = (
        P(None, None, "gx", "gy", "gz", None),
        P(None, None, "gx", "gy", "gz", None),
        P(None, None, "gx", "gy", "gz", None),
        P(None, "gx", "gy", "gz", None),
        P(None, "gx", "gy", "gz"),
        P(None, "gx", "gy", "gz"),
        P(),
    )
    return jax.shard_map(
        on_device,
        mesh=mesh,
        in_specs=placed,
        out_specs=(P(None, "gx", "gy", "gz"), P(None, "gx", "gy", "gz")),
        check_vma=False,
    )
```

```python
import functools

import jax
import jax.numpy as jnp
from jax import lax
from jax.experimental import pallas as pl
from jax.experimental.pallas import tpu as pltpu
from jax.sharding import PartitionSpec as P

BLOCK = 256
FIRST, SECOND, AHEAD = 6, 4, 1
SPACING = 0.5
DAMPING = 1.0
OFFSETS = (
    (1, 0, 0),
    (0, 1, 0),
    (0, 0, 1),
    (1, 1, -1),
    (1, -1, 1),
    (-1, 1, 1),
    (1, 1, 0),
    (1, 0, 1),
    (0, 1, 1),
    (1, 1, 1),
    (1, -1, 0),
    (0, 1, -1),
    (-1, 0, 1),
)
AXES = ("gx", "gy", "gz")
MESH = pl.DeviceIdType.MESH
LANES = 128
TY, TZ, TILES = 4, 2, 8
COMPS = 12
ROWS = COMPS * TILES
WIDE = ROWS + TILES
F32 = jnp.float32


def shifts(offset):
    seconds = (0,) if offset[1] == 0 else (0, offset[1])
    thirds = (0,) if offset[2] == 0 else (0, offset[2])
    return [(offset[0], y, z) for y in seconds for z in thirds]


SELF = (0, 0, 0)
REACH = (
    SELF,
    *sorted(
        {s for o in OFFSETS for s in shifts(o)} - {SELF}, key=lambda s: (-sum(map(abs, s)), s)
    ),
)
OTHERS = len(REACH) - 1
GREET = tuple(sorted({s for s in REACH[1:]} | {tuple(-p for p in s) for s in REACH[1:]}))


def spans(part, shift, length):
    if part == 0:
        return 0, length
    if shift == 0:
        return (1 if part > 0 else 0), length - 1
    return (0 if part > 0 else length - 1), 1


ORDER = tuple(sorted(range(len(OFFSETS)), key=lambda d: ((0, 2, 1)[OFFSETS[d][0]], d)))
PIECES = tuple(
    (d, s, *spans(OFFSETS[d][1], s[1], TY), *spans(OFFSETS[d][2], s[2], TZ))
    for d in ORDER
    for s in shifts(OFFSETS[d])
    if s != SELF
)


def device_at(shift, sign):
    there = []
    for axis, part in zip(AXES, shift):
        size = lax.axis_size(axis)
        there.append(lax.rem(lax.axis_index(axis) + (sign * part + size), size))
    return tuple(there)


def remote(source, target, sent, got, device):
    return pltpu.make_async_remote_copy(
        src_ref=source,
        dst_ref=target,
        send_sem=sent,
        recv_sem=got,
        device_id=device,
        device_id_type=MESH,
    )


def iotas(rows=TILES):
    return (
        lax.broadcasted_iota(jnp.int32, (rows, LANES), 0),
        lax.broadcasted_iota(jnp.int32, (rows, LANES), 1),
    )


def tiled(mask, times):
    return jnp.concatenate([mask] * times, axis=0)


def cross(left, right):
    return lax.dot_general(
        left,
        right,
        (((1,), (1,)), ((), ())),
        precision=lax.Precision.HIGHEST,
        preferred_element_type=F32,
    )


def split(x):
    big = x * 4097.0
    high = big - (big - x)
    return high, x - high


def exact_product(x, y):
    (xh, xl), (yh, yl) = split(x), split(y)
    product = x * y
    return product, ((xh * yh - product) + xh * yl + xl * yh) + xl * yl


def lane_total(values, small, bound):
    grid = bound * 256.0
    top = (values + grid) - grid
    rest = values - top
    grid = grid * 2.0**-16
    middle = (rest + grid) - grid
    small = small + (rest - middle)
    top, middle, small = (jnp.sum(v, axis=1, keepdims=True) for v in (top, middle, small))
    high = top + middle
    back = high - top
    return high, ((top - (high - back)) + (middle - back)) + small


def compensated(parts):
    total, error = parts[0], jnp.zeros_like(parts[0])
    for part in parts[1:]:
        following = total + part
        back = following - total
        error = error + ((total - (following - back)) + (part - back))
        total = following
    high, low = total[0:1], error[0:1] + total[1:2]
    both = high + low
    return both, low - (both - high)


def step_kernel(plan, *refs):
    first_steps, second_steps, ahead, amounts = plan
    steps = len(amounts)
    source_out, target_out, normal_out, weight_out, counts, affines, anchor = refs[:7]
    update, residual = refs[7:9]
    source, target, normal, weight, moved, affine, affine_there = refs[9:16]
    slab, here, here_weighted, there, there_weighted, packed, small = refs[16:23]
    small_count, masked, blocks, shares, own = refs[23:28]
    shares_there, matrix, inverse, chain, chain_lifted, basis, lifted = refs[28:35]
    pair_sum, line_sum, pair_send, line_send = refs[35:39]
    rest = refs[39:]
    send_rows, got_rows, back_rows, got_back = (rest[k * steps : (k + 1) * steps] for k in range(4))
    loaded, sent, got, share_sent, share_got, halo_sems, sum_sems = rest[4 * steps :]
    loads = [
        pltpu.make_async_copy(outer, ref, loaded.at[number])
        for number, (outer, ref) in enumerate(
            (
                (target_out, target),
                (source_out, source),
                (normal_out, normal),
                (weight_out, weight),
            )
        )
    ]
    for load in loads:
        load.start()
    first, second, third = (lax.axis_index(a) for a in AXES)
    size_first, size_second, size_third = (lax.axis_size(a) for a in AXES)
    in_pair = second * size_third + third
    pair_size = size_second * size_third

    def pair_peer(k):
        there = lax.rem(in_pair + k, pair_size)
        return (first, there // size_third, lax.rem(there, size_third))

    def line_peer(k):
        return (lax.rem(first + k, size_first), second, third)

    barrier = pltpu.get_barrier_semaphore()
    for shift in GREET:
        pl.semaphore_signal(barrier, inc=1, device_id=device_at(shift, 1), device_id_type=MESH)

    @pl.loop(1, pair_size)
    def _(k):
        pl.semaphore_signal(barrier, inc=1, device_id=pair_peer(k), device_id_type=MESH)

    @pl.loop(1, size_first)
    def _(k):
        pl.semaphore_signal(barrier, inc=1, device_id=line_peer(k), device_id_type=MESH)

    sub, lane = iotas()
    slot = lane & (TILES - 1)
    same = sub == slot
    eyes = [lane == sub + a * TILES for a in range(COMPS)]
    wide_sub, wide_lane = iotas(16)

    def column(row):
        return [jnp.sum(jnp.where(eyes[a], row, 0.0), axis=1, keepdims=True) for a in range(COMPS)]

    def group(a):
        return slice(a * TILES, (a + 1) * TILES)

    def positions(tile):
        return (first, second * TY + tile // TZ, third * TZ + tile % TZ)

    extents = (size_first, size_second * TY, size_third * TZ)

    def kept(tile):
        x, y, z = positions(tile)
        return jnp.where((x * extents[1] + y) * extents[2] + z != anchor[0], 1.0, 0.0)

    for y in range(TY):
        small[2 * y : 2 * y + 2, 0:COMPS] = affines[0, y]
    affine_columns = [
        small[:, a : a + 1] + (1.0 if a % 5 == 0 else 0.0) for a in range(COMPS)
    ]
    row = jnp.zeros((TILES, LANES), F32)
    for a in range(COMPS):
        row = row + jnp.where(eyes[a], affine_columns[a], 0.0)
    row = jnp.sum(row, axis=0, keepdims=True)
    row = jnp.where((lane[:1] >= ROWS) & (lane[:1] < WIDE), -SPACING, row)
    affine[...] = row

    pl.semaphore_wait(barrier, len(GREET) + pair_size - 1 + size_first - 1)
    loads[0].wait()
    copies = {}
    for number, (index, shift, low, count, low_z, count_z) in enumerate(PIECES):
        at = (slice(None), index, pl.ds(low, count), pl.ds(low_z, count_z))
        copy = remote(
            target.at[(slice(None), index, 0, *at[2:])],
            moved.at[at],
            sent.at[number],
            got.at[number],
            device_at(shift, -1),
        )
        copy.start()
        copies.setdefault(index, []).append(copy)
    affine_copies = []
    for number, shift in enumerate(REACH[1:]):
        at = len(PIECES) + number
        affine_copies.append(
            remote(affine, affine_there.at[number], sent.at[at], got.at[at], device_at(shift, -1))
        )
        affine_copies[-1].start()

    for ref in (blocks, shares, own, packed):
        ref[...] = jnp.zeros_like(ref)
    points = here.shape[1]
    here[WIDE:, :] = jnp.zeros((LANES - WIDE, points), F32)
    there[ROWS:, :] = jnp.zeros((LANES - ROWS, points), F32)
    numbers = lax.broadcasted_iota(jnp.int32, (TILES, points), 1)
    tile_column = sub[:, 0:1]
    for load in loads[1:]:
        load.wait()
    for index in ORDER:
        offset = OFFSETS[index]
        for y in range(TY):
            for c in range(3):
                slab[c, 2 * y : 2 * y + 2, :] = source[c, index, 0, y]
                slab[3 + c, 2 * y : 2 * y + 2, :] = normal[c, index, 0, y]
            slab[6, 2 * y : 2 * y + 2, :] = weight[index, 0, y]
            small_count[2 * y : 2 * y + 2, :] = counts[0, y, :, index : index + 1]
        inside = functools.reduce(
            jnp.logical_and,
            [
                (p + o >= 0) & (p + o < extent)
                for p, o, extent in zip(positions(tile_column), offset, extents)
            ],
        )
        limit = jnp.where(inside, BLOCK * small_count[...], 0)
        share = jnp.where(numbers < limit, slab[6], 0.0)
        masked[index] = share
        for c in range(3):
            n = slab[3 + c]
            for e in range(4):
                at = (4 * c + e) * TILES
                a = n * slab[e] if e < 3 else n
                here[at : at + TILES, :] = a
                here_weighted[index, at : at + TILES, :] = a * share
        along = sum(part * slab[3 + c] for c, part in enumerate(offset) if part != 0)
        here[ROWS:WIDE, :] = along
        here_weighted[index, ROWS:WIDE, :] = along * share
        own[...] += cross(here_weighted[index, :ROWS, :], here[...])
    own[...] = jnp.where(tiled(same, COMPS), own[...], 0.0)

    for index in ORDER:
        offset = OFFSETS[index]
        for copy in copies.get(index, ()):
            copy.wait()
        for y in range(TY):
            before = (y - offset[1]) % TY
            shift_y = (y - offset[1]) // TY
            for z in range(TZ):
                back = (z - offset[2]) % TZ
                shift_z = (z - offset[2]) // TZ
                to, come = y * TZ + z, before * TZ + back
                local = (offset[0], -shift_y, -shift_z) == SELF
                for c in range(3):
                    slab[6 + c, to : to + 1, :] = normal[c, index, 0, before, back : back + 1, :]
                    if local:
                        slab[9 + c, to : to + 1, :] = target[c, index, 0, y, z : z + 1, :]
                    else:
                        slab[9 + c, to : to + 1, :] = moved[c, index, y, z : z + 1, :]
                slab[12, to : to + 1, :] = masked[index, come : come + 1, :]
        share_there = slab[12]
        for c in range(3):
            m = slab[6 + c]
            for e in range(4):
                at = (4 * c + e) * TILES
                b = -(m * slab[9 + e]) if e < 3 else -m
                there[at : at + TILES, :] = b
                there_weighted[at : at + TILES, :] = b * share_there
        pair = cross(here_weighted[index], there[...])
        back = cross(there_weighted[...], there[...])
        for a in range(COMPS):
            packed[a : a + 1, :] = jnp.sum(
                jnp.where(same, back[group(a), :], 0.0), axis=0, keepdims=True
            )
        to_y, to_z = sub // TZ + offset[1], sub % TZ + offset[2]
        slot_y, slot_z = slot // TZ, slot % TZ
        all_slots = packed[...]
        for shift in shifts(offset):
            j = REACH.index(shift)
            meets = (slot_y + TY * shift[1] == to_y) & (slot_z + TZ * shift[2] == to_z)
            blocks[j] += jnp.where(tiled(meets, WIDE // TILES), pair, 0.0)
            from_y, from_z = slot_y - offset[1] + TY * shift[1], slot_z - offset[2] + TZ * shift[2]
            owned = (from_y >= 0) & (from_y < TY) & (from_z >= 0) & (from_z < TZ)
            shares[j] += jnp.where(tiled(owned, 2), all_slots, 0.0)
    extended = [*affine_columns, jnp.full((TILES, 1), -SPACING, F32)]
    for j in (*range(1, OTHERS + 1), 0):
        total = jnp.zeros((TILES, LANES), F32)
        for a in range(COMPS + 1):
            total = total + blocks[j, group(a), :] * extended[a]
        shares[j, COMPS : COMPS + 1, :] = jnp.sum(total, axis=0, keepdims=True)
        if j > 0:
            remote(
                shares.at[j], shares_there.at[j - 1], share_sent, share_got, device_at(REACH[j], 1)
            ).start()
    for copy in affine_copies:
        copy.wait()

    keep_row, keep_one = kept(slot[:1]), kept(tile_column)
    keep_column = [keep_one] * COMPS
    sums = []
    for a in range(COMPS):
        total = own[group(a), :] * row + blocks[0, group(a), :] * row
        for j in range(OTHERS):
            total = total + blocks[j + 1, group(a), :] * affine_there[j]
        sums.append(total)
    everything = pltpu.make_async_copy(shares_there, shares_there, share_got)
    everything.wait()
    pltpu.make_async_copy(shares_there, shares_there, share_sent).wait()
    gathered = shares[0]
    for j in range(OTHERS):
        gathered = gathered + shares_there[j]
    right = []
    for a in range(COMPS):
        spread = jnp.where(same & (lane < ROWS), gathered[a : a + 1, :], 0.0)
        total = sums[a] + spread * row + jnp.where(eyes[a], gathered[COMPS : COMPS + 1, :], 0.0)
        right.append(-keep_column[a] * jnp.sum(total, axis=1, keepdims=True))
        mine = jnp.where(lane < ROWS, own[group(a), :], 0.0)
        compact = jnp.sum(mine, axis=0, keepdims=True) + gathered[a : a + 1, :]
        unit = jnp.where((lane[:1] >= a * TILES) & (lane[:1] < (a + 1) * TILES), 1.0, 0.0)
        compact = keep_row * (compact + DAMPING * unit) + (1.0 - keep_row) * unit
        picked = jnp.where(wide_lane // TILES == wide_sub, compact, 0.0)
        for by in (8, 16, 32, 64):
            picked = picked + pltpu.roll(picked, by, 1)
        matrix[a] = picked

    rows = [matrix[a] for a in range(COMPS)]
    for k in range(COMPS):
        factor = 1.0 / rows[k][k : k + 1, :]
        at_pivot = wide_sub == k
        pivot_row = jnp.where(at_pivot, factor, rows[k] * factor)
        for i in range(COMPS):
            if i != k:
                f = rows[i][k : k + 1, :]
                rows[i] = jnp.where(at_pivot, 0.0, rows[i]) - f * pivot_row
        rows[k] = pivot_row
    for a in range(COMPS):
        compact = jnp.sum(
            jnp.where(wide_lane // TILES == wide_sub, rows[a], 0.0), axis=0, keepdims=True
        )
        inverse[group(a), :] = jnp.where(same & (lane < ROWS), compact, 0.0)

    def as_row(col):
        total = jnp.zeros((TILES, LANES), F32)
        for a in range(COMPS):
            total = total + jnp.where(eyes[a], col[a], 0.0)
        return jnp.sum(total, axis=0, keepdims=True)

    def precondition(col):
        total = jnp.zeros((TILES, LANES), F32)
        for a in range(COMPS):
            total = total + inverse[group(a), :] * col[a]
        return jnp.sum(total, axis=0, keepdims=True)

    def couple(step, vectors, meanwhile=None):
        amount = len(vectors)
        cols = [column(v) for v in vectors]
        for r, v in enumerate(vectors):
            send_rows[step][0, r : r + 1, :] = v
        for number, shift in enumerate(REACH[1:]):
            remote(
                send_rows[step].at[0],
                got_rows[step].at[number],
                halo_sems.at[step, 0],
                halo_sems.at[step, 1],
                device_at(shift, -1),
            ).start()
        local = []
        for j in range(OTHERS + 1):
            totals = [jnp.zeros((TILES, LANES), F32) for _ in vectors]
            for a in range(COMPS):
                block = blocks[j, group(a), :]
                for r in range(amount):
                    totals[r] = totals[r] + block * cols[r][a]
            for r in range(amount):
                total = jnp.sum(totals[r], axis=0, keepdims=True)
                if j == 0:
                    local.append(total)
                else:
                    back_rows[step][j - 1, r : r + 1, :] = total
            if j > 0:
                remote(
                    back_rows[step].at[j - 1],
                    got_back[step].at[j - 1],
                    halo_sems.at[step, 2],
                    halo_sems.at[step, 3],
                    device_at(REACH[j], 1),
                ).start()
        if meanwhile is not None:
            meanwhile()
        sums = [[blocks[0, group(a), :] * v for a in range(COMPS)] for v in vectors]
        rows_there, back_there = got_rows[step], got_back[step]
        pltpu.make_async_copy(rows_there, rows_there, halo_sems.at[step, 1]).wait()
        for j in range(OTHERS):
            for r in range(amount):
                v = rows_there[j, r : r + 1, :]
                for a in range(COMPS):
                    sums[r][a] = sums[r][a] + blocks[j + 1, group(a), :] * v
        pltpu.make_async_copy(back_there, back_there, halo_sems.at[step, 3]).wait()
        results = []
        for r in range(amount):
            came = local[r]
            for j in range(OTHERS):
                came = came + back_there[j, r : r + 1, :]
            results.append(
                [
                    keep_column[a]
                    * jnp.sum(sums[r][a] + jnp.where(eyes[a], came, 0.0), axis=1, keepdims=True)
                    for a in range(COMPS)
                ]
            )
        pltpu.make_async_copy(rows_there, rows_there, halo_sems.at[step, 0]).wait()
        pltpu.make_async_copy(back_there, back_there, halo_sems.at[step, 2]).wait()
        return results

    def pair_part(at):
        return pair_sum.at[at, pl.ds(0, pair_size - 1)]

    def line_part(at):
        return line_sum.at[at, pl.ds(0, size_first - 1)]

    def wait_for(part, sem):
        pltpu.make_async_copy(part, part, sem).wait()

    def start_sum(high, low, at):
        for row, value in ((0, high), (1, low)):
            pair_send[at, row : row + 1, :] = value
            pair_sum[at, in_pair, row : row + 1, :] = value

        @pl.loop(1, pair_size)
        def _(k):
            remote(
                pair_send.at[at],
                pair_sum.at[at, in_pair],
                sum_sems.at[at, 0],
                sum_sems.at[at, 1],
                pair_peer(k),
            ).start()

    def go_on_sum(at):
        wait_for(pair_part(at), sum_sems.at[at, 1])
        high, low = compensated([pair_sum[at, k] for k in range(pair_size)])
        for row, value in ((0, high), (1, low)):
            line_send[at, row : row + 1, :] = value
            line_sum[at, first, row : row + 1, :] = value

        @pl.loop(1, size_first)
        def _(k):
            remote(
                line_send.at[at],
                line_sum.at[at, first],
                sum_sems.at[at, 2],
                sum_sems.at[at, 3],
                line_peer(k),
            ).start()

    def end_sum(at):
        wait_for(line_part(at), sum_sems.at[at, 3])
        high, low = compensated([line_sum[at, k] for k in range(size_first)])
        wait_for(pair_part(at), sum_sems.at[at, 0])
        wait_for(line_part(at), sum_sems.at[at, 2])
        return tuple(jnp.broadcast_to(v, (TILES, LANES)) for v in (high, low))

    def largest(values):
        return jnp.max(jnp.abs(values), axis=1, keepdims=True)

    def gram(count, ys, zs):
        y_bound, z_bound = largest(ys), largest(zs)
        row_of, lane_of = iotas(ys.shape[0])
        high = low = jnp.zeros(ys.shape, F32)
        for j in range(count):
            at = (lane_of == row_of * count + j) & (row_of < count)
            product, error = exact_product(ys, zs[j : j + 1, :])
            h, l = lane_total(product, error, y_bound * z_bound[j : j + 1, :])
            high, low = jnp.where(at, h, high), jnp.where(at, l, low)
        return tuple(jnp.sum(v, axis=0, keepdims=True) for v in (high, low))

    def iterate(count, amount, at_p, at_r, high, low):
        major = jnp.zeros((TILES, LANES), jnp.int32)
        for k in range(1, count + 1):
            major = major + jnp.where(lane >= k * count, 1, 0)
        minor = lane - count * major

        def form(mask):
            return jnp.where(mask & (lane < count * count), 1.0, 0.0)

        g_bound = largest(high)

        def inner(x, y, bound):
            product, error = exact_product(x, y)
            values, small = exact_product(product, high)
            total = lane_total(values, small + (product * low + error * high), g_bound * bound)
            return total[0] + total[1]

        p_major, p_minor = form(major == at_p), form(minor == at_p)
        r_major, r_minor = form(major == at_r), form(minor == at_r)
        u_minor = jnp.zeros((TILES, LANES), F32)
        p_most = r_most = jnp.ones((TILES, 1), F32)
        product = inner(r_major, r_minor, r_most)
        for _ in range(amount):
            a_major = p_major + pltpu.roll(p_major, count, 1)
            a_minor = p_minor + pltpu.roll(p_minor, 1, 1)
            a_most = 2.0 * p_most
            alpha = product / inner(p_major, a_minor, p_most * a_most)
            u_minor = u_minor + alpha * p_minor
            r_major = r_major - alpha * a_major
            r_minor = r_minor - alpha * a_minor
            r_most = (r_most + jnp.abs(alpha) * a_most) * 1.01
            following = inner(r_major, r_minor, r_most * r_most)
            ratio = following / product
            p_major = r_major + ratio * p_major
            p_minor = r_minor + ratio * p_minor
            p_most = (r_most + jnp.abs(ratio) * p_most) * 1.01
            product = following
        return u_minor, r_minor, p_minor

    def combined(count, minor_form, vectors, by=0):
        both = jnp.concatenate([minor_form, minor_form], axis=0)
        weights = jnp.sum(
            jnp.where((wide_lane + by == wide_sub) & (wide_lane < count), both, 0.0),
            axis=1,
            keepdims=True,
        )
        return jnp.sum(weights * vectors, axis=0, keepdims=True)

    for ref in (chain, chain_lifted, basis, lifted):
        ref[...] = jnp.zeros_like(ref)
    chain[0:1, :] = as_row(right)
    chain_lifted[0:1, :] = precondition(right)

    def extend(step, places, ys, zs, meanwhile=None):
        found = couple(step, [zs[at : at + 1, :] for at in places], meanwhile)
        for at, col in zip(places, found):
            ys[at + 1 : at + 2, :] = as_row(col)
            zs[at + 1 : at + 2, :] = precondition(col)

    for step in range(first_steps):
        extend(step, [step], chain, chain_lifted)
    count = first_steps + 1
    start_sum(*gram(count, chain[0:8, :], chain_lifted[0:8, :]), 0)
    for step in range(first_steps, first_steps + ahead):
        extend(
            step,
            [step],
            chain,
            chain_lifted,
            functools.partial(go_on_sum, 0) if step == first_steps else None,
        )
    u_form, r_form, p_form = iterate(count, first_steps, 0, 0, *end_sum(0))
    ys, zs = chain[...], chain_lifted[...]
    part = combined(count, u_form, zs)
    at_r = second_steps + 1
    for begin, shape in ((0, p_form), (at_r, r_form)):
        for by in range(ahead + 1):
            at = begin + by
            basis[at : at + 1, :] = combined(count, shape, ys, by)
            lifted[at : at + 1, :] = combined(count, shape, zs, by)
    for step in range(first_steps + ahead, steps):
        degree = step - first_steps
        extend(step, [degree, at_r + degree][: amounts[step]], basis, lifted)
    count = 2 * second_steps + 1
    start_sum(*gram(count, basis[...], lifted[...]), 1)
    go_on_sum(1)
    u_form, r_form, _ = iterate(count, second_steps, 0, at_r, *end_sum(1))
    results = (
        (update, part + combined(count, u_form, lifted[...])),
        (residual, combined(count, r_form, basis[...])),
    )
    for out, row in results:
        spread = jnp.zeros((TILES, LANES), F32)
        for a, col in enumerate(column(row)):
            spread = jnp.where(lane == a, col, spread)
        small[...] = spread
        for y in range(TY):
            out[0, y] = small[2 * y : 2 * y + 2, 0:COMPS]


def vmem(*shape):
    return pltpu.VMEM(shape, F32)


def on_device(source_points, target_points, normals, weights, blocks, affines, anchor):
    points = source_points.shape[5]
    dirs = len(OFFSETS)
    sizes = [lax.axis_size(a) for a in AXES]
    later = SECOND - AHEAD
    amounts = (1,) * (FIRST + AHEAD) + (2,) * (later - 1) + (1,)
    steps = len(amounts)
    pair_size = sizes[1] * sizes[2]
    anywhere = pl.BlockSpec(memory_space=pl.ANY)
    in_vmem = pl.BlockSpec(memory_space=pltpu.VMEM)
    in_smem = pl.BlockSpec(memory_space=pltpu.SMEM)
    copies = len(PIECES) + OTHERS
    dma = pltpu.SemaphoreType.DMA
    last = (1, 2, 3, 0)
    outs = pl.pallas_call(
        functools.partial(step_kernel, (FIRST, SECOND, AHEAD, amounts)),
        out_shape=(jax.ShapeDtypeStruct((1, TY, TZ, COMPS), F32),) * 2,
        in_specs=[anywhere] * 4 + [in_vmem] * 2 + [in_smem],
        out_specs=[in_vmem] * 2,
        scratch_shapes=[
            vmem(*source_points.shape),
            vmem(*target_points.shape),
            vmem(*normals.shape),
            vmem(*weights.shape),
            vmem(3, dirs, TY, TZ, points),
            vmem(1, LANES),
            vmem(OTHERS, 1, LANES),
            vmem(13, TILES, points),
            vmem(LANES, points),
            vmem(dirs, WIDE, points),
            vmem(LANES, points),
            vmem(ROWS, points),
            vmem(16, LANES),
            vmem(TILES, LANES),
            pltpu.VMEM((TILES, 1), jnp.int32),
            vmem(dirs, TILES, points),
            vmem(OTHERS + 1, WIDE, LANES),
            vmem(OTHERS + 1, 16, LANES),
            vmem(ROWS, LANES),
            vmem(OTHERS, 16, LANES),
            vmem(COMPS, 16, LANES),
            vmem(ROWS, LANES),
            *[vmem(16, LANES)] * 4,
            vmem(2, pair_size, 2, LANES),
            vmem(2, sizes[0], 2, LANES),
            vmem(2, 2, LANES),
            vmem(2, 2, LANES),
            *[vmem(1, r, LANES) for r in amounts],
            *[vmem(OTHERS, r, LANES) for r in amounts],
            *[vmem(OTHERS, r, LANES) for r in amounts],
            *[vmem(OTHERS, r, LANES) for r in amounts],
            dma((4,)),
            dma((copies,)),
            dma((copies,)),
            dma,
            dma,
            dma((steps, 4)),
            dma((2, 4)),
        ],
        compiler_params=pltpu.CompilerParams(
            collective_id=0, has_side_effects=True, vmem_limit_bytes=60 * 2**20
        ),
        name="step",
    )(
        source_points,
        target_points,
        normals,
        weights,
        jnp.transpose(blocks, last),
        jnp.transpose(affines, last),
        anchor,
    )
    return tuple(jnp.transpose(out, (3, 0, 1, 2)) for out in outs)


def solution(mesh):
    placed = (
        P(None, None, "gx", "gy", "gz", None),
        P(None, None, "gx", "gy", "gz", None),
        P(None, None, "gx", "gy", "gz", None),
        P(None, "gx", "gy", "gz", None),
        P(None, "gx", "gy", "gz"),
        P(None, "gx", "gy", "gz"),
        P(),
    )
    return jax.shard_map(
        on_device,
        mesh=mesh,
        in_specs=placed,
        out_specs=(P(None, "gx", "gy", "gz"), P(None, "gx", "gy", "gz")),
        check_vma=False,
    )
```

```python
import functools

import jax
import jax.numpy as jnp
from jax import lax
from jax.experimental import pallas as pl
from jax.experimental.pallas import tpu as pltpu
from jax.sharding import PartitionSpec as P

BLOCK = 256
FIRST, SECOND, AHEAD = 6, 4, 1
SPACING = 0.5
DAMPING = 1.0
OFFSETS = (
    (1, 0, 0),
    (0, 1, 0),
    (0, 0, 1),
    (1, 1, -1),
    (1, -1, 1),
    (-1, 1, 1),
    (1, 1, 0),
    (1, 0, 1),
    (0, 1, 1),
    (1, 1, 1),
    (1, -1, 0),
    (0, 1, -1),
    (-1, 0, 1),
)
AXES = ("gx", "gy", "gz")
MESH = pl.DeviceIdType.MESH
LANES = 128
TY, TZ, TILES = 4, 2, 8
COMPS = 12
ROWS = COMPS * TILES
WIDE = ROWS + TILES
F32 = jnp.float32


def shifts(offset):
    seconds = (0,) if offset[1] == 0 else (0, offset[1])
    thirds = (0,) if offset[2] == 0 else (0, offset[2])
    return [(offset[0], y, z) for y in seconds for z in thirds]


SELF = (0, 0, 0)
REACH = (
    SELF,
    *sorted(
        {s for o in OFFSETS for s in shifts(o)} - {SELF}, key=lambda s: (-sum(map(abs, s)), s)
    ),
)
OTHERS = len(REACH) - 1
GREET = tuple(sorted({s for s in REACH[1:]} | {tuple(-p for p in s) for s in REACH[1:]}))


def spans(part, shift, length):
    if part == 0:
        return 0, length
    if shift == 0:
        return (1 if part > 0 else 0), length - 1
    return (0 if part > 0 else length - 1), 1


ORDER = tuple(sorted(range(len(OFFSETS)), key=lambda d: ((0, 2, 1)[OFFSETS[d][0]], d)))
PIECES = tuple(
    (d, s, *spans(OFFSETS[d][1], s[1], TY), *spans(OFFSETS[d][2], s[2], TZ))
    for d in ORDER
    for s in shifts(OFFSETS[d])
    if s != SELF
)


def device_at(shift, sign):
    there = []
    for axis, part in zip(AXES, shift):
        size = lax.axis_size(axis)
        there.append(lax.rem(lax.axis_index(axis) + (sign * part + size), size))
    return tuple(there)


def exists(shift):
    found = True
    for axis, part in zip(AXES, shift):
        if part > 0:
            found = jnp.logical_and(lax.axis_index(axis) + part < lax.axis_size(axis), found)
        elif part < 0:
            found = jnp.logical_and(lax.axis_index(axis) + part >= 0, found)
    return found


def either(condition, then, otherwise):
    lax.cond(condition, lambda: (then(), None)[1], lambda: (otherwise(), None)[1])


def remote(source, target, sent, got, device):
    return pltpu.make_async_remote_copy(
        src_ref=source,
        dst_ref=target,
        send_sem=sent,
        recv_sem=got,
        device_id=device,
        device_id_type=MESH,
    )


def iotas(rows=TILES):
    return (
        lax.broadcasted_iota(jnp.int32, (rows, LANES), 0),
        lax.broadcasted_iota(jnp.int32, (rows, LANES), 1),
    )


def tiled(mask, times):
    return jnp.concatenate([mask] * times, axis=0)


def cross(left, right):
    return lax.dot_general(
        left,
        right,
        (((1,), (1,)), ((), ())),
        precision=lax.Precision.HIGHEST,
        preferred_element_type=F32,
    )


def split(x):
    big = x * 4097.0
    high = big - (big - x)
    return high, x - high


def exact_product(x, y):
    (xh, xl), (yh, yl) = split(x), split(y)
    product = x * y
    return product, ((xh * yh - product) + xh * yl + xl * yh) + xl * yl


def lane_total(values, small, bound):
    grid = bound * 256.0
    top = (values + grid) - grid
    rest = values - top
    grid = grid * 2.0**-16
    middle = (rest + grid) - grid
    small = small + (rest - middle)
    top, middle, small = (jnp.sum(v, axis=1, keepdims=True) for v in (top, middle, small))
    high = top + middle
    back = high - top
    return high, ((top - (high - back)) + (middle - back)) + small


def compensated(parts):
    total, error = parts[0], jnp.zeros_like(parts[0])
    for part in parts[1:]:
        following = total + part
        back = following - total
        error = error + ((total - (following - back)) + (part - back))
        total = following
    high, low = total[0:1], error[0:1] + total[1:2]
    both = high + low
    return both, low - (both - high)


def step_kernel(plan, *refs):
    first_steps, second_steps, ahead, amounts = plan
    steps = len(amounts)
    source_out, target_out, normal_out, weight_out, counts, affines, anchor = refs[:7]
    update, residual = refs[7:9]
    source, target, normal, weight, moved, affine, affine_there = refs[9:16]
    slab, here, here_weighted, there, there_weighted, packed, small = refs[16:23]
    small_count, masked, blocks, shares, own = refs[23:28]
    shares_there, matrix, inverse, chain, chain_lifted, basis, lifted = refs[28:35]
    pair_sum, line_sum, pair_send, line_send = refs[35:39]
    rest = refs[39:]
    send_rows, got_rows, back_rows, got_back = (rest[k * steps : (k + 1) * steps] for k in range(4))
    zero_one, zero_two, zero_share, spare_one, spare_two, spare_share = rest[4 * steps :][:6]
    loaded, sent, got, share_sent, share_got, halo_sems, sum_sems = rest[4 * steps + 6 :]
    loads = [
        pltpu.make_async_copy(outer, ref, loaded.at[number])
        for number, (outer, ref) in enumerate(
            (
                (target_out, target),
                (source_out, source),
                (normal_out, normal),
                (weight_out, weight),
            )
        )
    ]
    for load in loads:
        load.start()
    first, second, third = (lax.axis_index(a) for a in AXES)
    size_first, size_second, size_third = (lax.axis_size(a) for a in AXES)
    in_pair = second * size_third + third
    pair_size = size_second * size_third

    def pair_peer(k):
        there = lax.rem(in_pair + k, pair_size)
        return (first, there // size_third, lax.rem(there, size_third))

    def line_peer(k):
        return (lax.rem(first + k, size_first), second, third)

    barrier = pltpu.get_barrier_semaphore()
    for ref in (moved, affine_there, zero_one, zero_two, zero_share):
        ref[...] = jnp.zeros_like(ref)
    neighbours = 0
    for shift in GREET:
        near = exists(shift)
        neighbours = neighbours + jnp.where(near, 1, 0)

        @pl.when(near)
        def _(shift=shift):
            pl.semaphore_signal(barrier, inc=1, device_id=device_at(shift, 1), device_id_type=MESH)


    @pl.loop(1, pair_size)
    def _(k):
        pl.semaphore_signal(barrier, inc=1, device_id=pair_peer(k), device_id_type=MESH)

    @pl.loop(1, size_first)
    def _(k):
        pl.semaphore_signal(barrier, inc=1, device_id=line_peer(k), device_id_type=MESH)

    sub, lane = iotas()
    slot = lane & (TILES - 1)
    same = sub == slot
    eyes = [lane == sub + a * TILES for a in range(COMPS)]
    wide_sub, wide_lane = iotas(16)

    def column(row):
        return [jnp.sum(jnp.where(eyes[a], row, 0.0), axis=1, keepdims=True) for a in range(COMPS)]

    def group(a):
        return slice(a * TILES, (a + 1) * TILES)

    def positions(tile):
        return (first, second * TY + tile // TZ, third * TZ + tile % TZ)

    extents = (size_first, size_second * TY, size_third * TZ)

    def kept(tile):
        x, y, z = positions(tile)
        return jnp.where((x * extents[1] + y) * extents[2] + z != anchor[0], 1.0, 0.0)

    for y in range(TY):
        small[2 * y : 2 * y + 2, 0:COMPS] = affines[0, y]
    affine_columns = [
        small[:, a : a + 1] + (1.0 if a % 5 == 0 else 0.0) for a in range(COMPS)
    ]
    row = jnp.zeros((TILES, LANES), F32)
    for a in range(COMPS):
        row = row + jnp.where(eyes[a], affine_columns[a], 0.0)
    row = jnp.sum(row, axis=0, keepdims=True)
    row = jnp.where((lane[:1] >= ROWS) & (lane[:1] < WIDE), -SPACING, row)
    affine[...] = row

    pl.semaphore_wait(barrier, neighbours + (pair_size - 1 + size_first - 1))
    loads[0].wait()
    zeros = {1: (zero_one, spare_one), 2: (zero_two, spare_two), 16: (zero_share, spare_share)}
    ahead_there = [exists(shift) for shift in REACH[1:]]
    behind_there = [exists(tuple(-part for part in shift)) for shift in REACH[1:]]

    def fill(count, place, number, arrival, departure):
        nothing, spare = zeros[count]
        pltpu.make_async_copy(nothing, place, arrival).start()
        pltpu.make_async_copy(nothing, spare.at[number], departure).start()

    copies = {}
    for number, (index, shift, low, count, low_z, count_z) in enumerate(PIECES):
        at = (slice(None), index, pl.ds(low, count), pl.ds(low_z, count_z))
        copy = remote(
            target.at[(slice(None), index, 0, *at[2:])],
            moved.at[at],
            sent.at[number],
            got.at[number],
            device_at(shift, -1),
        )
        number = REACH.index(shift) - 1
        pl.when(behind_there[number])(copy.start)
        copies.setdefault(index, []).append((copy, number))
    affine_copies = []
    for number, shift in enumerate(REACH[1:]):
        at = len(PIECES) + number
        affine_copies.append(
            remote(affine, affine_there.at[number], sent.at[at], got.at[at], device_at(shift, -1))
        )
        pl.when(behind_there[number])(affine_copies[-1].start)

    for ref in (blocks, shares, own, packed):
        ref[...] = jnp.zeros_like(ref)
    points = here.shape[1]
    here[WIDE:, :] = jnp.zeros((LANES - WIDE, points), F32)
    there[ROWS:, :] = jnp.zeros((LANES - ROWS, points), F32)
    numbers = lax.broadcasted_iota(jnp.int32, (TILES, points), 1)
    tile_column = sub[:, 0:1]
    for load in loads[1:]:
        load.wait()
    for index in ORDER:
        offset = OFFSETS[index]
        for y in range(TY):
            for c in range(3):
                slab[c, 2 * y : 2 * y + 2, :] = source[c, index, 0, y]
                slab[3 + c, 2 * y : 2 * y + 2, :] = normal[c, index, 0, y]
            slab[6, 2 * y : 2 * y + 2, :] = weight[index, 0, y]
            small_count[2 * y : 2 * y + 2, :] = counts[0, y, :, index : index + 1]
        inside = functools.reduce(
            jnp.logical_and,
            [
                (p + o >= 0) & (p + o < extent)
                for p, o, extent in zip(positions(tile_column), offset, extents)
            ],
        )
        limit = jnp.where(inside, BLOCK * small_count[...], 0)
        share = jnp.where(numbers < limit, slab[6], 0.0)
        masked[index] = share
        for c in range(3):
            n = slab[3 + c]
            for e in range(4):
                at = (4 * c + e) * TILES
                a = n * slab[e] if e < 3 else n
                here[at : at + TILES, :] = a
                here_weighted[index, at : at + TILES, :] = a * share
        along = sum(part * slab[3 + c] for c, part in enumerate(offset) if part != 0)
        here[ROWS:WIDE, :] = along
        here_weighted[index, ROWS:WIDE, :] = along * share
        own[...] += cross(here_weighted[index, :ROWS, :], here[...])
    own[...] = jnp.where(tiled(same, COMPS), own[...], 0.0)

    for index in ORDER:
        offset = OFFSETS[index]
        for copy, number in copies.get(index, ()):
            pl.when(ahead_there[number])(copy.wait_recv)
        for y in range(TY):
            before = (y - offset[1]) % TY
            shift_y = (y - offset[1]) // TY
            for z in range(TZ):
                back = (z - offset[2]) % TZ
                shift_z = (z - offset[2]) // TZ
                to, come = y * TZ + z, before * TZ + back
                local = (offset[0], -shift_y, -shift_z) == SELF
                for c in range(3):
                    slab[6 + c, to : to + 1, :] = normal[c, index, 0, before, back : back + 1, :]
                    if local:
                        slab[9 + c, to : to + 1, :] = target[c, index, 0, y, z : z + 1, :]
                    else:
                        slab[9 + c, to : to + 1, :] = moved[c, index, y, z : z + 1, :]
                slab[12, to : to + 1, :] = masked[index, come : come + 1, :]
        share_there = slab[12]
        for c in range(3):
            m = slab[6 + c]
            for e in range(4):
                at = (4 * c + e) * TILES
                b = -(m * slab[9 + e]) if e < 3 else -m
                there[at : at + TILES, :] = b
                there_weighted[at : at + TILES, :] = b * share_there
        pair = cross(here_weighted[index], there[...])
        back = cross(there_weighted[...], there[...])
        for a in range(COMPS):
            packed[a : a + 1, :] = jnp.sum(
                jnp.where(same, back[group(a), :], 0.0), axis=0, keepdims=True
            )
        to_y, to_z = sub // TZ + offset[1], sub % TZ + offset[2]
        slot_y, slot_z = slot // TZ, slot % TZ
        all_slots = packed[...]
        for shift in shifts(offset):
            j = REACH.index(shift)
            meets = (slot_y + TY * shift[1] == to_y) & (slot_z + TZ * shift[2] == to_z)
            blocks[j] += jnp.where(tiled(meets, WIDE // TILES), pair, 0.0)
            from_y, from_z = slot_y - offset[1] + TY * shift[1], slot_z - offset[2] + TZ * shift[2]
            owned = (from_y >= 0) & (from_y < TY) & (from_z >= 0) & (from_z < TZ)
            shares[j] += jnp.where(tiled(owned, 2), all_slots, 0.0)
    extended = [*affine_columns, jnp.full((TILES, 1), -SPACING, F32)]
    for j in range(OTHERS + 1):
        total = jnp.zeros((TILES, LANES), F32)
        for a in range(COMPS + 1):
            total = total + blocks[j, group(a), :] * extended[a]
        shares[j, COMPS : COMPS + 1, :] = jnp.sum(total, axis=0, keepdims=True)
    for number, shift in enumerate(REACH[1:]):
        copy = remote(
            shares.at[number + 1],
            shares_there.at[number],
            share_sent,
            share_got,
            device_at(shift, 1),
        )
        pl.when(ahead_there[number])(copy.start)

        @pl.when(jnp.logical_not(behind_there[number]))
        def _(number=number):
            nothing = zeros[16][0]
            pltpu.make_async_copy(nothing, shares_there.at[number], share_got).start()

        @pl.when(jnp.logical_not(ahead_there[number]))
        def _(number=number):
            nothing, spare = zeros[16]
            pltpu.make_async_copy(nothing, spare.at[number], share_sent).start()

    for index in ORDER:
        for copy, number in copies.get(index, ()):
            pl.when(behind_there[number])(copy.wait_send)
    for number, copy in enumerate(affine_copies):
        pl.when(ahead_there[number])(copy.wait_recv)
        pl.when(behind_there[number])(copy.wait_send)

    keep_row, keep_one = kept(slot[:1]), kept(tile_column)
    keep_column = [keep_one] * COMPS
    sums = []
    for a in range(COMPS):
        total = own[group(a), :] * row + blocks[0, group(a), :] * row
        for j in range(OTHERS):
            total = total + blocks[j + 1, group(a), :] * affine_there[j]
        sums.append(total)
    everything = pltpu.make_async_copy(shares_there, shares_there, share_got)
    everything.wait()
    pltpu.make_async_copy(shares_there, shares_there, share_sent).wait()
    gathered = shares[0]
    for j in range(OTHERS):
        gathered = gathered + shares_there[j]
    right = []
    for a in range(COMPS):
        spread = jnp.where(same & (lane < ROWS), gathered[a : a + 1, :], 0.0)
        total = sums[a] + spread * row + jnp.where(eyes[a], gathered[COMPS : COMPS + 1, :], 0.0)
        right.append(-keep_column[a] * jnp.sum(total, axis=1, keepdims=True))
        mine = jnp.where(lane < ROWS, own[group(a), :], 0.0)
        compact = jnp.sum(mine, axis=0, keepdims=True) + gathered[a : a + 1, :]
        unit = jnp.where((lane[:1] >= a * TILES) & (lane[:1] < (a + 1) * TILES), 1.0, 0.0)
        compact = keep_row * (compact + DAMPING * unit) + (1.0 - keep_row) * unit
        picked = jnp.where(wide_lane // TILES == wide_sub, compact, 0.0)
        for by in (8, 16, 32, 64):
            picked = picked + pltpu.roll(picked, by, 1)
        matrix[a] = picked

    rows = [matrix[a] for a in range(COMPS)]
    for k in range(COMPS):
        factor = 1.0 / rows[k][k : k + 1, :]
        at_pivot = wide_sub == k
        pivot_row = jnp.where(at_pivot, factor, rows[k] * factor)
        for i in range(COMPS):
            if i != k:
                f = rows[i][k : k + 1, :]
                rows[i] = jnp.where(at_pivot, 0.0, rows[i]) - f * pivot_row
        rows[k] = pivot_row
    for a in range(COMPS):
        compact = jnp.sum(
            jnp.where(wide_lane // TILES == wide_sub, rows[a], 0.0), axis=0, keepdims=True
        )
        inverse[group(a), :] = jnp.where(same & (lane < ROWS), compact, 0.0)

    def as_row(col):
        total = jnp.zeros((TILES, LANES), F32)
        for a in range(COMPS):
            total = total + jnp.where(eyes[a], col[a], 0.0)
        return jnp.sum(total, axis=0, keepdims=True)

    def precondition(col):
        total = jnp.zeros((TILES, LANES), F32)
        for a in range(COMPS):
            total = total + inverse[group(a), :] * col[a]
        return jnp.sum(total, axis=0, keepdims=True)

    def couple(step, vectors, meanwhile=None):
        amount = len(vectors)
        for r, v in enumerate(vectors):
            send_rows[step][0, r : r + 1, :] = v
        for number, shift in enumerate(REACH[1:]):
            copy = remote(
                send_rows[step].at[0],
                got_rows[step].at[number],
                halo_sems.at[step, 0],
                halo_sems.at[step, 1],
                device_at(shift, -1),
            )
            empty = functools.partial(
                fill,
                amount,
                got_back[step].at[number],
                number,
                halo_sems.at[step, 3],
                halo_sems.at[step, 0],
            )
            either(behind_there[number], copy.start, empty)
        cols = [column(v) for v in vectors]
        local = []
        for j in range(OTHERS + 1):
            totals = [jnp.zeros((TILES, LANES), F32) for _ in vectors]
            for a in range(COMPS):
                block = blocks[j, group(a), :]
                for r in range(amount):
                    totals[r] = totals[r] + block * cols[r][a]
            for r in range(amount):
                total = jnp.sum(totals[r], axis=0, keepdims=True)
                if j == 0:
                    local.append(total)
                else:
                    back_rows[step][j - 1, r : r + 1, :] = total
        for number, shift in enumerate(REACH[1:]):
            copy = remote(
                back_rows[step].at[number],
                got_back[step].at[number],
                halo_sems.at[step, 2],
                halo_sems.at[step, 3],
                device_at(shift, 1),
            )
            empty = functools.partial(
                fill,
                amount,
                got_rows[step].at[number],
                OTHERS + number,
                halo_sems.at[step, 1],
                halo_sems.at[step, 2],
            )
            either(ahead_there[number], copy.start, empty)
        if meanwhile is not None:
            meanwhile()
        sums = [[blocks[0, group(a), :] * v for a in range(COMPS)] for v in vectors]
        rows_there, back_there = got_rows[step], got_back[step]
        pltpu.make_async_copy(rows_there, rows_there, halo_sems.at[step, 1]).wait()
        for j in range(OTHERS):
            for r in range(amount):
                v = rows_there[j, r : r + 1, :]
                for a in range(COMPS):
                    sums[r][a] = sums[r][a] + blocks[j + 1, group(a), :] * v
        pltpu.make_async_copy(back_there, back_there, halo_sems.at[step, 3]).wait()
        results = []
        for r in range(amount):
            came = local[r]
            for j in range(OTHERS):
                came = came + back_there[j, r : r + 1, :]
            results.append(
                [
                    keep_column[a]
                    * jnp.sum(sums[r][a] + jnp.where(eyes[a], came, 0.0), axis=1, keepdims=True)
                    for a in range(COMPS)
                ]
            )
        pltpu.make_async_copy(rows_there, rows_there, halo_sems.at[step, 0]).wait()
        pltpu.make_async_copy(back_there, back_there, halo_sems.at[step, 2]).wait()
        return results

    def pair_part(at):
        return pair_sum.at[at, pl.ds(0, pair_size - 1)]

    def line_part(at):
        return line_sum.at[at, pl.ds(0, size_first - 1)]

    def wait_for(part, sem):
        pltpu.make_async_copy(part, part, sem).wait()

    def start_sum(high, low, at):
        for row, value in ((0, high), (1, low)):
            pair_send[at, row : row + 1, :] = value
            pair_sum[at, in_pair, row : row + 1, :] = value

        @pl.loop(1, pair_size)
        def _(k):
            remote(
                pair_send.at[at],
                pair_sum.at[at, in_pair],
                sum_sems.at[at, 0],
                sum_sems.at[at, 1],
                pair_peer(k),
            ).start()

    def go_on_sum(at):
        wait_for(pair_part(at), sum_sems.at[at, 1])
        high, low = compensated([pair_sum[at, k] for k in range(pair_size)])
        for row, value in ((0, high), (1, low)):
            line_send[at, row : row + 1, :] = value
            line_sum[at, first, row : row + 1, :] = value

        @pl.loop(1, size_first)
        def _(k):
            remote(
                line_send.at[at],
                line_sum.at[at, first],
                sum_sems.at[at, 2],
                sum_sems.at[at, 3],
                line_peer(k),
            ).start()

    def end_sum(at):
        wait_for(line_part(at), sum_sems.at[at, 3])
        high, low = compensated([line_sum[at, k] for k in range(size_first)])
        wait_for(pair_part(at), sum_sems.at[at, 0])
        wait_for(line_part(at), sum_sems.at[at, 2])
        return tuple(jnp.broadcast_to(v, (TILES, LANES)) for v in (high, low))

    def largest(values):
        return jnp.max(jnp.abs(values), axis=1, keepdims=True)

    def gram(count, ys, zs):
        y_bound, z_bound = largest(ys), largest(zs)
        row_of, lane_of = iotas(ys.shape[0])
        high = low = jnp.zeros(ys.shape, F32)
        for j in range(count):
            at = (lane_of == row_of * count + j) & (row_of < count)
            product, error = exact_product(ys, zs[j : j + 1, :])
            h, l = lane_total(product, error, y_bound * z_bound[j : j + 1, :])
            high, low = jnp.where(at, h, high), jnp.where(at, l, low)
        return tuple(jnp.sum(v, axis=0, keepdims=True) for v in (high, low))

    def iterate(count, amount, at_p, at_r, high, low):
        major = jnp.zeros((TILES, LANES), jnp.int32)
        for k in range(1, count + 1):
            major = major + jnp.where(lane >= k * count, 1, 0)
        minor = lane - count * major

        def form(mask):
            return jnp.where(mask & (lane < count * count), 1.0, 0.0)

        g_bound = largest(high)

        def inner(x, y, bound):
            product, error = exact_product(x, y)
            values, small = exact_product(product, high)
            total = lane_total(values, small + (product * low + error * high), g_bound * bound)
            return total[0] + total[1]

        p_major, p_minor = form(major == at_p), form(minor == at_p)
        r_major, r_minor = form(major == at_r), form(minor == at_r)
        u_minor = jnp.zeros((TILES, LANES), F32)
        p_most = r_most = jnp.ones((TILES, 1), F32)
        product = inner(r_major, r_minor, r_most)
        for _ in range(amount):
            a_major = p_major + pltpu.roll(p_major, count, 1)
            a_minor = p_minor + pltpu.roll(p_minor, 1, 1)
            a_most = 2.0 * p_most
            alpha = product / inner(p_major, a_minor, p_most * a_most)
            u_minor = u_minor + alpha * p_minor
            r_major = r_major - alpha * a_major
            r_minor = r_minor - alpha * a_minor
            r_most = (r_most + jnp.abs(alpha) * a_most) * 1.01
            following = inner(r_major, r_minor, r_most * r_most)
            ratio = following / product
            p_major = r_major + ratio * p_major
            p_minor = r_minor + ratio * p_minor
            p_most = (r_most + jnp.abs(ratio) * p_most) * 1.01
            product = following
        return u_minor, r_minor, p_minor

    def combined(count, minor_form, vectors, by=0):
        both = jnp.concatenate([minor_form, minor_form], axis=0)
        weights = jnp.sum(
            jnp.where((wide_lane + by == wide_sub) & (wide_lane < count), both, 0.0),
            axis=1,
            keepdims=True,
        )
        return jnp.sum(weights * vectors, axis=0, keepdims=True)

    for ref in (chain, chain_lifted, basis, lifted):
        ref[...] = jnp.zeros_like(ref)
    chain[0:1, :] = as_row(right)
    chain_lifted[0:1, :] = precondition(right)

    def extend(step, places, ys, zs, meanwhile=None):
        found = couple(step, [zs[at : at + 1, :] for at in places], meanwhile)
        for at, col in zip(places, found):
            ys[at + 1 : at + 2, :] = as_row(col)
            zs[at + 1 : at + 2, :] = precondition(col)

    for step in range(first_steps):
        extend(step, [step], chain, chain_lifted)
    count = first_steps + 1
    start_sum(*gram(count, chain[0:8, :], chain_lifted[0:8, :]), 0)
    for step in range(first_steps, first_steps + ahead):
        extend(
            step,
            [step],
            chain,
            chain_lifted,
            functools.partial(go_on_sum, 0) if step == first_steps else None,
        )
    u_form, r_form, p_form = iterate(count, first_steps, 0, 0, *end_sum(0))
    ys, zs = chain[...], chain_lifted[...]
    part = combined(count, u_form, zs)
    at_r = second_steps + 1
    for begin, shape in ((0, p_form), (at_r, r_form)):
        for by in range(ahead + 1):
            at = begin + by
            basis[at : at + 1, :] = combined(count, shape, ys, by)
            lifted[at : at + 1, :] = combined(count, shape, zs, by)
    for step in range(first_steps + ahead, steps):
        degree = step - first_steps
        extend(step, [degree, at_r + degree][: amounts[step]], basis, lifted)
    count = 2 * second_steps + 1
    start_sum(*gram(count, basis[...], lifted[...]), 1)
    go_on_sum(1)
    u_form, r_form, _ = iterate(count, second_steps, 0, at_r, *end_sum(1))
    results = (
        (update, part + combined(count, u_form, lifted[...])),
        (residual, combined(count, r_form, basis[...])),
    )
    for out, row in results:
        spread = jnp.zeros((TILES, LANES), F32)
        for a, col in enumerate(column(row)):
            spread = jnp.where(lane == a, col, spread)
        small[...] = spread
        for y in range(TY):
            out[0, y] = small[2 * y : 2 * y + 2, 0:COMPS]


def vmem(*shape):
    return pltpu.VMEM(shape, F32)


def on_device(source_points, target_points, normals, weights, blocks, affines, anchor):
    points = source_points.shape[5]
    dirs = len(OFFSETS)
    sizes = [lax.axis_size(a) for a in AXES]
    later = SECOND - AHEAD
    amounts = (1,) * (FIRST + AHEAD) + (2,) * (later - 1) + (1,)
    steps = len(amounts)
    pair_size = sizes[1] * sizes[2]
    anywhere = pl.BlockSpec(memory_space=pl.ANY)
    in_vmem = pl.BlockSpec(memory_space=pltpu.VMEM)
    in_smem = pl.BlockSpec(memory_space=pltpu.SMEM)
    copies = len(PIECES) + OTHERS
    dma = pltpu.SemaphoreType.DMA
    last = (1, 2, 3, 0)
    outs = pl.pallas_call(
        functools.partial(step_kernel, (FIRST, SECOND, AHEAD, amounts)),
        out_shape=(jax.ShapeDtypeStruct((1, TY, TZ, COMPS), F32),) * 2,
        in_specs=[anywhere] * 4 + [in_vmem] * 2 + [in_smem],
        out_specs=[in_vmem] * 2,
        scratch_shapes=[
            vmem(*source_points.shape),
            vmem(*target_points.shape),
            vmem(*normals.shape),
            vmem(*weights.shape),
            vmem(3, dirs, TY, TZ, points),
            vmem(1, LANES),
            vmem(OTHERS, 1, LANES),
            vmem(13, TILES, points),
            vmem(LANES, points),
            vmem(dirs, WIDE, points),
            vmem(LANES, points),
            vmem(ROWS, points),
            vmem(16, LANES),
            vmem(TILES, LANES),
            pltpu.VMEM((TILES, 1), jnp.int32),
            vmem(dirs, TILES, points),
            vmem(OTHERS + 1, WIDE, LANES),
            vmem(OTHERS + 1, 16, LANES),
            vmem(ROWS, LANES),
            vmem(OTHERS, 16, LANES),
            vmem(COMPS, 16, LANES),
            vmem(ROWS, LANES),
            *[vmem(16, LANES)] * 4,
            vmem(2, pair_size, 2, LANES),
            vmem(2, sizes[0], 2, LANES),
            vmem(2, 2, LANES),
            vmem(2, 2, LANES),
            *[vmem(1, r, LANES) for r in amounts],
            *[vmem(OTHERS, r, LANES) for r in amounts],
            *[vmem(OTHERS, r, LANES) for r in amounts],
            *[vmem(OTHERS, r, LANES) for r in amounts],
            vmem(1, LANES),
            vmem(2, LANES),
            vmem(16, LANES),
            vmem(2 * OTHERS, 1, LANES),
            vmem(2 * OTHERS, 2, LANES),
            vmem(OTHERS, 16, LANES),
            dma((4,)),
            dma((copies,)),
            dma((copies,)),
            dma,
            dma,
            dma((steps, 4)),
            dma((2, 4)),
        ],
        compiler_params=pltpu.CompilerParams(
            collective_id=0, has_side_effects=True, vmem_limit_bytes=60 * 2**20
        ),
        name="step",
    )(
        source_points,
        target_points,
        normals,
        weights,
        jnp.transpose(blocks, last),
        jnp.transpose(affines, last),
        anchor,
    )
    return tuple(jnp.transpose(out, (3, 0, 1, 2)) for out in outs)


def solution(mesh):
    placed = (
        P(None, None, "gx", "gy", "gz", None),
        P(None, None, "gx", "gy", "gz", None),
        P(None, None, "gx", "gy", "gz", None),
        P(None, "gx", "gy", "gz", None),
        P(None, "gx", "gy", "gz"),
        P(None, "gx", "gy", "gz"),
        P(),
    )
    return jax.shard_map(
        on_device,
        mesh=mesh,
        in_specs=placed,
        out_specs=(P(None, "gx", "gy", "gz"), P(None, "gx", "gy", "gz")),
        check_vma=False,
    )
```

```python
import functools

import jax
import jax.numpy as jnp
from jax import lax
from jax.experimental import pallas as pl
from jax.experimental.pallas import tpu as pltpu
from jax.sharding import PartitionSpec as P

BLOCK = 256
FIRST, SECOND, AHEAD = 5, 5, 2
SPACING = 0.5
DAMPING = 1.0
OFFSETS = (
    (1, 0, 0),
    (0, 1, 0),
    (0, 0, 1),
    (1, 1, -1),
    (1, -1, 1),
    (-1, 1, 1),
    (1, 1, 0),
    (1, 0, 1),
    (0, 1, 1),
    (1, 1, 1),
    (1, -1, 0),
    (0, 1, -1),
    (-1, 0, 1),
)
AXES = ("gx", "gy", "gz")
MESH = pl.DeviceIdType.MESH
LANES = 128
TY, TZ, TILES = 4, 2, 8
COMPS = 12
ROWS = COMPS * TILES
WIDE = ROWS + TILES
F32 = jnp.float32


def shifts(offset):
    seconds = (0,) if offset[1] == 0 else (0, offset[1])
    thirds = (0,) if offset[2] == 0 else (0, offset[2])
    return [(offset[0], y, z) for y in seconds for z in thirds]


SELF = (0, 0, 0)
REACH = (
    SELF,
    *sorted(
        {s for o in OFFSETS for s in shifts(o)} - {SELF}, key=lambda s: (-sum(map(abs, s)), s)
    ),
)
OTHERS = len(REACH) - 1
PAIRS = tuple(dict.fromkeys((s[0], s[2]) for s in REACH))
MEMBERS = tuple({s[1]: REACH.index(s) for s in REACH if (s[0], s[2]) == pair} for pair in PAIRS)
GREET = tuple(sorted({s for s in REACH[1:]} | {tuple(-p for p in s) for s in REACH[1:]}))


def spans(part, shift, length):
    if part == 0:
        return 0, length
    if shift == 0:
        return (1 if part > 0 else 0), length - 1
    return (0 if part > 0 else length - 1), 1


ORDER = tuple(sorted(range(len(OFFSETS)), key=lambda d: ((0, 2, 1)[OFFSETS[d][0]], d)))
PIECES = tuple(
    (d, s, *spans(OFFSETS[d][1], s[1], TY), *spans(OFFSETS[d][2], s[2], TZ))
    for d in ORDER
    for s in shifts(OFFSETS[d])
    if s != SELF
)


def device_at(shift, sign):
    there = []
    for axis, part in zip(AXES, shift):
        size = lax.axis_size(axis)
        there.append(lax.rem(lax.axis_index(axis) + (sign * part + size), size))
    return tuple(there)


def exists(shift):
    found = True
    for axis, part in zip(AXES, shift):
        if part > 0:
            found = jnp.logical_and(lax.axis_index(axis) + part < lax.axis_size(axis), found)
        elif part < 0:
            found = jnp.logical_and(lax.axis_index(axis) + part >= 0, found)
    return found


def either(condition, then, otherwise):
    lax.cond(condition, lambda: (then(), None)[1], lambda: (otherwise(), None)[1])


def remote(source, target, sent, got, device):
    return pltpu.make_async_remote_copy(
        src_ref=source,
        dst_ref=target,
        send_sem=sent,
        recv_sem=got,
        device_id=device,
        device_id_type=MESH,
    )


def iotas(rows=TILES):
    return (
        lax.broadcasted_iota(jnp.int32, (rows, LANES), 0),
        lax.broadcasted_iota(jnp.int32, (rows, LANES), 1),
    )


def tiled(mask, times):
    return jnp.concatenate([mask] * times, axis=0)


def cross(left, right):
    return lax.dot_general(
        left,
        right,
        (((1,), (1,)), ((), ())),
        precision=lax.Precision.HIGHEST,
        preferred_element_type=F32,
    )


def split(x):
    big = x * 4097.0
    high = big - (big - x)
    return high, x - high


def exact_product(x, y):
    (xh, xl), (yh, yl) = split(x), split(y)
    product = x * y
    return product, ((xh * yh - product) + xh * yl + xl * yh) + xl * yl


def lane_total(values, small, bound):
    grid = bound * 256.0
    top = (values + grid) - grid
    rest = values - top
    grid = grid * 2.0**-16
    middle = (rest + grid) - grid
    small = small + (rest - middle)
    top, middle, small = (jnp.sum(v, axis=1, keepdims=True) for v in (top, middle, small))
    high = top + middle
    back = high - top
    return high, ((top - (high - back)) + (middle - back)) + small


def compensated(parts):
    total, error = parts[0], jnp.zeros_like(parts[0])
    for part in parts[1:]:
        following = total + part
        back = following - total
        error = error + ((total - (following - back)) + (part - back))
        total = following
    high, low = total[0:1], error[0:1] + total[1:2]
    both = high + low
    return both, low - (both - high)


def step_kernel(plan, *refs):
    first_steps, second_steps, ahead, amounts = plan
    steps = len(amounts)
    source_out, target_out, normal_out, weight_out, counts, affines, anchor = refs[:7]
    update, residual = refs[7:9]
    source, target, normal, weight, moved, affine, affine_there = refs[9:16]
    slab, here, here_weighted, there, there_weighted, packed, small = refs[16:23]
    small_count, masked, blocks, shares, own = refs[23:28]
    shares_there, matrix, inverse, chain, chain_lifted, basis, lifted = refs[28:35]
    pair_sum, line_sum, pair_send, line_send = refs[35:39]
    rest = refs[39:]
    send_rows, got_rows, back_rows, got_back = (rest[k * steps : (k + 1) * steps] for k in range(4))
    zero_one, zero_two, zero_share, spare_one, spare_two, spare_share = rest[4 * steps :][:6]
    loaded, sent, got, share_sent, share_got, halo_sems, sum_sems = rest[4 * steps + 6 :]
    loads = [
        pltpu.make_async_copy(outer, ref, loaded.at[number])
        for number, (outer, ref) in enumerate(
            (
                (target_out, target),
                (source_out, source),
                (normal_out, normal),
                (weight_out, weight),
            )
        )
    ]
    for load in loads:
        load.start()
    first, second, third = (lax.axis_index(a) for a in AXES)
    size_first, size_second, size_third = (lax.axis_size(a) for a in AXES)
    in_pair = second * size_third + third
    pair_size = size_second * size_third

    def pair_peer(k):
        there = lax.rem(in_pair + k, pair_size)
        return (first, there // size_third, lax.rem(there, size_third))

    def line_peer(k):
        return (lax.rem(first + k, size_first), second, third)

    barrier = pltpu.get_barrier_semaphore()
    for ref in (moved, affine_there, zero_one, zero_two, zero_share):
        ref[...] = jnp.zeros_like(ref)
    neighbours = 0
    for shift in GREET:
        near = exists(shift)
        neighbours = neighbours + jnp.where(near, 1, 0)

        @pl.when(near)
        def _(shift=shift):
            pl.semaphore_signal(barrier, inc=1, device_id=device_at(shift, 1), device_id_type=MESH)


    @pl.loop(1, pair_size)
    def _(k):
        pl.semaphore_signal(barrier, inc=1, device_id=pair_peer(k), device_id_type=MESH)

    @pl.loop(1, size_first)
    def _(k):
        pl.semaphore_signal(barrier, inc=1, device_id=line_peer(k), device_id_type=MESH)

    sub, lane = iotas()
    slot = lane & (TILES - 1)
    same = sub == slot
    eyes = [lane == sub + a * TILES for a in range(COMPS)]
    wide_sub, wide_lane = iotas(16)

    def column(row):
        return [jnp.sum(jnp.where(eyes[a], row, 0.0), axis=1, keepdims=True) for a in range(COMPS)]

    def group(a):
        return slice(a * TILES, (a + 1) * TILES)

    def positions(tile):
        return (first, second * TY + tile // TZ, third * TZ + tile % TZ)

    extents = (size_first, size_second * TY, size_third * TZ)

    def kept(tile):
        x, y, z = positions(tile)
        return jnp.where((x * extents[1] + y) * extents[2] + z != anchor[0], 1.0, 0.0)

    for y in range(TY):
        small[2 * y : 2 * y + 2, 0:COMPS] = affines[0, y]
    affine_columns = [
        small[:, a : a + 1] + (1.0 if a % 5 == 0 else 0.0) for a in range(COMPS)
    ]
    row = jnp.zeros((TILES, LANES), F32)
    for a in range(COMPS):
        row = row + jnp.where(eyes[a], affine_columns[a], 0.0)
    row = jnp.sum(row, axis=0, keepdims=True)
    row = jnp.where((lane[:1] >= ROWS) & (lane[:1] < WIDE), -SPACING, row)
    affine[...] = row

    pl.semaphore_wait(barrier, neighbours + (pair_size - 1 + size_first - 1))
    loads[0].wait()
    zeros = {1: (zero_one, spare_one), 2: (zero_two, spare_two), 16: (zero_share, spare_share)}
    ahead_there = [exists(shift) for shift in REACH[1:]]
    behind_there = [exists(tuple(-part for part in shift)) for shift in REACH[1:]]

    def fill(count, place, number, arrival, departure):
        nothing, spare = zeros[count]
        pltpu.make_async_copy(nothing, place, arrival).start()
        pltpu.make_async_copy(nothing, spare.at[number], departure).start()

    copies = {}
    for number, (index, shift, low, count, low_z, count_z) in enumerate(PIECES):
        at = (slice(None), index, pl.ds(low, count), pl.ds(low_z, count_z))
        copy = remote(
            target.at[(slice(None), index, 0, *at[2:])],
            moved.at[at],
            sent.at[number],
            got.at[number],
            device_at(shift, -1),
        )
        number = REACH.index(shift) - 1
        pl.when(behind_there[number])(copy.start)
        copies.setdefault(index, []).append((copy, number))
    affine_copies = []
    for number, shift in enumerate(REACH[1:]):
        at = len(PIECES) + number
        affine_copies.append(
            remote(affine, affine_there.at[number], sent.at[at], got.at[at], device_at(shift, -1))
        )
        pl.when(behind_there[number])(affine_copies[-1].start)

    for ref in (blocks, shares, own, packed):
        ref[...] = jnp.zeros_like(ref)
    points = here.shape[1]
    here[WIDE:, :] = jnp.zeros((LANES - WIDE, points), F32)
    there[ROWS:, :] = jnp.zeros((LANES - ROWS, points), F32)
    numbers = lax.broadcasted_iota(jnp.int32, (TILES, points), 1)
    tile_column = sub[:, 0:1]
    for load in loads[1:]:
        load.wait()
    for index in ORDER:
        offset = OFFSETS[index]
        for y in range(TY):
            for c in range(3):
                slab[c, 2 * y : 2 * y + 2, :] = source[c, index, 0, y]
                slab[3 + c, 2 * y : 2 * y + 2, :] = normal[c, index, 0, y]
            slab[6, 2 * y : 2 * y + 2, :] = weight[index, 0, y]
            small_count[2 * y : 2 * y + 2, :] = counts[0, y, :, index : index + 1]
        inside = functools.reduce(
            jnp.logical_and,
            [
                (p + o >= 0) & (p + o < extent)
                for p, o, extent in zip(positions(tile_column), offset, extents)
            ],
        )
        limit = jnp.where(inside, BLOCK * small_count[...], 0)
        share = jnp.where(numbers < limit, slab[6], 0.0)
        masked[index] = share
        for c in range(3):
            n = slab[3 + c]
            for e in range(4):
                at = (4 * c + e) * TILES
                a = n * slab[e] if e < 3 else n
                here[at : at + TILES, :] = a
                here_weighted[index, at : at + TILES, :] = a * share
        along = sum(part * slab[3 + c] for c, part in enumerate(offset) if part != 0)
        here[ROWS:WIDE, :] = along
        here_weighted[index, ROWS:WIDE, :] = along * share
        own[...] += cross(here_weighted[index, :ROWS, :], here[...])
    own[...] = jnp.where(tiled(same, COMPS), own[...], 0.0)

    for index in ORDER:
        offset = OFFSETS[index]
        for copy, number in copies.get(index, ()):
            pl.when(ahead_there[number])(copy.wait_recv)
        for y in range(TY):
            before = (y - offset[1]) % TY
            shift_y = (y - offset[1]) // TY
            for z in range(TZ):
                back = (z - offset[2]) % TZ
                shift_z = (z - offset[2]) // TZ
                to, come = y * TZ + z, before * TZ + back
                local = (offset[0], -shift_y, -shift_z) == SELF
                for c in range(3):
                    slab[6 + c, to : to + 1, :] = normal[c, index, 0, before, back : back + 1, :]
                    if local:
                        slab[9 + c, to : to + 1, :] = target[c, index, 0, y, z : z + 1, :]
                    else:
                        slab[9 + c, to : to + 1, :] = moved[c, index, y, z : z + 1, :]
                slab[12, to : to + 1, :] = masked[index, come : come + 1, :]
        share_there = slab[12]
        for c in range(3):
            m = slab[6 + c]
            for e in range(4):
                at = (4 * c + e) * TILES
                b = -(m * slab[9 + e]) if e < 3 else -m
                there[at : at + TILES, :] = b
                there_weighted[at : at + TILES, :] = b * share_there
        pair = cross(here_weighted[index], there[...])
        back = cross(there_weighted[...], there[...])
        for a in range(COMPS):
            packed[a : a + 1, :] = jnp.sum(
                jnp.where(same, back[group(a), :], 0.0), axis=0, keepdims=True
            )
        to_y, to_z = sub // TZ + offset[1], sub % TZ + offset[2]
        slot_y, slot_z = slot // TZ, slot % TZ
        all_slots = packed[...]
        for k, (pair_x, pair_z) in enumerate(PAIRS):
            ways = [w for w in shifts(offset) if (w[0], w[2]) == (pair_x, pair_z)]
            if not ways:
                continue
            meets = functools.reduce(
                jnp.logical_or, [slot_y + TY * w[1] == to_y for w in ways]
            ) & (slot_z + TZ * pair_z == to_z)
            blocks[k] += jnp.where(tiled(meets, WIDE // TILES), pair, 0.0)
        for shift in shifts(offset):
            j = REACH.index(shift)
            from_y, from_z = slot_y - offset[1] + TY * shift[1], slot_z - offset[2] + TZ * shift[2]
            owned = (from_y >= 0) & (from_y < TY) & (from_z >= 0) & (from_z < TZ)
            shares[j] += jnp.where(tiled(owned, 2), all_slots, 0.0)
    crossing_up = (sub // TZ == TY - 1) & (slot // TZ == 0)
    crossing_down = (sub // TZ == 0) & (slot // TZ == TY - 1)
    staying = jnp.logical_not(crossing_up | crossing_down)
    sides = {0: staying, 1: crossing_up, -1: crossing_down}

    def mixed(k, row_of):
        value = jnp.broadcast_to(row_of(MEMBERS[k][0]), (TILES, LANES))
        for side in (1, -1):
            if side in MEMBERS[k]:
                value = jnp.where(sides[side], row_of(MEMBERS[k][side]), value)
        return value

    def parted(k, total):
        return [
            (j, jnp.sum(jnp.where(sides[side], total, 0.0), axis=0, keepdims=True))
            for side, j in MEMBERS[k].items()
        ]

    extended = [*affine_columns, jnp.full((TILES, 1), -SPACING, F32)]
    for k in range(len(PAIRS)):
        total = jnp.zeros((TILES, LANES), F32)
        for a in range(COMPS + 1):
            total = total + blocks[k, group(a), :] * extended[a]
        for j, part in parted(k, total):
            shares[j, COMPS : COMPS + 1, :] = part
    for number, shift in enumerate(REACH[1:]):
        copy = remote(
            shares.at[number + 1],
            shares_there.at[number],
            share_sent,
            share_got,
            device_at(shift, 1),
        )
        pl.when(ahead_there[number])(copy.start)

        @pl.when(jnp.logical_not(behind_there[number]))
        def _(number=number):
            nothing = zeros[16][0]
            pltpu.make_async_copy(nothing, shares_there.at[number], share_got).start()

        @pl.when(jnp.logical_not(ahead_there[number]))
        def _(number=number):
            nothing, spare = zeros[16]
            pltpu.make_async_copy(nothing, spare.at[number], share_sent).start()

    for index in ORDER:
        for copy, number in copies.get(index, ()):
            pl.when(behind_there[number])(copy.wait_send)
    for number, copy in enumerate(affine_copies):
        pl.when(ahead_there[number])(copy.wait_recv)
        pl.when(behind_there[number])(copy.wait_send)

    keep_row, keep_one = kept(slot[:1]), kept(tile_column)
    keep_column = [keep_one] * COMPS
    mixes = [mixed(k, lambda j: affine_there[j - 1] if j else row) for k in range(len(PAIRS))]
    sums = []
    for a in range(COMPS):
        total = own[group(a), :] * row
        for k, mix in enumerate(mixes):
            total = total + blocks[k, group(a), :] * mix
        sums.append(total)
    everything = pltpu.make_async_copy(shares_there, shares_there, share_got)
    everything.wait()
    pltpu.make_async_copy(shares_there, shares_there, share_sent).wait()
    gathered = shares[0]
    for j in range(OTHERS):
        gathered = gathered + shares_there[j]
    right = []
    for a in range(COMPS):
        spread = jnp.where(same & (lane < ROWS), gathered[a : a + 1, :], 0.0)
        total = sums[a] + spread * row + jnp.where(eyes[a], gathered[COMPS : COMPS + 1, :], 0.0)
        right.append(-keep_column[a] * jnp.sum(total, axis=1, keepdims=True))
        mine = jnp.where(lane < ROWS, own[group(a), :], 0.0)
        compact = jnp.sum(mine, axis=0, keepdims=True) + gathered[a : a + 1, :]
        unit = jnp.where((lane[:1] >= a * TILES) & (lane[:1] < (a + 1) * TILES), 1.0, 0.0)
        compact = keep_row * (compact + DAMPING * unit) + (1.0 - keep_row) * unit
        picked = jnp.where(wide_lane // TILES == wide_sub, compact, 0.0)
        for by in (8, 16, 32, 64):
            picked = picked + pltpu.roll(picked, by, 1)
        matrix[a] = picked

    rows = [matrix[a] for a in range(COMPS)]
    for k in range(COMPS):
        factor = 1.0 / rows[k][k : k + 1, :]
        at_pivot = wide_sub == k
        pivot_row = jnp.where(at_pivot, factor, rows[k] * factor)
        for i in range(COMPS):
            if i != k:
                f = rows[i][k : k + 1, :]
                rows[i] = jnp.where(at_pivot, 0.0, rows[i]) - f * pivot_row
        rows[k] = pivot_row
    for a in range(COMPS):
        compact = jnp.sum(
            jnp.where(wide_lane // TILES == wide_sub, rows[a], 0.0), axis=0, keepdims=True
        )
        inverse[group(a), :] = jnp.where(same & (lane < ROWS), compact, 0.0)

    def as_row(col):
        total = jnp.zeros((TILES, LANES), F32)
        for a in range(COMPS):
            total = total + jnp.where(eyes[a], col[a], 0.0)
        return jnp.sum(total, axis=0, keepdims=True)

    def precondition(col):
        total = jnp.zeros((TILES, LANES), F32)
        for a in range(COMPS):
            total = total + inverse[group(a), :] * col[a]
        return jnp.sum(total, axis=0, keepdims=True)

    def couple(step, vectors, meanwhile=None):
        amount = len(vectors)
        for r, v in enumerate(vectors):
            send_rows[step][0, r : r + 1, :] = v
        for number, shift in enumerate(REACH[1:]):
            copy = remote(
                send_rows[step].at[0],
                got_rows[step].at[number],
                halo_sems.at[step, 0],
                halo_sems.at[step, 1],
                device_at(shift, -1),
            )
            empty = functools.partial(
                fill,
                amount,
                got_back[step].at[number],
                number,
                halo_sems.at[step, 3],
                halo_sems.at[step, 0],
            )
            either(behind_there[number], copy.start, empty)
        cols = [column(v) for v in vectors]
        local = [None] * amount
        for k in range(len(PAIRS)):
            totals = [jnp.zeros((TILES, LANES), F32) for _ in vectors]
            for a in range(COMPS):
                block = blocks[k, group(a), :]
                for r in range(amount):
                    totals[r] = totals[r] + block * cols[r][a]
            for r in range(amount):
                for j, part in parted(k, totals[r]):
                    if j == 0:
                        local[r] = part
                    else:
                        back_rows[step][j - 1, r : r + 1, :] = part
        for number, shift in enumerate(REACH[1:]):
            copy = remote(
                back_rows[step].at[number],
                got_back[step].at[number],
                halo_sems.at[step, 2],
                halo_sems.at[step, 3],
                device_at(shift, 1),
            )
            empty = functools.partial(
                fill,
                amount,
                got_rows[step].at[number],
                OTHERS + number,
                halo_sems.at[step, 1],
                halo_sems.at[step, 2],
            )
            either(ahead_there[number], copy.start, empty)
        if meanwhile is not None:
            meanwhile()
        rows_there, back_there = got_rows[step], got_back[step]
        pltpu.make_async_copy(rows_there, rows_there, halo_sems.at[step, 1]).wait()
        sums = [[None] * COMPS for _ in vectors]
        for k in range(len(PAIRS)):
            mixes = [
                mixed(k, lambda j, r=r, v=v: rows_there[j - 1, r : r + 1, :] if j else v)
                for r, v in enumerate(vectors)
            ]
            for a in range(COMPS):
                block = blocks[k, group(a), :]
                for r in range(amount):
                    part = block * mixes[r]
                    sums[r][a] = part if k == 0 else sums[r][a] + part
        pltpu.make_async_copy(back_there, back_there, halo_sems.at[step, 3]).wait()
        results = []
        for r in range(amount):
            came = local[r]
            for j in range(OTHERS):
                came = came + back_there[j, r : r + 1, :]
            results.append(
                [
                    keep_column[a]
                    * jnp.sum(sums[r][a] + jnp.where(eyes[a], came, 0.0), axis=1, keepdims=True)
                    for a in range(COMPS)
                ]
            )
        pltpu.make_async_copy(rows_there, rows_there, halo_sems.at[step, 0]).wait()
        pltpu.make_async_copy(back_there, back_there, halo_sems.at[step, 2]).wait()
        return results

    def pair_part(at):
        return pair_sum.at[at, pl.ds(0, pair_size - 1)]

    def line_part(at):
        return line_sum.at[at, pl.ds(0, size_first - 1)]

    def wait_for(part, sem):
        pltpu.make_async_copy(part, part, sem).wait()

    def start_sum(high, low, at):
        for row, value in ((0, high), (1, low)):
            pair_send[at, row : row + 1, :] = value
            pair_sum[at, in_pair, row : row + 1, :] = value

        @pl.loop(1, pair_size)
        def _(k):
            remote(
                pair_send.at[at],
                pair_sum.at[at, in_pair],
                sum_sems.at[at, 0],
                sum_sems.at[at, 1],
                pair_peer(k),
            ).start()

    def go_on_sum(at):
        wait_for(pair_part(at), sum_sems.at[at, 1])
        high, low = compensated([pair_sum[at, k] for k in range(pair_size)])
        for row, value in ((0, high), (1, low)):
            line_send[at, row : row + 1, :] = value
            line_sum[at, first, row : row + 1, :] = value

        @pl.loop(1, size_first)
        def _(k):
            remote(
                line_send.at[at],
                line_sum.at[at, first],
                sum_sems.at[at, 2],
                sum_sems.at[at, 3],
                line_peer(k),
            ).start()

    def end_sum(at):
        wait_for(line_part(at), sum_sems.at[at, 3])
        high, low = compensated([line_sum[at, k] for k in range(size_first)])
        wait_for(pair_part(at), sum_sems.at[at, 0])
        wait_for(line_part(at), sum_sems.at[at, 2])
        return tuple(jnp.broadcast_to(v, (TILES, LANES)) for v in (high, low))

    def largest(values):
        return jnp.max(jnp.abs(values), axis=1, keepdims=True)

    def gram(count, ys, zs):
        y_bound, z_bound = largest(ys), largest(zs)
        row_of, lane_of = iotas(ys.shape[0])
        high = low = jnp.zeros(ys.shape, F32)
        for j in range(count):
            at = (lane_of == row_of * count + j) & (row_of < count)
            product, error = exact_product(ys, zs[j : j + 1, :])
            h, l = lane_total(product, error, y_bound * z_bound[j : j + 1, :])
            high, low = jnp.where(at, h, high), jnp.where(at, l, low)
        return tuple(jnp.sum(v, axis=0, keepdims=True) for v in (high, low))

    def iterate(count, amount, at_p, at_r, high, low):
        major = jnp.zeros((TILES, LANES), jnp.int32)
        for k in range(1, count + 1):
            major = major + jnp.where(lane >= k * count, 1, 0)
        minor = lane - count * major

        def form(mask):
            return jnp.where(mask & (lane < count * count), 1.0, 0.0)

        g_bound = largest(high)

        def inner(x, y, bound):
            product, error = exact_product(x, y)
            values, small = exact_product(product, high)
            total = lane_total(values, small + (product * low + error * high), g_bound * bound)
            return total[0] + total[1]

        p_major, p_minor = form(major == at_p), form(minor == at_p)
        r_major, r_minor = form(major == at_r), form(minor == at_r)
        u_minor = jnp.zeros((TILES, LANES), F32)
        p_most = r_most = jnp.ones((TILES, 1), F32)
        product = inner(r_major, r_minor, r_most)
        for _ in range(amount):
            a_major = p_major + pltpu.roll(p_major, count, 1)
            a_minor = p_minor + pltpu.roll(p_minor, 1, 1)
            a_most = 2.0 * p_most
            alpha = product / inner(p_major, a_minor, p_most * a_most)
            u_minor = u_minor + alpha * p_minor
            r_major = r_major - alpha * a_major
            r_minor = r_minor - alpha * a_minor
            r_most = (r_most + jnp.abs(alpha) * a_most) * 1.01
            following = inner(r_major, r_minor, r_most * r_most)
            ratio = following / product
            p_major = r_major + ratio * p_major
            p_minor = r_minor + ratio * p_minor
            p_most = (r_most + jnp.abs(ratio) * p_most) * 1.01
            product = following
        return u_minor, r_minor, p_minor

    def combined(count, minor_form, vectors, by=0):
        both = jnp.concatenate([minor_form, minor_form], axis=0)
        weights = jnp.sum(
            jnp.where((wide_lane + by == wide_sub) & (wide_lane < count), both, 0.0),
            axis=1,
            keepdims=True,
        )
        return jnp.sum(weights * vectors, axis=0, keepdims=True)

    for ref in (chain, chain_lifted, basis, lifted):
        ref[...] = jnp.zeros_like(ref)
    chain[0:1, :] = as_row(right)
    chain_lifted[0:1, :] = precondition(right)

    def extend(step, places, ys, zs, meanwhile=None):
        found = couple(step, [zs[at : at + 1, :] for at in places], meanwhile)
        for at, col in zip(places, found):
            ys[at + 1 : at + 2, :] = as_row(col)
            zs[at + 1 : at + 2, :] = precondition(col)

    for step in range(first_steps):
        extend(step, [step], chain, chain_lifted)
    count = first_steps + 1
    start_sum(*gram(count, chain[0:8, :], chain_lifted[0:8, :]), 0)
    for step in range(first_steps, first_steps + ahead):
        extend(
            step,
            [step],
            chain,
            chain_lifted,
            functools.partial(go_on_sum, 0) if step == first_steps else None,
        )
    u_form, r_form, p_form = iterate(count, first_steps, 0, 0, *end_sum(0))
    ys, zs = chain[...], chain_lifted[...]
    part = combined(count, u_form, zs)
    at_r = second_steps + 1
    for begin, shape in ((0, p_form), (at_r, r_form)):
        for by in range(ahead + 1):
            at = begin + by
            basis[at : at + 1, :] = combined(count, shape, ys, by)
            lifted[at : at + 1, :] = combined(count, shape, zs, by)
    for step in range(first_steps + ahead, steps):
        degree = step - first_steps
        extend(step, [degree, at_r + degree][: amounts[step]], basis, lifted)
    count = 2 * second_steps + 1
    start_sum(*gram(count, basis[...], lifted[...]), 1)
    go_on_sum(1)
    u_form, r_form, _ = iterate(count, second_steps, 0, at_r, *end_sum(1))
    results = (
        (update, part + combined(count, u_form, lifted[...])),
        (residual, combined(count, r_form, basis[...])),
    )
    for out, row in results:
        spread = jnp.zeros((TILES, LANES), F32)
        for a, col in enumerate(column(row)):
            spread = jnp.where(lane == a, col, spread)
        small[...] = spread
        for y in range(TY):
            out[0, y] = small[2 * y : 2 * y + 2, 0:COMPS]


def finish_kernel(first, second, first_out, second_out, sems):
    copies = [
        pltpu.make_async_copy(first, first_out, sems.at[0]),
        pltpu.make_async_copy(second, second_out, sems.at[1]),
    ]
    for copy in copies:
        copy.start()
    for copy in copies:
        copy.wait()


def vmem(*shape):
    return pltpu.VMEM(shape, F32)


def on_device(source_points, target_points, normals, weights, blocks, affines, anchor):
    points = source_points.shape[5]
    dirs = len(OFFSETS)
    sizes = [lax.axis_size(a) for a in AXES]
    later = SECOND - AHEAD
    amounts = (1,) * (FIRST + AHEAD) + (2,) * (later - 1) + (1,)
    steps = len(amounts)
    pair_size = sizes[1] * sizes[2]
    anywhere = pl.BlockSpec(memory_space=pl.ANY)
    in_vmem = pl.BlockSpec(memory_space=pltpu.VMEM)
    in_smem = pl.BlockSpec(memory_space=pltpu.SMEM)
    copies = len(PIECES) + OTHERS
    dma = pltpu.SemaphoreType.DMA
    last = (1, 2, 3, 0)
    outs = pl.pallas_call(
        functools.partial(step_kernel, (FIRST, SECOND, AHEAD, amounts)),
        out_shape=(jax.ShapeDtypeStruct((1, TY, TZ, COMPS), F32),) * 2,
        in_specs=[anywhere] * 4 + [in_vmem] * 2 + [in_smem],
        out_specs=[in_vmem] * 2,
        scratch_shapes=[
            vmem(*source_points.shape),
            vmem(*target_points.shape),
            vmem(*normals.shape),
            vmem(*weights.shape),
            vmem(3, dirs, TY, TZ, points),
            vmem(1, LANES),
            vmem(OTHERS, 1, LANES),
            vmem(13, TILES, points),
            vmem(LANES, points),
            vmem(dirs, WIDE, points),
            vmem(LANES, points),
            vmem(ROWS, points),
            vmem(16, LANES),
            vmem(TILES, LANES),
            pltpu.VMEM((TILES, 1), jnp.int32),
            vmem(dirs, TILES, points),
            vmem(len(PAIRS), WIDE, LANES),
            vmem(OTHERS + 1, 16, LANES),
            vmem(ROWS, LANES),
            vmem(OTHERS, 16, LANES),
            vmem(COMPS, 16, LANES),
            vmem(ROWS, LANES),
            *[vmem(16, LANES)] * 4,
            vmem(2, pair_size, 2, LANES),
            vmem(2, sizes[0], 2, LANES),
            vmem(2, 2, LANES),
            vmem(2, 2, LANES),
            *[vmem(1, r, LANES) for r in amounts],
            *[vmem(OTHERS, r, LANES) for r in amounts],
            *[vmem(OTHERS, r, LANES) for r in amounts],
            *[vmem(OTHERS, r, LANES) for r in amounts],
            vmem(1, LANES),
            vmem(2, LANES),
            vmem(16, LANES),
            vmem(2 * OTHERS, 1, LANES),
            vmem(2 * OTHERS, 2, LANES),
            vmem(OTHERS, 16, LANES),
            dma((4,)),
            dma((copies,)),
            dma((copies,)),
            dma,
            dma,
            dma((steps, 4)),
            dma((2, 4)),
        ],
        compiler_params=pltpu.CompilerParams(
            collective_id=0, has_side_effects=True, vmem_limit_bytes=60 * 2**20
        ),
        name="step",
    )(
        source_points,
        target_points,
        normals,
        weights,
        jnp.transpose(blocks, last),
        jnp.transpose(affines, last),
        anchor,
    )
    outs = pl.pallas_call(
        finish_kernel,
        out_shape=tuple(jax.ShapeDtypeStruct(out.shape, F32) for out in outs),
        in_specs=[anywhere] * 2,
        out_specs=[anywhere] * 2,
        scratch_shapes=[dma((2,))],
        name="finish",
    )(*outs)
    return tuple(jnp.transpose(out, (3, 0, 1, 2)) for out in outs)


def solution(mesh):
    placed = (
        P(None, None, "gx", "gy", "gz", None),
        P(None, None, "gx", "gy", "gz", None),
        P(None, None, "gx", "gy", "gz", None),
        P(None, "gx", "gy", "gz", None),
        P(None, "gx", "gy", "gz"),
        P(None, "gx", "gy", "gz"),
        P(),
    )
    return jax.shard_map(
        on_device,
        mesh=mesh,
        in_specs=placed,
        out_specs=(P(None, "gx", "gy", "gz"), P(None, "gx", "gy", "gz")),
        check_vma=False,
    )
```

```python
import functools

import jax
import jax.numpy as jnp
from jax import lax
from jax.experimental import pallas as pl
from jax.experimental.pallas import tpu as pltpu
from jax.sharding import PartitionSpec as P

BLOCK = 256
FIRST, SECOND, AHEAD = 5, 5, 2
SPACING = 0.5
DAMPING = 1.0
OFFSETS = (
    (1, 0, 0),
    (0, 1, 0),
    (0, 0, 1),
    (1, 1, -1),
    (1, -1, 1),
    (-1, 1, 1),
    (1, 1, 0),
    (1, 0, 1),
    (0, 1, 1),
    (1, 1, 1),
    (1, -1, 0),
    (0, 1, -1),
    (-1, 0, 1),
)
AXES = ("gx", "gy", "gz")
MESH = pl.DeviceIdType.MESH
LANES = 128
TY, TZ, TILES = 4, 2, 8
COMPS = 12
ROWS = COMPS * TILES
WIDE = ROWS + TILES
F32 = jnp.float32


def shifts(offset):
    seconds = (0,) if offset[1] == 0 else (0, offset[1])
    thirds = (0,) if offset[2] == 0 else (0, offset[2])
    return [(offset[0], y, z) for y in seconds for z in thirds]


SELF = (0, 0, 0)
REACH = (
    SELF,
    *sorted(
        {s for o in OFFSETS for s in shifts(o)} - {SELF}, key=lambda s: (-sum(map(abs, s)), s)
    ),
)
OTHERS = len(REACH) - 1
PAIRS = tuple(dict.fromkeys((s[0], s[2]) for s in REACH))
MEMBERS = tuple({s[1]: REACH.index(s) for s in REACH if (s[0], s[2]) == pair} for pair in PAIRS)
GREET = tuple(sorted({s for s in REACH[1:]} | {tuple(-p for p in s) for s in REACH[1:]}))


def spans(part, shift, length):
    if part == 0:
        return 0, length
    if shift == 0:
        return (1 if part > 0 else 0), length - 1
    return (0 if part > 0 else length - 1), 1


ORDER = tuple(sorted(range(len(OFFSETS)), key=lambda d: ((0, 2, 1)[OFFSETS[d][0]], d)))
PIECES = tuple(
    (d, s, *spans(OFFSETS[d][1], s[1], TY), *spans(OFFSETS[d][2], s[2], TZ))
    for d in ORDER
    for s in shifts(OFFSETS[d])
    if s != SELF
)


def device_at(shift, sign):
    there = []
    for axis, part in zip(AXES, shift):
        size = lax.axis_size(axis)
        there.append(lax.rem(lax.axis_index(axis) + (sign * part + size), size))
    return tuple(there)


def exists(shift):
    found = True
    for axis, part in zip(AXES, shift):
        if part > 0:
            found = jnp.logical_and(lax.axis_index(axis) + part < lax.axis_size(axis), found)
        elif part < 0:
            found = jnp.logical_and(lax.axis_index(axis) + part >= 0, found)
    return found


def either(condition, then, otherwise):
    lax.cond(condition, lambda: (then(), None)[1], lambda: (otherwise(), None)[1])


def remote(source, target, sent, got, device):
    return pltpu.make_async_remote_copy(
        src_ref=source,
        dst_ref=target,
        send_sem=sent,
        recv_sem=got,
        device_id=device,
        device_id_type=MESH,
    )


def iotas(rows=TILES):
    return (
        lax.broadcasted_iota(jnp.int32, (rows, LANES), 0),
        lax.broadcasted_iota(jnp.int32, (rows, LANES), 1),
    )


def tiled(mask, times):
    return jnp.concatenate([mask] * times, axis=0)


def cross(left, right):
    return lax.dot_general(
        left,
        right,
        (((1,), (1,)), ((), ())),
        precision=lax.Precision.HIGHEST,
        preferred_element_type=F32,
    )


def halves(x):
    top = x.astype(jnp.bfloat16)
    return top, (x - top.astype(F32)).astype(jnp.bfloat16)


def narrow_cross(left, right):
    return lax.dot_general(
        left, right, (((1,), (1,)), ((), ())), preferred_element_type=F32
    )


def cross_of(left_top, left_rest, right):
    top, rest = halves(right)
    both = narrow_cross(jnp.concatenate([left_top, left_rest], axis=0), top)
    count = left_top.shape[0]
    return both[:count] + (both[count:] + narrow_cross(left_top, rest))


def split(x):
    big = x * 4097.0
    high = big - (big - x)
    return high, x - high


def exact_product(x, y):
    (xh, xl), (yh, yl) = split(x), split(y)
    product = x * y
    return product, ((xh * yh - product) + xh * yl + xl * yh) + xl * yl


def lane_total(values, small, bound):
    grid = bound * 256.0
    top = (values + grid) - grid
    rest = values - top
    grid = grid * 2.0**-16
    middle = (rest + grid) - grid
    small = small + (rest - middle)
    top, middle, small = (jnp.sum(v, axis=1, keepdims=True) for v in (top, middle, small))
    high = top + middle
    back = high - top
    return high, ((top - (high - back)) + (middle - back)) + small


def compensated(parts):
    total, error = parts[0], jnp.zeros_like(parts[0])
    for part in parts[1:]:
        following = total + part
        back = following - total
        error = error + ((total - (following - back)) + (part - back))
        total = following
    high, low = total[0:1], error[0:1] + total[1:2]
    both = high + low
    return both, low - (both - high)


def step_kernel(plan, *refs):
    first_steps, second_steps, ahead, amounts = plan
    steps = len(amounts)
    source_out, target_out, normal_out, weight_out, counts, affines, anchor = refs[:7]
    update, residual = refs[7:9]
    source, target, normal, weight, moved, affine, affine_there = refs[9:16]
    slab, here, here_weighted, there, packed, small = refs[16:22]
    small_count, masked, blocks, shares, own = refs[22:27]
    shares_there, matrix, inverse, chain, chain_lifted, basis, lifted = refs[27:34]
    pair_sum, line_sum, pair_send, line_send = refs[34:38]
    rest = refs[38:]
    send_rows, got_rows, back_rows, got_back = (rest[k * steps : (k + 1) * steps] for k in range(4))
    zero_one, zero_two, zero_share, spare_one, spare_two, spare_share = rest[4 * steps :][:6]
    loaded, sent, got, share_sent, share_got, halo_sems, sum_sems = rest[4 * steps + 6 :]
    loads = [
        pltpu.make_async_copy(outer, ref, loaded.at[number])
        for number, (outer, ref) in enumerate(
            (
                (target_out, target),
                (source_out, source),
                (normal_out, normal),
                (weight_out, weight),
            )
        )
    ]
    for load in loads:
        load.start()
    first, second, third = (lax.axis_index(a) for a in AXES)
    size_first, size_second, size_third = (lax.axis_size(a) for a in AXES)
    in_pair = second * size_third + third
    pair_size = size_second * size_third

    def pair_peer(k):
        there = lax.rem(in_pair + k, pair_size)
        return (first, there // size_third, lax.rem(there, size_third))

    def line_peer(k):
        return (lax.rem(first + k, size_first), second, third)

    barrier = pltpu.get_barrier_semaphore()
    for ref in (moved, affine_there, zero_one, zero_two, zero_share):
        ref[...] = jnp.zeros_like(ref)
    neighbours = 0
    for shift in GREET:
        near = exists(shift)
        neighbours = neighbours + jnp.where(near, 1, 0)

        @pl.when(near)
        def _(shift=shift):
            pl.semaphore_signal(barrier, inc=1, device_id=device_at(shift, 1), device_id_type=MESH)


    @pl.loop(1, pair_size)
    def _(k):
        pl.semaphore_signal(barrier, inc=1, device_id=pair_peer(k), device_id_type=MESH)

    @pl.loop(1, size_first)
    def _(k):
        pl.semaphore_signal(barrier, inc=1, device_id=line_peer(k), device_id_type=MESH)

    sub, lane = iotas()
    slot = lane & (TILES - 1)
    same = sub == slot
    eyes = [lane == sub + a * TILES for a in range(COMPS)]
    wide_sub, wide_lane = iotas(16)

    def column(row):
        return [jnp.sum(jnp.where(eyes[a], row, 0.0), axis=1, keepdims=True) for a in range(COMPS)]

    def group(a):
        return slice(a * TILES, (a + 1) * TILES)

    def positions(tile):
        return (first, second * TY + tile // TZ, third * TZ + tile % TZ)

    extents = (size_first, size_second * TY, size_third * TZ)

    def kept(tile):
        x, y, z = positions(tile)
        return jnp.where((x * extents[1] + y) * extents[2] + z != anchor[0], 1.0, 0.0)

    for y in range(TY):
        small[2 * y : 2 * y + 2, 0:COMPS] = affines[0, y]
    affine_columns = [
        small[:, a : a + 1] + (1.0 if a % 5 == 0 else 0.0) for a in range(COMPS)
    ]
    row = jnp.zeros((TILES, LANES), F32)
    for a in range(COMPS):
        row = row + jnp.where(eyes[a], affine_columns[a], 0.0)
    row = jnp.sum(row, axis=0, keepdims=True)
    row = jnp.where((lane[:1] >= ROWS) & (lane[:1] < WIDE), -SPACING, row)
    affine[...] = row

    pl.semaphore_wait(barrier, neighbours + (pair_size - 1 + size_first - 1))
    loads[0].wait()
    zeros = {1: (zero_one, spare_one), 2: (zero_two, spare_two), 16: (zero_share, spare_share)}
    ahead_there = [exists(shift) for shift in REACH[1:]]
    behind_there = [exists(tuple(-part for part in shift)) for shift in REACH[1:]]

    def fill(count, place, number, arrival, departure):
        nothing, spare = zeros[count]
        pltpu.make_async_copy(nothing, place, arrival).start()
        pltpu.make_async_copy(nothing, spare.at[number], departure).start()

    copies = {}
    for number, (index, shift, low, count, low_z, count_z) in enumerate(PIECES):
        at = (slice(None), index, pl.ds(low, count), pl.ds(low_z, count_z))
        copy = remote(
            target.at[(slice(None), index, 0, *at[2:])],
            moved.at[at],
            sent.at[number],
            got.at[number],
            device_at(shift, -1),
        )
        number = REACH.index(shift) - 1
        pl.when(behind_there[number])(copy.start)
        copies.setdefault(index, []).append((copy, number))
    affine_copies = []
    for number, shift in enumerate(REACH[1:]):
        at = len(PIECES) + number
        affine_copies.append(
            remote(affine, affine_there.at[number], sent.at[at], got.at[at], device_at(shift, -1))
        )
        pl.when(behind_there[number])(affine_copies[-1].start)

    for ref in (blocks, shares, own, packed):
        ref[...] = jnp.zeros_like(ref)
    points = here.shape[1]
    here[WIDE:, :] = jnp.zeros((LANES - WIDE, points), F32)
    there[ROWS:, :] = jnp.zeros((LANES - ROWS, points), F32)
    for index in ORDER:
        here_weighted[index, WIDE + ROWS :, :] = jnp.zeros((TILES, points), F32)
    numbers = lax.broadcasted_iota(jnp.int32, (TILES, points), 1)
    tile_column = sub[:, 0:1]
    for load in loads[1:]:
        load.wait()
    for index in ORDER:
        offset = OFFSETS[index]
        for y in range(TY):
            for c in range(3):
                slab[c, 2 * y : 2 * y + 2, :] = source[c, index, 0, y]
                slab[3 + c, 2 * y : 2 * y + 2, :] = normal[c, index, 0, y]
            slab[6, 2 * y : 2 * y + 2, :] = weight[index, 0, y]
            small_count[2 * y : 2 * y + 2, :] = counts[0, y, :, index : index + 1]
        inside = functools.reduce(
            jnp.logical_and,
            [
                (p + o >= 0) & (p + o < extent)
                for p, o, extent in zip(positions(tile_column), offset, extents)
            ],
        )
        limit = jnp.where(inside, BLOCK * small_count[...], 0)
        share = jnp.where(numbers < limit, slab[6], 0.0)
        masked[index] = share
        for c in range(3):
            n = slab[3 + c]
            for e in range(4):
                at = (4 * c + e) * TILES
                a = n * slab[e] if e < 3 else n
                here[at : at + TILES, :] = a
                here_weighted[index, at : at + TILES, :] = a * share
        along = sum(part * slab[3 + c] for c, part in enumerate(offset) if part != 0)
        here[ROWS:WIDE, :] = along
        here_weighted[index, ROWS:WIDE, :] = along * share
        own[...] += cross_of(*halves(here_weighted[index, :ROWS, :]), here[...])
    own[...] = jnp.where(tiled(same, COMPS), own[...], 0.0)

    for index in ORDER:
        offset = OFFSETS[index]
        for copy, number in copies.get(index, ()):
            pl.when(ahead_there[number])(copy.wait_recv)
        for y in range(TY):
            before = (y - offset[1]) % TY
            shift_y = (y - offset[1]) // TY
            for z in range(TZ):
                back = (z - offset[2]) % TZ
                shift_z = (z - offset[2]) // TZ
                to, come = y * TZ + z, before * TZ + back
                local = (offset[0], -shift_y, -shift_z) == SELF
                for c in range(3):
                    slab[6 + c, to : to + 1, :] = normal[c, index, 0, before, back : back + 1, :]
                    if local:
                        slab[9 + c, to : to + 1, :] = target[c, index, 0, y, z : z + 1, :]
                    else:
                        slab[9 + c, to : to + 1, :] = moved[c, index, y, z : z + 1, :]
                slab[12, to : to + 1, :] = masked[index, come : come + 1, :]
        share_there = slab[12]
        for c in range(3):
            m = slab[6 + c]
            for e in range(4):
                at = (4 * c + e) * TILES
                b = -(m * slab[9 + e]) if e < 3 else -m
                there[at : at + TILES, :] = b
                here_weighted[index, WIDE + at : WIDE + at + TILES, :] = b * share_there
        both = cross_of(*halves(here_weighted[index]), there[...])
        pair, back = both[:WIDE], both[WIDE : WIDE + ROWS]
        for a in range(COMPS):
            packed[a : a + 1, :] = jnp.sum(
                jnp.where(same, back[group(a), :], 0.0), axis=0, keepdims=True
            )
        to_y, to_z = sub // TZ + offset[1], sub % TZ + offset[2]
        slot_y, slot_z = slot // TZ, slot % TZ
        all_slots = packed[...]
        for k, (pair_x, pair_z) in enumerate(PAIRS):
            ways = [w for w in shifts(offset) if (w[0], w[2]) == (pair_x, pair_z)]
            if not ways:
                continue
            meets = functools.reduce(
                jnp.logical_or, [slot_y + TY * w[1] == to_y for w in ways]
            ) & (slot_z + TZ * pair_z == to_z)
            blocks[k] += jnp.where(tiled(meets, WIDE // TILES), pair, 0.0)
        for shift in shifts(offset):
            j = REACH.index(shift)
            from_y, from_z = slot_y - offset[1] + TY * shift[1], slot_z - offset[2] + TZ * shift[2]
            owned = (from_y >= 0) & (from_y < TY) & (from_z >= 0) & (from_z < TZ)
            shares[j] += jnp.where(tiled(owned, 2), all_slots, 0.0)
    crossing_up = (sub // TZ == TY - 1) & (slot // TZ == 0)
    crossing_down = (sub // TZ == 0) & (slot // TZ == TY - 1)
    staying = jnp.logical_not(crossing_up | crossing_down)
    sides = {0: staying, 1: crossing_up, -1: crossing_down}

    def mixed(k, row_of):
        value = jnp.broadcast_to(row_of(MEMBERS[k][0]), (TILES, LANES))
        for side in (1, -1):
            if side in MEMBERS[k]:
                value = jnp.where(sides[side], row_of(MEMBERS[k][side]), value)
        return value

    def parted(k, total):
        return [
            (j, jnp.sum(jnp.where(sides[side], total, 0.0), axis=0, keepdims=True))
            for side, j in MEMBERS[k].items()
        ]

    extended = [*affine_columns, jnp.full((TILES, 1), -SPACING, F32)]
    for k in range(len(PAIRS)):
        total = jnp.zeros((TILES, LANES), F32)
        for a in range(COMPS + 1):
            total = total + blocks[k, group(a), :] * extended[a]
        for j, part in parted(k, total):
            shares[j, COMPS : COMPS + 1, :] = part
    for number, shift in enumerate(REACH[1:]):
        copy = remote(
            shares.at[number + 1],
            shares_there.at[number],
            share_sent,
            share_got,
            device_at(shift, 1),
        )
        pl.when(ahead_there[number])(copy.start)

        @pl.when(jnp.logical_not(behind_there[number]))
        def _(number=number):
            nothing = zeros[16][0]
            pltpu.make_async_copy(nothing, shares_there.at[number], share_got).start()

        @pl.when(jnp.logical_not(ahead_there[number]))
        def _(number=number):
            nothing, spare = zeros[16]
            pltpu.make_async_copy(nothing, spare.at[number], share_sent).start()

    for index in ORDER:
        for copy, number in copies.get(index, ()):
            pl.when(behind_there[number])(copy.wait_send)
    for number, copy in enumerate(affine_copies):
        pl.when(ahead_there[number])(copy.wait_recv)
        pl.when(behind_there[number])(copy.wait_send)

    keep_row, keep_one = kept(slot[:1]), kept(tile_column)
    keep_column = [keep_one] * COMPS
    mixes = [mixed(k, lambda j: affine_there[j - 1] if j else row) for k in range(len(PAIRS))]
    sums = []
    for a in range(COMPS):
        total = own[group(a), :] * row
        for k, mix in enumerate(mixes):
            total = total + blocks[k, group(a), :] * mix
        sums.append(total)
    everything = pltpu.make_async_copy(shares_there, shares_there, share_got)
    everything.wait()
    pltpu.make_async_copy(shares_there, shares_there, share_sent).wait()
    gathered = shares[0]
    for j in range(OTHERS):
        gathered = gathered + shares_there[j]
    right = []
    for a in range(COMPS):
        spread = jnp.where(same & (lane < ROWS), gathered[a : a + 1, :], 0.0)
        total = sums[a] + spread * row + jnp.where(eyes[a], gathered[COMPS : COMPS + 1, :], 0.0)
        right.append(-keep_column[a] * jnp.sum(total, axis=1, keepdims=True))
        mine = jnp.where(lane < ROWS, own[group(a), :], 0.0)
        compact = jnp.sum(mine, axis=0, keepdims=True) + gathered[a : a + 1, :]
        unit = jnp.where((lane[:1] >= a * TILES) & (lane[:1] < (a + 1) * TILES), 1.0, 0.0)
        compact = keep_row * (compact + DAMPING * unit) + (1.0 - keep_row) * unit
        picked = jnp.where(wide_lane // TILES == wide_sub, compact, 0.0)
        for by in (8, 16, 32, 64):
            picked = picked + pltpu.roll(picked, by, 1)
        matrix[a] = picked

    rows = [matrix[a] for a in range(COMPS)]
    for k in range(COMPS):
        factor = 1.0 / rows[k][k : k + 1, :]
        at_pivot = wide_sub == k
        pivot_row = jnp.where(at_pivot, factor, rows[k] * factor)
        for i in range(COMPS):
            if i != k:
                f = rows[i][k : k + 1, :]
                rows[i] = jnp.where(at_pivot, 0.0, rows[i]) - f * pivot_row
        rows[k] = pivot_row
    for a in range(COMPS):
        compact = jnp.sum(
            jnp.where(wide_lane // TILES == wide_sub, rows[a], 0.0), axis=0, keepdims=True
        )
        inverse[group(a), :] = jnp.where(same & (lane < ROWS), compact, 0.0)

    def as_row(col):
        total = jnp.zeros((TILES, LANES), F32)
        for a in range(COMPS):
            total = total + jnp.where(eyes[a], col[a], 0.0)
        return jnp.sum(total, axis=0, keepdims=True)

    def precondition(col):
        total = jnp.zeros((TILES, LANES), F32)
        for a in range(COMPS):
            total = total + inverse[group(a), :] * col[a]
        return jnp.sum(total, axis=0, keepdims=True)

    def couple(step, vectors, meanwhile=None):
        amount = len(vectors)
        for r, v in enumerate(vectors):
            send_rows[step][0, r : r + 1, :] = v
        for number, shift in enumerate(REACH[1:]):
            copy = remote(
                send_rows[step].at[0],
                got_rows[step].at[number],
                halo_sems.at[step, 0],
                halo_sems.at[step, 1],
                device_at(shift, -1),
            )
            empty = functools.partial(
                fill,
                amount,
                got_back[step].at[number],
                number,
                halo_sems.at[step, 3],
                halo_sems.at[step, 0],
            )
            either(behind_there[number], copy.start, empty)
        cols = [column(v) for v in vectors]
        local = [None] * amount
        for k in range(len(PAIRS)):
            totals = [jnp.zeros((TILES, LANES), F32) for _ in vectors]
            for a in range(COMPS):
                block = blocks[k, group(a), :]
                for r in range(amount):
                    totals[r] = totals[r] + block * cols[r][a]
            for r in range(amount):
                for j, part in parted(k, totals[r]):
                    if j == 0:
                        local[r] = part
                    else:
                        back_rows[step][j - 1, r : r + 1, :] = part
        for number, shift in enumerate(REACH[1:]):
            copy = remote(
                back_rows[step].at[number],
                got_back[step].at[number],
                halo_sems.at[step, 2],
                halo_sems.at[step, 3],
                device_at(shift, 1),
            )
            empty = functools.partial(
                fill,
                amount,
                got_rows[step].at[number],
                OTHERS + number,
                halo_sems.at[step, 1],
                halo_sems.at[step, 2],
            )
            either(ahead_there[number], copy.start, empty)
        if meanwhile is not None:
            meanwhile()
        rows_there, back_there = got_rows[step], got_back[step]
        pltpu.make_async_copy(rows_there, rows_there, halo_sems.at[step, 1]).wait()
        sums = [[None] * COMPS for _ in vectors]
        for k in range(len(PAIRS)):
            mixes = [
                mixed(k, lambda j, r=r, v=v: rows_there[j - 1, r : r + 1, :] if j else v)
                for r, v in enumerate(vectors)
            ]
            for a in range(COMPS):
                block = blocks[k, group(a), :]
                for r in range(amount):
                    part = block * mixes[r]
                    sums[r][a] = part if k == 0 else sums[r][a] + part
        pltpu.make_async_copy(back_there, back_there, halo_sems.at[step, 3]).wait()
        results = []
        for r in range(amount):
            came = local[r]
            for j in range(OTHERS):
                came = came + back_there[j, r : r + 1, :]
            results.append(
                [
                    keep_column[a]
                    * jnp.sum(sums[r][a] + jnp.where(eyes[a], came, 0.0), axis=1, keepdims=True)
                    for a in range(COMPS)
                ]
            )
        pltpu.make_async_copy(rows_there, rows_there, halo_sems.at[step, 0]).wait()
        pltpu.make_async_copy(back_there, back_there, halo_sems.at[step, 2]).wait()
        return results

    def pair_part(at):
        return pair_sum.at[at, pl.ds(0, pair_size - 1)]

    def line_part(at):
        return line_sum.at[at, pl.ds(0, size_first - 1)]

    def wait_for(part, sem):
        pltpu.make_async_copy(part, part, sem).wait()

    def start_sum(high, low, at):
        for row, value in ((0, high), (1, low)):
            pair_send[at, row : row + 1, :] = value
            pair_sum[at, in_pair, row : row + 1, :] = value

        @pl.loop(1, pair_size)
        def _(k):
            remote(
                pair_send.at[at],
                pair_sum.at[at, in_pair],
                sum_sems.at[at, 0],
                sum_sems.at[at, 1],
                pair_peer(k),
            ).start()

    def go_on_sum(at):
        wait_for(pair_part(at), sum_sems.at[at, 1])
        high, low = compensated([pair_sum[at, k] for k in range(pair_size)])
        for row, value in ((0, high), (1, low)):
            line_send[at, row : row + 1, :] = value
            line_sum[at, first, row : row + 1, :] = value

        @pl.loop(1, size_first)
        def _(k):
            remote(
                line_send.at[at],
                line_sum.at[at, first],
                sum_sems.at[at, 2],
                sum_sems.at[at, 3],
                line_peer(k),
            ).start()

    def end_sum(at):
        wait_for(line_part(at), sum_sems.at[at, 3])
        high, low = compensated([line_sum[at, k] for k in range(size_first)])
        wait_for(pair_part(at), sum_sems.at[at, 0])
        wait_for(line_part(at), sum_sems.at[at, 2])
        return tuple(jnp.broadcast_to(v, (TILES, LANES)) for v in (high, low))

    def largest(values):
        return jnp.max(jnp.abs(values), axis=1, keepdims=True)

    def gram(count, ys, zs):
        y_bound, z_bound = largest(ys), largest(zs)
        row_of, lane_of = iotas(ys.shape[0])
        high = low = jnp.zeros(ys.shape, F32)
        for j in range(count):
            at = (lane_of == row_of * count + j) & (row_of < count)
            product, error = exact_product(ys, zs[j : j + 1, :])
            h, l = lane_total(product, error, y_bound * z_bound[j : j + 1, :])
            high, low = jnp.where(at, h, high), jnp.where(at, l, low)
        return tuple(jnp.sum(v, axis=0, keepdims=True) for v in (high, low))

    def iterate(count, amount, at_p, at_r, high, low):
        major = jnp.zeros((TILES, LANES), jnp.int32)
        for k in range(1, count + 1):
            major = major + jnp.where(lane >= k * count, 1, 0)
        minor = lane - count * major

        def form(mask):
            return jnp.where(mask & (lane < count * count), 1.0, 0.0)

        g_bound = largest(high)

        def inner(x, y, bound):
            product, error = exact_product(x, y)
            values, small = exact_product(product, high)
            total = lane_total(values, small + (product * low + error * high), g_bound * bound)
            return total[0] + total[1]

        p_major, p_minor = form(major == at_p), form(minor == at_p)
        r_major, r_minor = form(major == at_r), form(minor == at_r)
        u_minor = jnp.zeros((TILES, LANES), F32)
        p_most = r_most = jnp.ones((TILES, 1), F32)
        product = inner(r_major, r_minor, r_most)
        for _ in range(amount):
            a_major = p_major + pltpu.roll(p_major, count, 1)
            a_minor = p_minor + pltpu.roll(p_minor, 1, 1)
            a_most = 2.0 * p_most
            alpha = product / inner(p_major, a_minor, p_most * a_most)
            u_minor = u_minor + alpha * p_minor
            r_major = r_major - alpha * a_major
            r_minor = r_minor - alpha * a_minor
            r_most = (r_most + jnp.abs(alpha) * a_most) * 1.01
            following = inner(r_major, r_minor, r_most * r_most)
            ratio = following / product
            p_major = r_major + ratio * p_major
            p_minor = r_minor + ratio * p_minor
            p_most = (r_most + jnp.abs(ratio) * p_most) * 1.01
            product = following
        return u_minor, r_minor, p_minor

    def combined(count, minor_form, vectors, by=0):
        both = jnp.concatenate([minor_form, minor_form], axis=0)
        weights = jnp.sum(
            jnp.where((wide_lane + by == wide_sub) & (wide_lane < count), both, 0.0),
            axis=1,
            keepdims=True,
        )
        return jnp.sum(weights * vectors, axis=0, keepdims=True)

    for ref in (chain, chain_lifted, basis, lifted):
        ref[...] = jnp.zeros_like(ref)
    chain[0:1, :] = as_row(right)
    chain_lifted[0:1, :] = precondition(right)

    def extend(step, places, ys, zs, meanwhile=None):
        found = couple(step, [zs[at : at + 1, :] for at in places], meanwhile)
        for at, col in zip(places, found):
            ys[at + 1 : at + 2, :] = as_row(col)
            zs[at + 1 : at + 2, :] = precondition(col)

    for step in range(first_steps):
        extend(step, [step], chain, chain_lifted)
    count = first_steps + 1
    start_sum(*gram(count, chain[0:8, :], chain_lifted[0:8, :]), 0)
    for step in range(first_steps, first_steps + ahead):
        extend(
            step,
            [step],
            chain,
            chain_lifted,
            functools.partial(go_on_sum, 0) if step == first_steps else None,
        )
    u_form, r_form, p_form = iterate(count, first_steps, 0, 0, *end_sum(0))
    ys, zs = chain[...], chain_lifted[...]
    part = combined(count, u_form, zs)
    at_r = second_steps + 1
    for begin, shape in ((0, p_form), (at_r, r_form)):
        for by in range(ahead + 1):
            at = begin + by
            basis[at : at + 1, :] = combined(count, shape, ys, by)
            lifted[at : at + 1, :] = combined(count, shape, zs, by)
    for step in range(first_steps + ahead, steps):
        degree = step - first_steps
        extend(step, [degree, at_r + degree][: amounts[step]], basis, lifted)
    count = 2 * second_steps + 1
    start_sum(*gram(count, basis[...], lifted[...]), 1)
    go_on_sum(1)
    u_form, r_form, _ = iterate(count, second_steps, 0, at_r, *end_sum(1))
    results = (
        (update, part + combined(count, u_form, lifted[...])),
        (residual, combined(count, r_form, basis[...])),
    )
    for out, row in results:
        spread = jnp.zeros((TILES, LANES), F32)
        for a, col in enumerate(column(row)):
            spread = jnp.where(lane == a, col, spread)
        small[...] = spread
        for y in range(TY):
            out[0, y] = small[2 * y : 2 * y + 2, 0:COMPS]


def finish_kernel(first, second, first_out, second_out, sems):
    copies = [
        pltpu.make_async_copy(first, first_out, sems.at[0]),
        pltpu.make_async_copy(second, second_out, sems.at[1]),
    ]
    for copy in copies:
        copy.start()
    for copy in copies:
        copy.wait()


def vmem(*shape):
    return pltpu.VMEM(shape, F32)


def on_device(source_points, target_points, normals, weights, blocks, affines, anchor):
    points = source_points.shape[5]
    dirs = len(OFFSETS)
    sizes = [lax.axis_size(a) for a in AXES]
    later = SECOND - AHEAD
    amounts = (1,) * (FIRST + AHEAD) + (2,) * (later - 1) + (1,)
    steps = len(amounts)
    pair_size = sizes[1] * sizes[2]
    anywhere = pl.BlockSpec(memory_space=pl.ANY)
    in_vmem = pl.BlockSpec(memory_space=pltpu.VMEM)
    in_smem = pl.BlockSpec(memory_space=pltpu.SMEM)
    copies = len(PIECES) + OTHERS
    dma = pltpu.SemaphoreType.DMA
    last = (1, 2, 3, 0)
    outs = pl.pallas_call(
        functools.partial(step_kernel, (FIRST, SECOND, AHEAD, amounts)),
        out_shape=(jax.ShapeDtypeStruct((1, TY, TZ, COMPS), F32),) * 2,
        in_specs=[anywhere] * 4 + [in_vmem] * 2 + [in_smem],
        out_specs=[in_vmem] * 2,
        scratch_shapes=[
            vmem(*source_points.shape),
            vmem(*target_points.shape),
            vmem(*normals.shape),
            vmem(*weights.shape),
            vmem(3, dirs, TY, TZ, points),
            vmem(1, LANES),
            vmem(OTHERS, 1, LANES),
            vmem(13, TILES, points),
            vmem(LANES, points),
            vmem(dirs, WIDE + ROWS + TILES, points),
            vmem(LANES, points),
            vmem(16, LANES),
            vmem(TILES, LANES),
            pltpu.VMEM((TILES, 1), jnp.int32),
            vmem(dirs, TILES, points),
            vmem(len(PAIRS), WIDE, LANES),
            vmem(OTHERS + 1, 16, LANES),
            vmem(ROWS, LANES),
            vmem(OTHERS, 16, LANES),
            vmem(COMPS, 16, LANES),
            vmem(ROWS, LANES),
            *[vmem(16, LANES)] * 4,
            vmem(2, pair_size, 2, LANES),
            vmem(2, sizes[0], 2, LANES),
            vmem(2, 2, LANES),
            vmem(2, 2, LANES),
            *[vmem(1, r, LANES) for r in amounts],
            *[vmem(OTHERS, r, LANES) for r in amounts],
            *[vmem(OTHERS, r, LANES) for r in amounts],
            *[vmem(OTHERS, r, LANES) for r in amounts],
            vmem(1, LANES),
            vmem(2, LANES),
            vmem(16, LANES),
            vmem(2 * OTHERS, 1, LANES),
            vmem(2 * OTHERS, 2, LANES),
            vmem(OTHERS, 16, LANES),
            dma((4,)),
            dma((copies,)),
            dma((copies,)),
            dma,
            dma,
            dma((steps, 4)),
            dma((2, 4)),
        ],
        compiler_params=pltpu.CompilerParams(
            collective_id=0, has_side_effects=True, vmem_limit_bytes=60 * 2**20
        ),
        name="step",
    )(
        source_points,
        target_points,
        normals,
        weights,
        jnp.transpose(blocks, last),
        jnp.transpose(affines, last),
        anchor,
    )
    outs = pl.pallas_call(
        finish_kernel,
        out_shape=tuple(jax.ShapeDtypeStruct(out.shape, F32) for out in outs),
        in_specs=[anywhere] * 2,
        out_specs=[anywhere] * 2,
        scratch_shapes=[dma((2,))],
        name="finish",
    )(*outs)
    return tuple(jnp.transpose(out, (3, 0, 1, 2)) for out in outs)


def solution(mesh):
    placed = (
        P(None, None, "gx", "gy", "gz", None),
        P(None, None, "gx", "gy", "gz", None),
        P(None, None, "gx", "gy", "gz", None),
        P(None, "gx", "gy", "gz", None),
        P(None, "gx", "gy", "gz"),
        P(None, "gx", "gy", "gz"),
        P(),
    )
    return jax.shard_map(
        on_device,
        mesh=mesh,
        in_specs=placed,
        out_specs=(P(None, "gx", "gy", "gz"), P(None, "gx", "gy", "gz")),
        check_vma=False,
    )
```

```python
import functools

import jax
import jax.numpy as jnp
from jax import lax
from jax.experimental import pallas as pl
from jax.experimental.pallas import tpu as pltpu
from jax.sharding import PartitionSpec as P

BLOCK = 256
FIRST, SECOND, AHEAD = 5, 5, 2
SPACING = 0.5
DAMPING = 1.0
OFFSETS = (
    (1, 0, 0),
    (0, 1, 0),
    (0, 0, 1),
    (1, 1, -1),
    (1, -1, 1),
    (-1, 1, 1),
    (1, 1, 0),
    (1, 0, 1),
    (0, 1, 1),
    (1, 1, 1),
    (1, -1, 0),
    (0, 1, -1),
    (-1, 0, 1),
)
AXES = ("gx", "gy", "gz")
MESH = pl.DeviceIdType.MESH
LANES = 128
TY, TZ, TILES = 4, 2, 8
COMPS = 12
ROWS = COMPS * TILES
WIDE = ROWS + TILES
F32 = jnp.float32


def shifts(offset):
    seconds = (0,) if offset[1] == 0 else (0, offset[1])
    thirds = (0,) if offset[2] == 0 else (0, offset[2])
    return [(offset[0], y, z) for y in seconds for z in thirds]


SELF = (0, 0, 0)
REACH = (
    SELF,
    *sorted(
        {s for o in OFFSETS for s in shifts(o)} - {SELF}, key=lambda s: (-sum(map(abs, s)), s)
    ),
)
OTHERS = len(REACH) - 1
EARLY = 6
PAIRS = tuple(dict.fromkeys((s[0], s[2]) for s in REACH))
MEMBERS = tuple({s[1]: REACH.index(s) for s in REACH if (s[0], s[2]) == pair} for pair in PAIRS)
GREET = tuple(sorted({s for s in REACH[1:]} | {tuple(-p for p in s) for s in REACH[1:]}))


def spans(part, shift, length):
    if part == 0:
        return 0, length
    if shift == 0:
        return (1 if part > 0 else 0), length - 1
    return (0 if part > 0 else length - 1), 1


ORDER = tuple(sorted(range(len(OFFSETS)), key=lambda d: ((0, 2, 1)[OFFSETS[d][0]], d)))
PIECES = tuple(
    (d, s, *spans(OFFSETS[d][1], s[1], TY), *spans(OFFSETS[d][2], s[2], TZ))
    for d in ORDER
    for s in shifts(OFFSETS[d])
    if s != SELF
)


def device_at(shift, sign):
    there = []
    for axis, part in zip(AXES, shift):
        size = lax.axis_size(axis)
        there.append(lax.rem(lax.axis_index(axis) + (sign * part + size), size))
    return tuple(there)


def exists(shift):
    found = True
    for axis, part in zip(AXES, shift):
        if part > 0:
            found = jnp.logical_and(lax.axis_index(axis) + part < lax.axis_size(axis), found)
        elif part < 0:
            found = jnp.logical_and(lax.axis_index(axis) + part >= 0, found)
    return found


def either(condition, then, otherwise):
    lax.cond(condition, lambda: (then(), None)[1], lambda: (otherwise(), None)[1])


def remote(source, target, sent, got, device):
    return pltpu.make_async_remote_copy(
        src_ref=source,
        dst_ref=target,
        send_sem=sent,
        recv_sem=got,
        device_id=device,
        device_id_type=MESH,
    )


def iotas(rows=TILES):
    return (
        lax.broadcasted_iota(jnp.int32, (rows, LANES), 0),
        lax.broadcasted_iota(jnp.int32, (rows, LANES), 1),
    )


def tiled(mask, times):
    return jnp.concatenate([mask] * times, axis=0)


def cross(left, right):
    return lax.dot_general(
        left,
        right,
        (((1,), (1,)), ((), ())),
        precision=lax.Precision.HIGHEST,
        preferred_element_type=F32,
    )


def halves(x):
    top = x.astype(jnp.bfloat16)
    return top, (x - top.astype(F32)).astype(jnp.bfloat16)


def narrow_cross(left, right):
    return lax.dot_general(
        left, right, (((1,), (1,)), ((), ())), preferred_element_type=F32
    )


def cross_of(left_top, left_rest, right):
    top, rest = halves(right)
    both = narrow_cross(jnp.concatenate([left_top, left_rest], axis=0), top)
    count = left_top.shape[0]
    return both[:count] + (both[count:] + narrow_cross(left_top, rest))


def split(x):
    big = x * 4097.0
    high = big - (big - x)
    return high, x - high


def exact_product(x, y):
    (xh, xl), (yh, yl) = split(x), split(y)
    product = x * y
    return product, ((xh * yh - product) + xh * yl + xl * yh) + xl * yl


def lane_total(values, small, bound):
    grid = bound * 256.0
    top = (values + grid) - grid
    rest = values - top
    grid = grid * 2.0**-16
    middle = (rest + grid) - grid
    small = small + (rest - middle)
    top, middle, small = (jnp.sum(v, axis=1, keepdims=True) for v in (top, middle, small))
    high = top + middle
    back = high - top
    return high, ((top - (high - back)) + (middle - back)) + small


def compensated(parts):
    total, error = parts[0], jnp.zeros_like(parts[0])
    for part in parts[1:]:
        following = total + part
        back = following - total
        error = error + ((total - (following - back)) + (part - back))
        total = following
    high, low = total[0:1], error[0:1] + total[1:2]
    both = high + low
    return both, low - (both - high)


def step_kernel(plan, *refs):
    first_steps, second_steps, ahead, amounts = plan
    steps = len(amounts)
    source_out, target_out, normal_out, weight_out, counts, affines, anchor = refs[:7]
    update, residual = refs[7:9]
    source, target, normal, weight, moved, affine, affine_there = refs[9:16]
    slab, here, here_weighted, there, packed, small = refs[16:22]
    small_count, masked, blocks, shares, own = refs[22:27]
    shares_there, matrix, inverse, chain, chain_lifted, basis, lifted = refs[27:34]
    pair_sum, line_sum, pair_send, line_send = refs[34:38]
    rest = refs[38:]
    send_rows, got_rows, back_rows, got_back = (rest[k * steps : (k + 1) * steps] for k in range(4))
    zero_one, zero_two, zero_share, spare_one, spare_two, spare_share = rest[4 * steps :][:6]
    loaded, sent, got, share_sent, share_got, halo_sems, sum_sems = rest[4 * steps + 6 :]
    loads = [
        pltpu.make_async_copy(outer, ref, loaded.at[number])
        for number, (outer, ref) in enumerate(
            (
                (target_out, target),
                (source_out, source),
                (normal_out, normal),
                (weight_out, weight),
            )
        )
    ]
    for load in loads:
        load.start()
    first, second, third = (lax.axis_index(a) for a in AXES)
    size_first, size_second, size_third = (lax.axis_size(a) for a in AXES)
    in_pair = second * size_third + third
    pair_size = size_second * size_third

    def pair_peer(k):
        there = lax.rem(in_pair + k, pair_size)
        return (first, there // size_third, lax.rem(there, size_third))

    def line_peer(k):
        return (lax.rem(first + k, size_first), second, third)

    barrier = pltpu.get_barrier_semaphore()
    for ref in (moved, affine_there, zero_one, zero_two, zero_share):
        ref[...] = jnp.zeros_like(ref)
    neighbours = 0
    for shift in GREET:
        near = exists(shift)
        neighbours = neighbours + jnp.where(near, 1, 0)

        @pl.when(near)
        def _(shift=shift):
            pl.semaphore_signal(barrier, inc=1, device_id=device_at(shift, 1), device_id_type=MESH)


    @pl.loop(1, pair_size)
    def _(k):
        pl.semaphore_signal(barrier, inc=1, device_id=pair_peer(k), device_id_type=MESH)

    @pl.loop(1, size_first)
    def _(k):
        pl.semaphore_signal(barrier, inc=1, device_id=line_peer(k), device_id_type=MESH)

    sub, lane = iotas()
    slot = lane & (TILES - 1)
    same = sub == slot
    eyes = [lane == sub + a * TILES for a in range(COMPS)]
    wide_sub, wide_lane = iotas(16)

    def column(row):
        return [jnp.sum(jnp.where(eyes[a], row, 0.0), axis=1, keepdims=True) for a in range(COMPS)]

    def group(a):
        return slice(a * TILES, (a + 1) * TILES)

    def positions(tile):
        return (first, second * TY + tile // TZ, third * TZ + tile % TZ)

    extents = (size_first, size_second * TY, size_third * TZ)

    def kept(tile):
        x, y, z = positions(tile)
        return jnp.where((x * extents[1] + y) * extents[2] + z != anchor[0], 1.0, 0.0)

    for y in range(TY):
        small[2 * y : 2 * y + 2, 0:COMPS] = affines[0, y]
    affine_columns = [
        small[:, a : a + 1] + (1.0 if a % 5 == 0 else 0.0) for a in range(COMPS)
    ]
    row = jnp.zeros((TILES, LANES), F32)
    for a in range(COMPS):
        row = row + jnp.where(eyes[a], affine_columns[a], 0.0)
    row = jnp.sum(row, axis=0, keepdims=True)
    row = jnp.where((lane[:1] >= ROWS) & (lane[:1] < WIDE), -SPACING, row)
    affine[...] = row

    for ref in (blocks, shares, own, packed):
        ref[...] = jnp.zeros_like(ref)
    points = here.shape[1]
    here[WIDE:, :] = jnp.zeros((LANES - WIDE, points), F32)
    there[ROWS:, :] = jnp.zeros((LANES - ROWS, points), F32)
    for index in ORDER:
        here_weighted[index, WIDE + ROWS :, :] = jnp.zeros((TILES, points), F32)
    numbers = lax.broadcasted_iota(jnp.int32, (TILES, points), 1)
    tile_column = sub[:, 0:1]
    for load in loads[1:]:
        load.wait()
    def source_part(index):
        offset = OFFSETS[index]
        for y in range(TY):
            for c in range(3):
                slab[c, 2 * y : 2 * y + 2, :] = source[c, index, 0, y]
                slab[3 + c, 2 * y : 2 * y + 2, :] = normal[c, index, 0, y]
            slab[6, 2 * y : 2 * y + 2, :] = weight[index, 0, y]
            small_count[2 * y : 2 * y + 2, :] = counts[0, y, :, index : index + 1]
        inside = functools.reduce(
            jnp.logical_and,
            [
                (p + o >= 0) & (p + o < extent)
                for p, o, extent in zip(positions(tile_column), offset, extents)
            ],
        )
        limit = jnp.where(inside, BLOCK * small_count[...], 0)
        share = jnp.where(numbers < limit, slab[6], 0.0)
        masked[index] = share
        for c in range(3):
            n = slab[3 + c]
            for e in range(4):
                at = (4 * c + e) * TILES
                a = n * slab[e] if e < 3 else n
                here[at : at + TILES, :] = a
                here_weighted[index, at : at + TILES, :] = a * share
        along = sum(part * slab[3 + c] for c, part in enumerate(offset) if part != 0)
        here[ROWS:WIDE, :] = along
        here_weighted[index, ROWS:WIDE, :] = along * share
        own[...] += cross_of(*halves(here_weighted[index, :ROWS, :]), here[...])

    for index in ORDER[:EARLY]:
        source_part(index)

    pl.semaphore_wait(barrier, neighbours + (pair_size - 1 + size_first - 1))
    loads[0].wait()
    zeros = {1: (zero_one, spare_one), 2: (zero_two, spare_two), 16: (zero_share, spare_share)}
    ahead_there = [exists(shift) for shift in REACH[1:]]
    behind_there = [exists(tuple(-part for part in shift)) for shift in REACH[1:]]

    def fill(count, place, number, arrival, departure):
        nothing, spare = zeros[count]
        pltpu.make_async_copy(nothing, place, arrival).start()
        pltpu.make_async_copy(nothing, spare.at[number], departure).start()

    copies = {}
    for number, (index, shift, low, count, low_z, count_z) in enumerate(PIECES):
        at = (slice(None), index, pl.ds(low, count), pl.ds(low_z, count_z))
        copy = remote(
            target.at[(slice(None), index, 0, *at[2:])],
            moved.at[at],
            sent.at[number],
            got.at[number],
            device_at(shift, -1),
        )
        number = REACH.index(shift) - 1
        pl.when(behind_there[number])(copy.start)
        copies.setdefault(index, []).append((copy, number))
    affine_copies = []
    for number, shift in enumerate(REACH[1:]):
        at = len(PIECES) + number
        affine_copies.append(
            remote(affine, affine_there.at[number], sent.at[at], got.at[at], device_at(shift, -1))
        )
        pl.when(behind_there[number])(affine_copies[-1].start)

    for index in ORDER[EARLY:]:
        source_part(index)
    own[...] = jnp.where(tiled(same, COMPS), own[...], 0.0)

    for index in ORDER:
        offset = OFFSETS[index]
        for copy, number in copies.get(index, ()):
            pl.when(ahead_there[number])(copy.wait_recv)
        for y in range(TY):
            before = (y - offset[1]) % TY
            shift_y = (y - offset[1]) // TY
            for z in range(TZ):
                back = (z - offset[2]) % TZ
                shift_z = (z - offset[2]) // TZ
                to, come = y * TZ + z, before * TZ + back
                local = (offset[0], -shift_y, -shift_z) == SELF
                for c in range(3):
                    slab[6 + c, to : to + 1, :] = normal[c, index, 0, before, back : back + 1, :]
                    if local:
                        slab[9 + c, to : to + 1, :] = target[c, index, 0, y, z : z + 1, :]
                    else:
                        slab[9 + c, to : to + 1, :] = moved[c, index, y, z : z + 1, :]
                slab[12, to : to + 1, :] = masked[index, come : come + 1, :]
        share_there = slab[12]
        for c in range(3):
            m = slab[6 + c]
            for e in range(4):
                at = (4 * c + e) * TILES
                b = -(m * slab[9 + e]) if e < 3 else -m
                there[at : at + TILES, :] = b
                here_weighted[index, WIDE + at : WIDE + at + TILES, :] = b * share_there
        both = cross_of(*halves(here_weighted[index]), there[...])
        pair, back = both[:WIDE], both[WIDE : WIDE + ROWS]
        for a in range(COMPS):
            packed[a : a + 1, :] = jnp.sum(
                jnp.where(same, back[group(a), :], 0.0), axis=0, keepdims=True
            )
        to_y, to_z = sub // TZ + offset[1], sub % TZ + offset[2]
        slot_y, slot_z = slot // TZ, slot % TZ
        all_slots = packed[...]
        for k, (pair_x, pair_z) in enumerate(PAIRS):
            ways = [w for w in shifts(offset) if (w[0], w[2]) == (pair_x, pair_z)]
            if not ways:
                continue
            meets = functools.reduce(
                jnp.logical_or, [slot_y + TY * w[1] == to_y for w in ways]
            ) & (slot_z + TZ * pair_z == to_z)
            blocks[k] += jnp.where(tiled(meets, WIDE // TILES), pair, 0.0)
        for shift in shifts(offset):
            j = REACH.index(shift)
            from_y, from_z = slot_y - offset[1] + TY * shift[1], slot_z - offset[2] + TZ * shift[2]
            owned = (from_y >= 0) & (from_y < TY) & (from_z >= 0) & (from_z < TZ)
            shares[j] += jnp.where(tiled(owned, 2), all_slots, 0.0)
    crossing_up = (sub // TZ == TY - 1) & (slot // TZ == 0)
    crossing_down = (sub // TZ == 0) & (slot // TZ == TY - 1)
    staying = jnp.logical_not(crossing_up | crossing_down)
    sides = {0: staying, 1: crossing_up, -1: crossing_down}

    def mixed(k, row_of):
        value = jnp.broadcast_to(row_of(MEMBERS[k][0]), (TILES, LANES))
        for side in (1, -1):
            if side in MEMBERS[k]:
                value = jnp.where(sides[side], row_of(MEMBERS[k][side]), value)
        return value

    def parted(k, total):
        return [
            (j, jnp.sum(jnp.where(sides[side], total, 0.0), axis=0, keepdims=True))
            for side, j in MEMBERS[k].items()
        ]

    extended = [*affine_columns, jnp.full((TILES, 1), -SPACING, F32)]
    for k in range(len(PAIRS)):
        total = jnp.zeros((TILES, LANES), F32)
        for a in range(COMPS + 1):
            total = total + blocks[k, group(a), :] * extended[a]
        for j, part in parted(k, total):
            shares[j, COMPS : COMPS + 1, :] = part
    for number, shift in enumerate(REACH[1:]):
        copy = remote(
            shares.at[number + 1],
            shares_there.at[number],
            share_sent,
            share_got,
            device_at(shift, 1),
        )
        pl.when(ahead_there[number])(copy.start)

        @pl.when(jnp.logical_not(behind_there[number]))
        def _(number=number):
            nothing = zeros[16][0]
            pltpu.make_async_copy(nothing, shares_there.at[number], share_got).start()

        @pl.when(jnp.logical_not(ahead_there[number]))
        def _(number=number):
            nothing, spare = zeros[16]
            pltpu.make_async_copy(nothing, spare.at[number], share_sent).start()

    for index in ORDER:
        for copy, number in copies.get(index, ()):
            pl.when(behind_there[number])(copy.wait_send)
    for number, copy in enumerate(affine_copies):
        pl.when(ahead_there[number])(copy.wait_recv)
        pl.when(behind_there[number])(copy.wait_send)

    keep_row, keep_one = kept(slot[:1]), kept(tile_column)
    keep_column = [keep_one] * COMPS
    mixes = [mixed(k, lambda j: affine_there[j - 1] if j else row) for k in range(len(PAIRS))]
    sums = []
    for a in range(COMPS):
        total = own[group(a), :] * row
        for k, mix in enumerate(mixes):
            total = total + blocks[k, group(a), :] * mix
        sums.append(total)
    everything = pltpu.make_async_copy(shares_there, shares_there, share_got)
    everything.wait()
    pltpu.make_async_copy(shares_there, shares_there, share_sent).wait()
    gathered = shares[0]
    for j in range(OTHERS):
        gathered = gathered + shares_there[j]
    right = []
    for a in range(COMPS):
        spread = jnp.where(same & (lane < ROWS), gathered[a : a + 1, :], 0.0)
        total = sums[a] + spread * row + jnp.where(eyes[a], gathered[COMPS : COMPS + 1, :], 0.0)
        right.append(-keep_column[a] * jnp.sum(total, axis=1, keepdims=True))
        mine = jnp.where(lane < ROWS, own[group(a), :], 0.0)
        compact = jnp.sum(mine, axis=0, keepdims=True) + gathered[a : a + 1, :]
        unit = jnp.where((lane[:1] >= a * TILES) & (lane[:1] < (a + 1) * TILES), 1.0, 0.0)
        compact = keep_row * (compact + DAMPING * unit) + (1.0 - keep_row) * unit
        picked = jnp.where(wide_lane // TILES == wide_sub, compact, 0.0)
        for by in (8, 16, 32, 64):
            picked = picked + pltpu.roll(picked, by, 1)
        matrix[a] = picked

    rows = [matrix[a] for a in range(COMPS)]
    for k in range(COMPS):
        factor = 1.0 / rows[k][k : k + 1, :]
        at_pivot = wide_sub == k
        pivot_row = jnp.where(at_pivot, factor, rows[k] * factor)
        for i in range(COMPS):
            if i != k:
                f = rows[i][k : k + 1, :]
                rows[i] = jnp.where(at_pivot, 0.0, rows[i]) - f * pivot_row
        rows[k] = pivot_row
    for a in range(COMPS):
        compact = jnp.sum(
            jnp.where(wide_lane // TILES == wide_sub, rows[a], 0.0), axis=0, keepdims=True
        )
        inverse[group(a), :] = jnp.where(same & (lane < ROWS), compact, 0.0)

    def as_row(col):
        total = jnp.zeros((TILES, LANES), F32)
        for a in range(COMPS):
            total = total + jnp.where(eyes[a], col[a], 0.0)
        return jnp.sum(total, axis=0, keepdims=True)

    def precondition(col):
        total = jnp.zeros((TILES, LANES), F32)
        for a in range(COMPS):
            total = total + inverse[group(a), :] * col[a]
        return jnp.sum(total, axis=0, keepdims=True)

    def couple(step, vectors, meanwhile=None):
        amount = len(vectors)
        for r, v in enumerate(vectors):
            send_rows[step][0, r : r + 1, :] = v
        for number, shift in enumerate(REACH[1:]):
            copy = remote(
                send_rows[step].at[0],
                got_rows[step].at[number],
                halo_sems.at[step, 0],
                halo_sems.at[step, 1],
                device_at(shift, -1),
            )
            empty = functools.partial(
                fill,
                amount,
                got_back[step].at[number],
                number,
                halo_sems.at[step, 3],
                halo_sems.at[step, 0],
            )
            either(behind_there[number], copy.start, empty)
        cols = [column(v) for v in vectors]
        local = [None] * amount
        for k in range(len(PAIRS)):
            totals = [jnp.zeros((TILES, LANES), F32) for _ in vectors]
            for a in range(COMPS):
                block = blocks[k, group(a), :]
                for r in range(amount):
                    totals[r] = totals[r] + block * cols[r][a]
            for r in range(amount):
                for j, part in parted(k, totals[r]):
                    if j == 0:
                        local[r] = part
                    else:
                        back_rows[step][j - 1, r : r + 1, :] = part
        for number, shift in enumerate(REACH[1:]):
            copy = remote(
                back_rows[step].at[number],
                got_back[step].at[number],
                halo_sems.at[step, 2],
                halo_sems.at[step, 3],
                device_at(shift, 1),
            )
            empty = functools.partial(
                fill,
                amount,
                got_rows[step].at[number],
                OTHERS + number,
                halo_sems.at[step, 1],
                halo_sems.at[step, 2],
            )
            either(ahead_there[number], copy.start, empty)
        if meanwhile is not None:
            meanwhile()
        rows_there, back_there = got_rows[step], got_back[step]
        pltpu.make_async_copy(rows_there, rows_there, halo_sems.at[step, 1]).wait()
        sums = [[None] * COMPS for _ in vectors]
        for k in range(len(PAIRS)):
            mixes = [
                mixed(k, lambda j, r=r, v=v: rows_there[j - 1, r : r + 1, :] if j else v)
                for r, v in enumerate(vectors)
            ]
            for a in range(COMPS):
                block = blocks[k, group(a), :]
                for r in range(amount):
                    part = block * mixes[r]
                    sums[r][a] = part if k == 0 else sums[r][a] + part
        pltpu.make_async_copy(back_there, back_there, halo_sems.at[step, 3]).wait()
        results = []
        for r in range(amount):
            came = local[r]
            for j in range(OTHERS):
                came = came + back_there[j, r : r + 1, :]
            results.append(
                [
                    keep_column[a]
                    * jnp.sum(sums[r][a] + jnp.where(eyes[a], came, 0.0), axis=1, keepdims=True)
                    for a in range(COMPS)
                ]
            )
        pltpu.make_async_copy(rows_there, rows_there, halo_sems.at[step, 0]).wait()
        pltpu.make_async_copy(back_there, back_there, halo_sems.at[step, 2]).wait()
        return results

    def pair_part(at):
        return pair_sum.at[at, pl.ds(0, pair_size - 1)]

    def line_part(at):
        return line_sum.at[at, pl.ds(0, size_first - 1)]

    def wait_for(part, sem):
        pltpu.make_async_copy(part, part, sem).wait()

    def start_sum(high, low, at):
        for row, value in ((0, high), (1, low)):
            pair_send[at, row : row + 1, :] = value
            pair_sum[at, in_pair, row : row + 1, :] = value

        for k in range(1, pair_size):
            remote(
                pair_send.at[at],
                pair_sum.at[at, in_pair],
                sum_sems.at[at, 0],
                sum_sems.at[at, 1],
                pair_peer(k),
            ).start()

    def go_on_sum(at):
        wait_for(pair_part(at), sum_sems.at[at, 1])
        high, low = compensated([pair_sum[at, k] for k in range(pair_size)])
        for row, value in ((0, high), (1, low)):
            line_send[at, row : row + 1, :] = value
            line_sum[at, first, row : row + 1, :] = value

        for k in range(1, size_first):
            remote(
                line_send.at[at],
                line_sum.at[at, first],
                sum_sems.at[at, 2],
                sum_sems.at[at, 3],
                line_peer(k),
            ).start()

    def end_sum(at):
        wait_for(line_part(at), sum_sems.at[at, 3])
        high, low = compensated([line_sum[at, k] for k in range(size_first)])
        wait_for(pair_part(at), sum_sems.at[at, 0])
        wait_for(line_part(at), sum_sems.at[at, 2])
        return tuple(jnp.broadcast_to(v, (TILES, LANES)) for v in (high, low))

    def largest(values):
        return jnp.max(jnp.abs(values), axis=1, keepdims=True)

    def gram(count, ys, zs):
        y_bound, z_bound = largest(ys), largest(zs)
        row_of, lane_of = iotas(ys.shape[0])
        high = low = jnp.zeros(ys.shape, F32)
        for j in range(count):
            at = (lane_of == row_of * count + j) & (row_of < count)
            product, error = exact_product(ys, zs[j : j + 1, :])
            h, l = lane_total(product, error, y_bound * z_bound[j : j + 1, :])
            high, low = jnp.where(at, h, high), jnp.where(at, l, low)
        return tuple(jnp.sum(v, axis=0, keepdims=True) for v in (high, low))

    def iterate(count, amount, at_p, at_r, high, low):
        major = jnp.zeros((TILES, LANES), jnp.int32)
        for k in range(1, count + 1):
            major = major + jnp.where(lane >= k * count, 1, 0)
        minor = lane - count * major

        def form(mask):
            return jnp.where(mask & (lane < count * count), 1.0, 0.0)

        g_bound = largest(high)

        def inner(x, y, bound):
            product, error = exact_product(x, y)
            values, small = exact_product(product, high)
            total = lane_total(values, small + (product * low + error * high), g_bound * bound)
            return total[0] + total[1]

        p_major, p_minor = form(major == at_p), form(minor == at_p)
        r_major, r_minor = form(major == at_r), form(minor == at_r)
        u_minor = jnp.zeros((TILES, LANES), F32)
        p_most = r_most = jnp.ones((TILES, 1), F32)
        product = inner(r_major, r_minor, r_most)
        for _ in range(amount):
            a_major = p_major + pltpu.roll(p_major, count, 1)
            a_minor = p_minor + pltpu.roll(p_minor, 1, 1)
            a_most = 2.0 * p_most
            alpha = product / inner(p_major, a_minor, p_most * a_most)
            u_minor = u_minor + alpha * p_minor
            r_major = r_major - alpha * a_major
            r_minor = r_minor - alpha * a_minor
            r_most = (r_most + jnp.abs(alpha) * a_most) * 1.01
            following = inner(r_major, r_minor, r_most * r_most)
            ratio = following / product
            p_major = r_major + ratio * p_major
            p_minor = r_minor + ratio * p_minor
            p_most = (r_most + jnp.abs(ratio) * p_most) * 1.01
            product = following
        return u_minor, r_minor, p_minor

    def combined(count, minor_form, vectors, by=0):
        both = jnp.concatenate([minor_form, minor_form], axis=0)
        weights = jnp.sum(
            jnp.where((wide_lane + by == wide_sub) & (wide_lane < count), both, 0.0),
            axis=1,
            keepdims=True,
        )
        return jnp.sum(weights * vectors, axis=0, keepdims=True)

    for ref in (chain, chain_lifted, basis, lifted):
        ref[...] = jnp.zeros_like(ref)
    chain[0:1, :] = as_row(right)
    chain_lifted[0:1, :] = precondition(right)

    def extend(step, places, ys, zs, meanwhile=None):
        found = couple(step, [zs[at : at + 1, :] for at in places], meanwhile)
        for at, col in zip(places, found):
            ys[at + 1 : at + 2, :] = as_row(col)
            zs[at + 1 : at + 2, :] = precondition(col)

    for step in range(first_steps):
        extend(step, [step], chain, chain_lifted)
    count = first_steps + 1
    start_sum(*gram(count, chain[0:8, :], chain_lifted[0:8, :]), 0)
    for step in range(first_steps, first_steps + ahead):
        extend(
            step,
            [step],
            chain,
            chain_lifted,
            functools.partial(go_on_sum, 0) if step == first_steps else None,
        )
    u_form, r_form, p_form = iterate(count, first_steps, 0, 0, *end_sum(0))
    ys, zs = chain[...], chain_lifted[...]
    part = combined(count, u_form, zs)
    at_r = second_steps + 1
    for begin, shape in ((0, p_form), (at_r, r_form)):
        for by in range(ahead + 1):
            at = begin + by
            basis[at : at + 1, :] = combined(count, shape, ys, by)
            lifted[at : at + 1, :] = combined(count, shape, zs, by)
    for step in range(first_steps + ahead, steps):
        degree = step - first_steps
        extend(step, [degree, at_r + degree][: amounts[step]], basis, lifted)
    count = 2 * second_steps + 1
    start_sum(*gram(count, basis[...], lifted[...]), 1)
    go_on_sum(1)
    u_form, r_form, _ = iterate(count, second_steps, 0, at_r, *end_sum(1))
    results = (
        (update, part + combined(count, u_form, lifted[...])),
        (residual, combined(count, r_form, basis[...])),
    )
    for out, row in results:
        spread = jnp.zeros((TILES, LANES), F32)
        for a, col in enumerate(column(row)):
            spread = jnp.where(lane == a, col, spread)
        small[...] = spread
        for y in range(TY):
            out[0, y] = small[2 * y : 2 * y + 2, 0:COMPS]


def finish_kernel(first, second, first_out, second_out, sems):
    copies = [
        pltpu.make_async_copy(first, first_out, sems.at[0]),
        pltpu.make_async_copy(second, second_out, sems.at[1]),
    ]
    for copy in copies:
        copy.start()
    for copy in copies:
        copy.wait()


def vmem(*shape):
    return pltpu.VMEM(shape, F32)


def on_device(source_points, target_points, normals, weights, blocks, affines, anchor):
    points = source_points.shape[5]
    dirs = len(OFFSETS)
    sizes = [lax.axis_size(a) for a in AXES]
    later = SECOND - AHEAD
    amounts = (1,) * (FIRST + AHEAD) + (2,) * (later - 1) + (1,)
    steps = len(amounts)
    pair_size = sizes[1] * sizes[2]
    anywhere = pl.BlockSpec(memory_space=pl.ANY)
    in_vmem = pl.BlockSpec(memory_space=pltpu.VMEM)
    in_smem = pl.BlockSpec(memory_space=pltpu.SMEM)
    copies = len(PIECES) + OTHERS
    dma = pltpu.SemaphoreType.DMA
    last = (1, 2, 3, 0)
    outs = pl.pallas_call(
        functools.partial(step_kernel, (FIRST, SECOND, AHEAD, amounts)),
        out_shape=(jax.ShapeDtypeStruct((1, TY, TZ, COMPS), F32),) * 2,
        in_specs=[anywhere] * 4 + [in_vmem] * 2 + [in_smem],
        out_specs=[in_vmem] * 2,
        scratch_shapes=[
            vmem(*source_points.shape),
            vmem(*target_points.shape),
            vmem(*normals.shape),
            vmem(*weights.shape),
            vmem(3, dirs, TY, TZ, points),
            vmem(1, LANES),
            vmem(OTHERS, 1, LANES),
            vmem(13, TILES, points),
            vmem(LANES, points),
            vmem(dirs, WIDE + ROWS + TILES, points),
            vmem(LANES, points),
            vmem(16, LANES),
            vmem(TILES, LANES),
            pltpu.VMEM((TILES, 1), jnp.int32),
            vmem(dirs, TILES, points),
            vmem(len(PAIRS), WIDE, LANES),
            vmem(OTHERS + 1, 16, LANES),
            vmem(ROWS, LANES),
            vmem(OTHERS, 16, LANES),
            vmem(COMPS, 16, LANES),
            vmem(ROWS, LANES),
            *[vmem(16, LANES)] * 4,
            vmem(2, pair_size, 2, LANES),
            vmem(2, sizes[0], 2, LANES),
            vmem(2, 2, LANES),
            vmem(2, 2, LANES),
            *[vmem(1, r, LANES) for r in amounts],
            *[vmem(OTHERS, r, LANES) for r in amounts],
            *[vmem(OTHERS, r, LANES) for r in amounts],
            *[vmem(OTHERS, r, LANES) for r in amounts],
            vmem(1, LANES),
            vmem(2, LANES),
            vmem(16, LANES),
            vmem(2 * OTHERS, 1, LANES),
            vmem(2 * OTHERS, 2, LANES),
            vmem(OTHERS, 16, LANES),
            dma((4,)),
            dma((copies,)),
            dma((copies,)),
            dma,
            dma,
            dma((steps, 4)),
            dma((2, 4)),
        ],
        compiler_params=pltpu.CompilerParams(
            collective_id=0, has_side_effects=True, vmem_limit_bytes=60 * 2**20
        ),
        name="step",
    )(
        source_points,
        target_points,
        normals,
        weights,
        jnp.transpose(blocks, last),
        jnp.transpose(affines, last),
        anchor,
    )
    outs = pl.pallas_call(
        finish_kernel,
        out_shape=tuple(jax.ShapeDtypeStruct(out.shape, F32) for out in outs),
        in_specs=[anywhere] * 2,
        out_specs=[anywhere] * 2,
        scratch_shapes=[dma((2,))],
        name="finish",
    )(*outs)
    return tuple(jnp.transpose(out, (3, 0, 1, 2)) for out in outs)


def solution(mesh):
    placed = (
        P(None, None, "gx", "gy", "gz", None),
        P(None, None, "gx", "gy", "gz", None),
        P(None, None, "gx", "gy", "gz", None),
        P(None, "gx", "gy", "gz", None),
        P(None, "gx", "gy", "gz"),
        P(None, "gx", "gy", "gz"),
        P(),
    )
    return jax.shard_map(
        on_device,
        mesh=mesh,
        in_specs=placed,
        out_specs=(P(None, "gx", "gy", "gz"), P(None, "gx", "gy", "gz")),
        check_vma=False,
    )
```

```python
import functools

import jax
import jax.numpy as jnp
from jax import lax
from jax.experimental import pallas as pl
from jax.experimental.pallas import tpu as pltpu
from jax.sharding import PartitionSpec as P

BLOCK = 256
FIRST, SECOND, AHEAD = 5, 5, 2
SPACING = 0.5
DAMPING = 1.0
OFFSETS = (
    (1, 0, 0),
    (0, 1, 0),
    (0, 0, 1),
    (1, 1, -1),
    (1, -1, 1),
    (-1, 1, 1),
    (1, 1, 0),
    (1, 0, 1),
    (0, 1, 1),
    (1, 1, 1),
    (1, -1, 0),
    (0, 1, -1),
    (-1, 0, 1),
)
AXES = ("gx", "gy", "gz")
MESH = pl.DeviceIdType.MESH
LANES = 128
TY, TZ, TILES = 4, 2, 8
COMPS = 12
ROWS = COMPS * TILES
WIDE = ROWS + TILES
F32 = jnp.float32


def shifts(offset):
    seconds = (0,) if offset[1] == 0 else (0, offset[1])
    thirds = (0,) if offset[2] == 0 else (0, offset[2])
    return [(offset[0], y, z) for y in seconds for z in thirds]


SELF = (0, 0, 0)
REACH = (
    SELF,
    *sorted(
        {s for o in OFFSETS for s in shifts(o)} - {SELF}, key=lambda s: (-sum(map(abs, s)), s)
    ),
)
OTHERS = len(REACH) - 1
EARLY = 6
PAIRS = tuple(dict.fromkeys((s[0], s[2]) for s in REACH))
MEMBERS = tuple({s[1]: REACH.index(s) for s in REACH if (s[0], s[2]) == pair} for pair in PAIRS)
GREET = tuple(sorted({s for s in REACH[1:]} | {tuple(-p for p in s) for s in REACH[1:]}))


def spans(part, shift, length):
    if part == 0:
        return 0, length
    if shift == 0:
        return (1 if part > 0 else 0), length - 1
    return (0 if part > 0 else length - 1), 1


ORDER = tuple(sorted(range(len(OFFSETS)), key=lambda d: ((0, 2, 1)[OFFSETS[d][0]], d)))
PIECES = tuple(
    (d, s, *spans(OFFSETS[d][1], s[1], TY), *spans(OFFSETS[d][2], s[2], TZ))
    for d in ORDER
    for s in shifts(OFFSETS[d])
    if s != SELF
)


def device_at(shift, sign):
    there = []
    for axis, part in zip(AXES, shift):
        size = lax.axis_size(axis)
        there.append(lax.rem(lax.axis_index(axis) + (sign * part + size), size))
    return tuple(there)


def exists(shift):
    found = True
    for axis, part in zip(AXES, shift):
        if part > 0:
            found = jnp.logical_and(lax.axis_index(axis) + part < lax.axis_size(axis), found)
        elif part < 0:
            found = jnp.logical_and(lax.axis_index(axis) + part >= 0, found)
    return found


def either(condition, then, otherwise):
    lax.cond(condition, lambda: (then(), None)[1], lambda: (otherwise(), None)[1])


def remote(source, target, sent, got, device):
    return pltpu.make_async_remote_copy(
        src_ref=source,
        dst_ref=target,
        send_sem=sent,
        recv_sem=got,
        device_id=device,
        device_id_type=MESH,
    )


def iotas(rows=TILES):
    return (
        lax.broadcasted_iota(jnp.int32, (rows, LANES), 0),
        lax.broadcasted_iota(jnp.int32, (rows, LANES), 1),
    )


def tiled(mask, times):
    return jnp.concatenate([mask] * times, axis=0)


def cross(left, right):
    return lax.dot_general(
        left,
        right,
        (((1,), (1,)), ((), ())),
        precision=lax.Precision.HIGHEST,
        preferred_element_type=F32,
    )


def halves(x):
    top = x.astype(jnp.bfloat16)
    return top, (x - top.astype(F32)).astype(jnp.bfloat16)


def narrow_cross(left, right):
    return lax.dot_general(
        left, right, (((1,), (1,)), ((), ())), preferred_element_type=F32
    )


def cross_of(left_top, left_rest, right):
    top, rest = halves(right)
    both = narrow_cross(jnp.concatenate([left_top, left_rest], axis=0), top)
    count = left_top.shape[0]
    return both[:count] + (both[count:] + narrow_cross(left_top, rest))


def split(x):
    big = x * 4097.0
    high = big - (big - x)
    return high, x - high


def exact_product(x, y):
    (xh, xl), (yh, yl) = split(x), split(y)
    product = x * y
    return product, ((xh * yh - product) + xh * yl + xl * yh) + xl * yl


def lane_total(values, small, bound):
    grid = bound * 256.0
    top = (values + grid) - grid
    rest = values - top
    grid = grid * 2.0**-16
    middle = (rest + grid) - grid
    small = small + (rest - middle)
    top, middle, small = (jnp.sum(v, axis=1, keepdims=True) for v in (top, middle, small))
    high = top + middle
    back = high - top
    return high, ((top - (high - back)) + (middle - back)) + small


def compensated(parts):
    total, error = parts[0], jnp.zeros_like(parts[0])
    for part in parts[1:]:
        following = total + part
        back = following - total
        error = error + ((total - (following - back)) + (part - back))
        total = following
    high, low = total[0:1], error[0:1] + total[1:2]
    both = high + low
    return both, low - (both - high)


def step_kernel(plan, *refs):
    first_steps, second_steps, ahead, amounts = plan
    steps = len(amounts)
    source_out, target_out, normal_out, weight_out, counts, affines, anchor = refs[:7]
    update, residual = refs[7:9]
    source, target, normal, weight, moved, affine, affine_there = refs[9:16]
    slab, here, here_weighted, there, packed, small = refs[16:22]
    small_count, masked, blocks, shares, own = refs[22:27]
    shares_there, matrix, inverse, chain, chain_lifted, basis, lifted = refs[27:34]
    pair_sum, line_sum, pair_send, line_send = refs[34:38]
    rest = refs[38:]
    send_rows, got_rows, back_rows, got_back = (rest[k * steps : (k + 1) * steps] for k in range(4))
    zero_one, zero_two, zero_share, spare_one, spare_two, spare_share = rest[4 * steps :][:6]
    loaded, sent, got, share_sent, share_got, halo_sems, sum_sems = rest[4 * steps + 6 :]
    loads = [
        pltpu.make_async_copy(outer, ref, loaded.at[number])
        for number, (outer, ref) in enumerate(
            (
                (target_out, target),
                (source_out, source),
                (normal_out, normal),
                (weight_out, weight),
            )
        )
    ]
    for load in loads:
        load.start()
    first, second, third = (lax.axis_index(a) for a in AXES)
    size_first, size_second, size_third = (lax.axis_size(a) for a in AXES)
    in_pair = second * size_third + third
    pair_size = size_second * size_third

    def pair_peer(k):
        there = lax.rem(in_pair + k, pair_size)
        return (first, there // size_third, lax.rem(there, size_third))

    def line_peer(k):
        return (lax.rem(first + k, size_first), second, third)

    barrier = pltpu.get_barrier_semaphore()
    for ref in (moved, affine_there, zero_one, zero_two, zero_share):
        ref[...] = jnp.zeros_like(ref)
    neighbours = 0
    for shift in GREET:
        near = exists(shift)
        neighbours = neighbours + jnp.where(near, 1, 0)

        @pl.when(near)
        def _(shift=shift):
            pl.semaphore_signal(barrier, inc=1, device_id=device_at(shift, 1), device_id_type=MESH)


    @pl.loop(1, pair_size)
    def _(k):
        pl.semaphore_signal(barrier, inc=1, device_id=pair_peer(k), device_id_type=MESH)

    @pl.loop(1, size_first)
    def _(k):
        pl.semaphore_signal(barrier, inc=1, device_id=line_peer(k), device_id_type=MESH)

    sub, lane = iotas()
    slot = lane & (TILES - 1)
    same = sub == slot
    eyes = [lane == sub + a * TILES for a in range(COMPS)]
    wide_sub, wide_lane = iotas(16)

    def column(row):
        return [jnp.sum(jnp.where(eyes[a], row, 0.0), axis=1, keepdims=True) for a in range(COMPS)]

    def group(a):
        return slice(a * TILES, (a + 1) * TILES)

    def positions(tile):
        return (first, second * TY + tile // TZ, third * TZ + tile % TZ)

    extents = (size_first, size_second * TY, size_third * TZ)

    def kept(tile):
        x, y, z = positions(tile)
        return jnp.where((x * extents[1] + y) * extents[2] + z != anchor[0], 1.0, 0.0)

    for y in range(TY):
        small[2 * y : 2 * y + 2, 0:COMPS] = affines[0, y]
    affine_columns = [
        small[:, a : a + 1] + (1.0 if a % 5 == 0 else 0.0) for a in range(COMPS)
    ]
    row = jnp.zeros((TILES, LANES), F32)
    for a in range(COMPS):
        row = row + jnp.where(eyes[a], affine_columns[a], 0.0)
    row = jnp.sum(row, axis=0, keepdims=True)
    row = jnp.where((lane[:1] >= ROWS) & (lane[:1] < WIDE), -SPACING, row)
    affine[...] = row

    for ref in (blocks, shares, own, packed):
        ref[...] = jnp.zeros_like(ref)
    points = here.shape[1]
    here[WIDE:, :] = jnp.zeros((LANES - WIDE, points), F32)
    there[ROWS:, :] = jnp.zeros((LANES - ROWS, points), F32)
    for index in ORDER:
        here_weighted[index, WIDE + ROWS :, :] = jnp.zeros((TILES, points), F32)
    numbers = lax.broadcasted_iota(jnp.int32, (TILES, points), 1)
    tile_column = sub[:, 0:1]
    for load in loads[1:]:
        load.wait()
    def source_part(index):
        offset = OFFSETS[index]
        for y in range(TY):
            for c in range(3):
                slab[c, 2 * y : 2 * y + 2, :] = source[c, index, 0, y]
                slab[3 + c, 2 * y : 2 * y + 2, :] = normal[c, index, 0, y]
            slab[6, 2 * y : 2 * y + 2, :] = weight[index, 0, y]
            small_count[2 * y : 2 * y + 2, :] = counts[0, y, :, index : index + 1]
        inside = functools.reduce(
            jnp.logical_and,
            [
                (p + o >= 0) & (p + o < extent)
                for p, o, extent in zip(positions(tile_column), offset, extents)
            ],
        )
        limit = jnp.where(inside, BLOCK * small_count[...], 0)
        share = jnp.where(numbers < limit, slab[6], 0.0)
        masked[index] = share
        for c in range(3):
            n = slab[3 + c]
            for e in range(4):
                at = (4 * c + e) * TILES
                a = n * slab[e] if e < 3 else n
                here[at : at + TILES, :] = a
                here_weighted[index, at : at + TILES, :] = a * share
        along = sum(part * slab[3 + c] for c, part in enumerate(offset) if part != 0)
        here[ROWS:WIDE, :] = along
        here_weighted[index, ROWS:WIDE, :] = along * share
        own[...] += cross_of(*halves(here_weighted[index, :ROWS, :]), here[...])

    for index in ORDER[:EARLY]:
        source_part(index)

    pl.semaphore_wait(barrier, neighbours + (pair_size - 1 + size_first - 1))
    loads[0].wait()
    zeros = {1: (zero_one, spare_one), 2: (zero_two, spare_two), 16: (zero_share, spare_share)}
    ahead_there = [exists(shift) for shift in REACH[1:]]
    behind_there = [exists(tuple(-part for part in shift)) for shift in REACH[1:]]

    def fill(count, place, number, arrival, departure):
        nothing, spare = zeros[count]
        pltpu.make_async_copy(nothing, place, arrival).start()
        pltpu.make_async_copy(nothing, spare.at[number], departure).start()

    copies = {}
    for number, (index, shift, low, count, low_z, count_z) in enumerate(PIECES):
        at = (slice(None), index, pl.ds(low, count), pl.ds(low_z, count_z))
        copy = remote(
            target.at[(slice(None), index, 0, *at[2:])],
            moved.at[at],
            sent.at[number],
            got.at[number],
            device_at(shift, -1),
        )
        number = REACH.index(shift) - 1
        pl.when(behind_there[number])(copy.start)
        copies.setdefault(index, []).append((copy, number))
    affine_copies = []
    for number, shift in enumerate(REACH[1:]):
        at = len(PIECES) + number
        affine_copies.append(
            remote(affine, affine_there.at[number], sent.at[at], got.at[at], device_at(shift, -1))
        )
        pl.when(behind_there[number])(affine_copies[-1].start)

    for index in ORDER[EARLY:]:
        source_part(index)
    own[...] = jnp.where(tiled(same, COMPS), own[...], 0.0)

    for index in ORDER:
        offset = OFFSETS[index]
        for copy, number in copies.get(index, ()):
            pl.when(ahead_there[number])(copy.wait_recv)
        for y in range(TY):
            before = (y - offset[1]) % TY
            shift_y = (y - offset[1]) // TY
            for z in range(TZ):
                back = (z - offset[2]) % TZ
                shift_z = (z - offset[2]) // TZ
                to, come = y * TZ + z, before * TZ + back
                local = (offset[0], -shift_y, -shift_z) == SELF
                for c in range(3):
                    slab[6 + c, to : to + 1, :] = normal[c, index, 0, before, back : back + 1, :]
                    if local:
                        slab[9 + c, to : to + 1, :] = target[c, index, 0, y, z : z + 1, :]
                    else:
                        slab[9 + c, to : to + 1, :] = moved[c, index, y, z : z + 1, :]
                slab[12, to : to + 1, :] = masked[index, come : come + 1, :]
        share_there = slab[12]
        for c in range(3):
            m = slab[6 + c]
            for e in range(4):
                at = (4 * c + e) * TILES
                b = -(m * slab[9 + e]) if e < 3 else -m
                there[at : at + TILES, :] = b
                here_weighted[index, WIDE + at : WIDE + at + TILES, :] = b * share_there
        both = cross_of(*halves(here_weighted[index]), there[...])
        pair, back = both[:WIDE], both[WIDE : WIDE + ROWS]
        for a in range(COMPS):
            packed[a : a + 1, :] = jnp.sum(
                jnp.where(same, back[group(a), :], 0.0), axis=0, keepdims=True
            )
        to_y, to_z = sub // TZ + offset[1], sub % TZ + offset[2]
        slot_y, slot_z = slot // TZ, slot % TZ
        all_slots = packed[...]
        for k, (pair_x, pair_z) in enumerate(PAIRS):
            ways = [w for w in shifts(offset) if (w[0], w[2]) == (pair_x, pair_z)]
            if not ways:
                continue
            meets = functools.reduce(
                jnp.logical_or, [slot_y + TY * w[1] == to_y for w in ways]
            ) & (slot_z + TZ * pair_z == to_z)
            blocks[k] += jnp.where(tiled(meets, WIDE // TILES), pair, 0.0)
        for shift in shifts(offset):
            j = REACH.index(shift)
            from_y, from_z = slot_y - offset[1] + TY * shift[1], slot_z - offset[2] + TZ * shift[2]
            owned = (from_y >= 0) & (from_y < TY) & (from_z >= 0) & (from_z < TZ)
            shares[j] += jnp.where(tiled(owned, 2), all_slots, 0.0)
    crossing_up = (sub // TZ == TY - 1) & (slot // TZ == 0)
    crossing_down = (sub // TZ == 0) & (slot // TZ == TY - 1)
    staying = jnp.logical_not(crossing_up | crossing_down)
    sides = {0: staying, 1: crossing_up, -1: crossing_down}

    def mixed(k, row_of):
        value = jnp.broadcast_to(row_of(MEMBERS[k][0]), (TILES, LANES))
        for side in (1, -1):
            if side in MEMBERS[k]:
                value = jnp.where(sides[side], row_of(MEMBERS[k][side]), value)
        return value

    def parted(k, total):
        return [
            (j, jnp.sum(jnp.where(sides[side], total, 0.0), axis=0, keepdims=True))
            for side, j in MEMBERS[k].items()
        ]

    extended = [*affine_columns, jnp.full((TILES, 1), -SPACING, F32)]
    for k in range(len(PAIRS)):
        total = jnp.zeros((TILES, LANES), F32)
        for a in range(COMPS + 1):
            total = total + blocks[k, group(a), :] * extended[a]
        for j, part in parted(k, total):
            shares[j, COMPS : COMPS + 1, :] = part
    for number, shift in enumerate(REACH[1:]):
        copy = remote(
            shares.at[number + 1],
            shares_there.at[number],
            share_sent,
            share_got,
            device_at(shift, 1),
        )
        pl.when(ahead_there[number])(copy.start)

        @pl.when(jnp.logical_not(behind_there[number]))
        def _(number=number):
            nothing = zeros[16][0]
            pltpu.make_async_copy(nothing, shares_there.at[number], share_got).start()

        @pl.when(jnp.logical_not(ahead_there[number]))
        def _(number=number):
            nothing, spare = zeros[16]
            pltpu.make_async_copy(nothing, spare.at[number], share_sent).start()

    for index in ORDER:
        for copy, number in copies.get(index, ()):
            pl.when(behind_there[number])(copy.wait_send)
    for number, copy in enumerate(affine_copies):
        pl.when(ahead_there[number])(copy.wait_recv)
        pl.when(behind_there[number])(copy.wait_send)

    keep_row, keep_one = kept(slot[:1]), kept(tile_column)
    keep_column = [keep_one] * COMPS
    mixes = [mixed(k, lambda j: affine_there[j - 1] if j else row) for k in range(len(PAIRS))]
    sums = []
    for a in range(COMPS):
        total = own[group(a), :] * row
        for k, mix in enumerate(mixes):
            total = total + blocks[k, group(a), :] * mix
        sums.append(total)
    everything = pltpu.make_async_copy(shares_there, shares_there, share_got)
    everything.wait()
    pltpu.make_async_copy(shares_there, shares_there, share_sent).wait()
    gathered = shares[0]
    for j in range(OTHERS):
        gathered = gathered + shares_there[j]
    right = []
    for a in range(COMPS):
        spread = jnp.where(same & (lane < ROWS), gathered[a : a + 1, :], 0.0)
        total = sums[a] + spread * row + jnp.where(eyes[a], gathered[COMPS : COMPS + 1, :], 0.0)
        right.append(-keep_column[a] * jnp.sum(total, axis=1, keepdims=True))
        mine = jnp.where(lane < ROWS, own[group(a), :], 0.0)
        compact = jnp.sum(mine, axis=0, keepdims=True) + gathered[a : a + 1, :]
        unit = jnp.where((lane[:1] >= a * TILES) & (lane[:1] < (a + 1) * TILES), 1.0, 0.0)
        compact = keep_row * (compact + DAMPING * unit) + (1.0 - keep_row) * unit
        picked = jnp.where(wide_lane // TILES == wide_sub, compact, 0.0)
        for by in (8, 16, 32, 64):
            picked = picked + pltpu.roll(picked, by, 1)
        matrix[a] = picked

    rows = [matrix[a] for a in range(COMPS)]
    for k in range(COMPS):
        factor = 1.0 / rows[k][k : k + 1, :]
        at_pivot = wide_sub == k
        pivot_row = jnp.where(at_pivot, factor, rows[k] * factor)
        for i in range(COMPS):
            if i != k:
                f = rows[i][k : k + 1, :]
                rows[i] = jnp.where(at_pivot, 0.0, rows[i]) - f * pivot_row
        rows[k] = pivot_row
    for a in range(COMPS):
        compact = jnp.sum(
            jnp.where(wide_lane // TILES == wide_sub, rows[a], 0.0), axis=0, keepdims=True
        )
        inverse[group(a), :] = jnp.where(same & (lane < ROWS), compact, 0.0)

    def as_row(col):
        total = jnp.zeros((TILES, LANES), F32)
        for a in range(COMPS):
            total = total + jnp.where(eyes[a], col[a], 0.0)
        return jnp.sum(total, axis=0, keepdims=True)

    def precondition(col):
        total = jnp.zeros((TILES, LANES), F32)
        for a in range(COMPS):
            total = total + inverse[group(a), :] * col[a]
        return jnp.sum(total, axis=0, keepdims=True)

    def couple(step, vectors, meanwhile=None):
        amount = len(vectors)
        for r, v in enumerate(vectors):
            send_rows[step][0, r : r + 1, :] = v
        for number, shift in enumerate(REACH[1:]):
            copy = remote(
                send_rows[step].at[0],
                got_rows[step].at[number],
                halo_sems.at[step, 0],
                halo_sems.at[step, 1],
                device_at(shift, -1),
            )
            empty = functools.partial(
                fill,
                amount,
                got_back[step].at[number],
                number,
                halo_sems.at[step, 3],
                halo_sems.at[step, 0],
            )
            either(behind_there[number], copy.start, empty)
        cols = [column(v) for v in vectors]
        local = [None] * amount
        for k in range(len(PAIRS)):
            totals = [jnp.zeros((TILES, LANES), F32) for _ in vectors]
            for a in range(COMPS):
                block = blocks[k, group(a), :]
                for r in range(amount):
                    totals[r] = totals[r] + block * cols[r][a]
            for r in range(amount):
                for j, part in parted(k, totals[r]):
                    if j == 0:
                        local[r] = part
                    else:
                        back_rows[step][j - 1, r : r + 1, :] = part
        for number, shift in enumerate(REACH[1:]):
            copy = remote(
                back_rows[step].at[number],
                got_back[step].at[number],
                halo_sems.at[step, 2],
                halo_sems.at[step, 3],
                device_at(shift, 1),
            )
            empty = functools.partial(
                fill,
                amount,
                got_rows[step].at[number],
                OTHERS + number,
                halo_sems.at[step, 1],
                halo_sems.at[step, 2],
            )
            either(ahead_there[number], copy.start, empty)
        if meanwhile is not None:
            meanwhile()
        rows_there, back_there = got_rows[step], got_back[step]
        pltpu.make_async_copy(rows_there, rows_there, halo_sems.at[step, 1]).wait()
        sums = [[None] * COMPS for _ in vectors]
        for k in range(len(PAIRS)):
            mixes = [
                mixed(k, lambda j, r=r, v=v: rows_there[j - 1, r : r + 1, :] if j else v)
                for r, v in enumerate(vectors)
            ]
            for a in range(COMPS):
                block = blocks[k, group(a), :]
                for r in range(amount):
                    part = block * mixes[r]
                    sums[r][a] = part if k == 0 else sums[r][a] + part
        pltpu.make_async_copy(back_there, back_there, halo_sems.at[step, 3]).wait()
        results = []
        for r in range(amount):
            came = local[r]
            for j in range(OTHERS):
                came = came + back_there[j, r : r + 1, :]
            results.append(
                [
                    keep_column[a]
                    * jnp.sum(sums[r][a] + jnp.where(eyes[a], came, 0.0), axis=1, keepdims=True)
                    for a in range(COMPS)
                ]
            )
        pltpu.make_async_copy(rows_there, rows_there, halo_sems.at[step, 0]).wait()
        pltpu.make_async_copy(back_there, back_there, halo_sems.at[step, 2]).wait()
        return results

    def pair_part(at):
        return pair_sum.at[at, pl.ds(0, pair_size - 1)]

    def line_part(at):
        return line_sum.at[at, pl.ds(0, size_first - 1)]

    def wait_for(part, sem):
        pltpu.make_async_copy(part, part, sem).wait()

    def start_sum(high, low, at):
        for row, value in ((0, high), (1, low)):
            pair_send[at, row : row + 1, :] = value
            pair_sum[at, in_pair, row : row + 1, :] = value

        for k in range(1, pair_size):
            remote(
                pair_send.at[at],
                pair_sum.at[at, in_pair],
                sum_sems.at[at, 0],
                sum_sems.at[at, 1],
                pair_peer(k),
            ).start()

    def go_on_sum(at):
        wait_for(pair_part(at), sum_sems.at[at, 1])
        high, low = compensated([pair_sum[at, k] for k in range(pair_size)])
        for row, value in ((0, high), (1, low)):
            line_send[at, row : row + 1, :] = value
            line_sum[at, first, row : row + 1, :] = value

        for k in range(1, size_first):
            remote(
                line_send.at[at],
                line_sum.at[at, first],
                sum_sems.at[at, 2],
                sum_sems.at[at, 3],
                line_peer(k),
            ).start()

    def end_sum(at):
        wait_for(line_part(at), sum_sems.at[at, 3])
        high, low = compensated([line_sum[at, k] for k in range(size_first)])
        wait_for(pair_part(at), sum_sems.at[at, 0])
        wait_for(line_part(at), sum_sems.at[at, 2])
        return tuple(jnp.broadcast_to(v, (TILES, LANES)) for v in (high, low))

    def largest(values):
        return jnp.max(jnp.abs(values), axis=1, keepdims=True)

    def gram(count, ys, zs):
        y_bound, z_bound = largest(ys), largest(zs)
        row_of, lane_of = iotas(ys.shape[0])
        high = low = jnp.zeros(ys.shape, F32)
        for j in range(count):
            at = (lane_of == row_of * count + j) & (row_of < count)
            product, error = exact_product(ys, zs[j : j + 1, :])
            h, l = lane_total(product, error, y_bound * z_bound[j : j + 1, :])
            high, low = jnp.where(at, h, high), jnp.where(at, l, low)
        return tuple(jnp.sum(v, axis=0, keepdims=True) for v in (high, low))

    def iterate(count, amount, at_p, at_r, high, low, final=False):
        major = jnp.zeros((TILES, LANES), jnp.int32)
        for k in range(1, count + 1):
            major = major + jnp.where(lane >= k * count, 1, 0)
        minor = lane - count * major

        def form(mask):
            return jnp.where(mask & (lane < count * count), 1.0, 0.0)

        g_bound = largest(high)

        def inner(x, y, bound):
            product, error = exact_product(x, y)
            values, small = exact_product(product, high)
            total = lane_total(values, small + (product * low + error * high), g_bound * bound)
            return total[0] + total[1]

        p_major, p_minor = form(major == at_p), form(minor == at_p)
        r_major, r_minor = form(major == at_r), form(minor == at_r)
        u_minor = jnp.zeros((TILES, LANES), F32)
        p_most = r_most = jnp.ones((TILES, 1), F32)
        product = inner(r_major, r_minor, r_most)
        for number in range(amount):
            a_major = p_major + pltpu.roll(p_major, count, 1)
            a_minor = p_minor + pltpu.roll(p_minor, 1, 1)
            a_most = 2.0 * p_most
            alpha = product / inner(p_major, a_minor, p_most * a_most)
            u_minor = u_minor + alpha * p_minor
            r_major = r_major - alpha * a_major
            r_minor = r_minor - alpha * a_minor
            r_most = (r_most + jnp.abs(alpha) * a_most) * 1.01
            if final and number == amount - 1:
                break
            following = inner(r_major, r_minor, r_most * r_most)
            ratio = following / product
            p_major = r_major + ratio * p_major
            p_minor = r_minor + ratio * p_minor
            p_most = (r_most + jnp.abs(ratio) * p_most) * 1.01
            product = following
        return u_minor, r_minor, p_minor

    def combined(count, minor_form, vectors, by=0):
        both = jnp.concatenate([minor_form, minor_form], axis=0)
        weights = jnp.sum(
            jnp.where((wide_lane + by == wide_sub) & (wide_lane < count), both, 0.0),
            axis=1,
            keepdims=True,
        )
        return jnp.sum(weights * vectors, axis=0, keepdims=True)

    for ref in (chain, chain_lifted, basis, lifted):
        ref[...] = jnp.zeros_like(ref)
    chain[0:1, :] = as_row(right)
    chain_lifted[0:1, :] = precondition(right)

    def extend(step, places, ys, zs, meanwhile=None):
        found = couple(step, [zs[at : at + 1, :] for at in places], meanwhile)
        for at, col in zip(places, found):
            ys[at + 1 : at + 2, :] = as_row(col)
            zs[at + 1 : at + 2, :] = precondition(col)

    for step in range(first_steps):
        extend(step, [step], chain, chain_lifted)
    count = first_steps + 1
    start_sum(*gram(count, chain[0:8, :], chain_lifted[0:8, :]), 0)
    for step in range(first_steps, first_steps + ahead):
        extend(
            step,
            [step],
            chain,
            chain_lifted,
            functools.partial(go_on_sum, 0) if step == first_steps else None,
        )
    u_form, r_form, p_form = iterate(count, first_steps, 0, 0, *end_sum(0))
    ys, zs = chain[...], chain_lifted[...]
    part = combined(count, u_form, zs)
    at_r = second_steps + 1
    for begin, shape in ((0, p_form), (at_r, r_form)):
        for by in range(ahead + 1):
            at = begin + by
            basis[at : at + 1, :] = combined(count, shape, ys, by)
            lifted[at : at + 1, :] = combined(count, shape, zs, by)
    for step in range(first_steps + ahead, steps):
        degree = step - first_steps
        extend(step, [degree, at_r + degree][: amounts[step]], basis, lifted)
    count = 2 * second_steps + 1
    start_sum(*gram(count, basis[...], lifted[...]), 1)
    go_on_sum(1)
    u_form, r_form, _ = iterate(count, second_steps, 0, at_r, *end_sum(1), final=True)
    results = (
        (update, part + combined(count, u_form, lifted[...])),
        (residual, combined(count, r_form, basis[...])),
    )
    for out, row in results:
        spread = jnp.zeros((TILES, LANES), F32)
        for a, col in enumerate(column(row)):
            spread = jnp.where(lane == a, col, spread)
        small[...] = spread
        for y in range(TY):
            out[0, y] = small[2 * y : 2 * y + 2, 0:COMPS]


def finish_kernel(first, second, first_out, second_out, sems):
    copies = [
        pltpu.make_async_copy(first, first_out, sems.at[0]),
        pltpu.make_async_copy(second, second_out, sems.at[1]),
    ]
    for copy in copies:
        copy.start()
    for copy in copies:
        copy.wait()


def vmem(*shape):
    return pltpu.VMEM(shape, F32)


def on_device(source_points, target_points, normals, weights, blocks, affines, anchor):
    points = source_points.shape[5]
    dirs = len(OFFSETS)
    sizes = [lax.axis_size(a) for a in AXES]
    later = SECOND - AHEAD
    amounts = (1,) * (FIRST + AHEAD) + (2,) * (later - 1) + (1,)
    steps = len(amounts)
    pair_size = sizes[1] * sizes[2]
    anywhere = pl.BlockSpec(memory_space=pl.ANY)
    in_vmem = pl.BlockSpec(memory_space=pltpu.VMEM)
    in_smem = pl.BlockSpec(memory_space=pltpu.SMEM)
    copies = len(PIECES) + OTHERS
    dma = pltpu.SemaphoreType.DMA
    last = (1, 2, 3, 0)
    outs = pl.pallas_call(
        functools.partial(step_kernel, (FIRST, SECOND, AHEAD, amounts)),
        out_shape=(jax.ShapeDtypeStruct((1, TY, TZ, COMPS), F32),) * 2,
        in_specs=[anywhere] * 4 + [in_vmem] * 2 + [in_smem],
        out_specs=[in_vmem] * 2,
        scratch_shapes=[
            vmem(*source_points.shape),
            vmem(*target_points.shape),
            vmem(*normals.shape),
            vmem(*weights.shape),
            vmem(3, dirs, TY, TZ, points),
            vmem(1, LANES),
            vmem(OTHERS, 1, LANES),
            vmem(13, TILES, points),
            vmem(LANES, points),
            vmem(dirs, WIDE + ROWS + TILES, points),
            vmem(LANES, points),
            vmem(16, LANES),
            vmem(TILES, LANES),
            pltpu.VMEM((TILES, 1), jnp.int32),
            vmem(dirs, TILES, points),
            vmem(len(PAIRS), WIDE, LANES),
            vmem(OTHERS + 1, 16, LANES),
            vmem(ROWS, LANES),
            vmem(OTHERS, 16, LANES),
            vmem(COMPS, 16, LANES),
            vmem(ROWS, LANES),
            *[vmem(16, LANES)] * 4,
            vmem(2, pair_size, 2, LANES),
            vmem(2, sizes[0], 2, LANES),
            vmem(2, 2, LANES),
            vmem(2, 2, LANES),
            *[vmem(1, r, LANES) for r in amounts],
            *[vmem(OTHERS, r, LANES) for r in amounts],
            *[vmem(OTHERS, r, LANES) for r in amounts],
            *[vmem(OTHERS, r, LANES) for r in amounts],
            vmem(1, LANES),
            vmem(2, LANES),
            vmem(16, LANES),
            vmem(2 * OTHERS, 1, LANES),
            vmem(2 * OTHERS, 2, LANES),
            vmem(OTHERS, 16, LANES),
            dma((4,)),
            dma((copies,)),
            dma((copies,)),
            dma,
            dma,
            dma((steps, 4)),
            dma((2, 4)),
        ],
        compiler_params=pltpu.CompilerParams(
            collective_id=0, has_side_effects=True, vmem_limit_bytes=60 * 2**20
        ),
        name="step",
    )(
        source_points,
        target_points,
        normals,
        weights,
        jnp.transpose(blocks, last),
        jnp.transpose(affines, last),
        anchor,
    )
    outs = pl.pallas_call(
        finish_kernel,
        out_shape=tuple(jax.ShapeDtypeStruct(out.shape, F32) for out in outs),
        in_specs=[anywhere] * 2,
        out_specs=[anywhere] * 2,
        scratch_shapes=[dma((2,))],
        name="finish",
    )(*outs)
    return tuple(jnp.transpose(out, (3, 0, 1, 2)) for out in outs)


def solution(mesh):
    placed = (
        P(None, None, "gx", "gy", "gz", None),
        P(None, None, "gx", "gy", "gz", None),
        P(None, None, "gx", "gy", "gz", None),
        P(None, "gx", "gy", "gz", None),
        P(None, "gx", "gy", "gz"),
        P(None, "gx", "gy", "gz"),
        P(),
    )
    return jax.shard_map(
        on_device,
        mesh=mesh,
        in_specs=placed,
        out_specs=(P(None, "gx", "gy", "gz"), P(None, "gx", "gy", "gz")),
        check_vma=False,
    )
```
